256 devices in a mesh: dp: 256 (over z, y, x, core).
Axes of the slice: x: 4, y: 4, z: 8, core: 2. Of those that a mesh axis runs over, the one named last changes fastest.
Arguments:
- features: bfloat16 [4096, 1024], P('dp')
- w_in: bfloat16 [1024, 1024], replicated
- w_out: bfloat16 [1024, 256], replicated
- item_table: bfloat16 [524288, 256], P('dp')
- cand_ids: int32 [524288], replicated
- log_q: float32 [524288], replicated
- targets: int32 [4096], P('dp')
Outputs:
- output 1: float32 [], replicated
- output 2: float32 [524288, 256], P('dp')
- output 3: float32 [1024, 1024], replicated
- output 4: float32 [1024, 256], replicated
All inputs are finite; a program needn't handle non-finite values.
Results may differ from the reference program's by a relative error of at most 0.001.
Values are sent between devices in bfloat16 or wider.
A program may use at most 768 MiB of HBM per device.

```python
import jax
import jax.numpy as jnp
from jax import lax

IN_DIM = 1024
HID_DIM = 1024
EMB_DIM = 256
NUM_ITEMS = 524288
GROUPS = 256
TOK_DEV = 16
CAND_DEV = 2048
TOKENS = 4096
NUM_CANDS = 524288
BLOCK_ROWS = 2048


def draw_ids(id_key):
    key_perm, key_blk_a, key_blk_b, key_hit, key_row = jax.random.split(id_key, 5)
    perm_keys = jax.random.split(key_perm, GROUPS)
    local_rows = jax.vmap(lambda perm_key: jax.random.permutation(perm_key, BLOCK_ROWS)[:CAND_DEV])(perm_keys)
    block_base = BLOCK_ROWS * jnp.arange(GROUPS, dtype=jnp.int32)
    cand_ids = (local_rows.astype(jnp.int32) + block_base[:, None]).reshape(NUM_CANDS)
    tok_pos = jnp.arange(TOKENS, dtype=jnp.int32)
    skew_block = jnp.minimum(jax.random.randint(key_blk_a, (TOKENS,), 0, GROUPS), jax.random.randint(key_blk_b, (TOKENS,), 0, GROUPS))
    owner_block = jnp.where(tok_pos < GROUPS, tok_pos, skew_block)
    hit_slot = owner_block * CAND_DEV + jax.random.randint(key_hit, (TOKENS,), 0, CAND_DEV)
    row_pair = jax.random.randint(key_row, (2, TOKENS), 0, BLOCK_ROWS)
    plain_row = owner_block * BLOCK_ROWS + jnp.minimum(row_pair[0], row_pair[1])
    targets = jnp.where(tok_pos % 4 == 1, cand_ids[hit_slot], plain_row)
    return cand_ids, targets.astype(jnp.int32)


def setup_inputs(seed: int = 0) -> dict:
    root_key = jax.random.key(seed)
    key_x, key_w1, key_w2, key_tab, key_lq, key_ids = jax.random.split(root_key, 6)
    cand_ids, targets = draw_ids(key_ids)
    features = jax.random.normal(key_x, (TOKENS, IN_DIM), jnp.float32).astype(jnp.bfloat16)
    w_in = (jax.random.normal(key_w1, (IN_DIM, HID_DIM), jnp.float32) * IN_DIM ** -0.5).astype(jnp.bfloat16)
    w_out = (jax.random.normal(key_w2, (HID_DIM, EMB_DIM), jnp.float32) * HID_DIM ** -0.5).astype(jnp.bfloat16)
    item_table = (jax.random.normal(key_tab, (NUM_ITEMS, EMB_DIM), jnp.float32) * (2.0 * EMB_DIM ** -0.5)).astype(jnp.bfloat16)
    log_q = jax.random.uniform(key_lq, (NUM_CANDS,), jnp.float32, -4.0, 0.0)
    return {"features": features, "w_in": w_in, "w_out": w_out, "item_table": item_table, "cand_ids": cand_ids, "log_q": log_q, "targets": targets}


def reference(features, w_in, w_out, item_table, cand_ids, log_q, targets):
    cand_rows = item_table[cand_ids]
    feat_blocks = features.reshape(GROUPS, TOK_DEV, IN_DIM)
    tgt_blocks = targets.reshape(GROUPS, TOK_DEV)

    def block_step(carry, block_in):
        grad_cand, grad_w_in, grad_w_out, loss_sum = carry
        feat_blk, tgt_blk = block_in
        pre_act = jnp.dot(feat_blk, w_in, preferred_element_type=jnp.float32)
        act_val, gelu_back = jax.vjp(jax.nn.gelu, pre_act)
        act_b = act_val.astype(jnp.bfloat16)
        query = jnp.dot(act_b, w_out, preferred_element_type=jnp.float32).astype(jnp.bfloat16)
        query_f = query.astype(jnp.float32)
        tgt_rows = item_table[tgt_blk].astype(jnp.float32)
        tgt_logit = jnp.sum(query_f * tgt_rows, axis=1)
        cand_logit = jnp.dot(query, cand_rows.T, preferred_element_type=jnp.float32) - log_q[None, :]
        cand_logit = jnp.where(cand_ids[None, :] == tgt_blk[:, None], -1e9, cand_logit)
        top_val = jnp.maximum(jnp.max(cand_logit, axis=1), tgt_logit)
        exp_sum = jnp.sum(jnp.exp(cand_logit - top_val[:, None]), axis=1) + jnp.exp(tgt_logit - top_val)
        log_norm = top_val + jnp.log(exp_sum)
        grad_tgt = (jnp.exp(tgt_logit - log_norm) - 1.0) / TOKENS
        cand_grad = (jnp.exp(cand_logit - log_norm[:, None]) / TOKENS).astype(jnp.bfloat16)
        d_query = (grad_tgt[:, None] * tgt_rows + jnp.dot(cand_grad, cand_rows, preferred_element_type=jnp.float32)).astype(jnp.bfloat16)
        d_act = jnp.dot(d_query, w_out.T, preferred_element_type=jnp.float32)
        d_pre = gelu_back(d_act)[0].astype(jnp.bfloat16)
        grad_cand = grad_cand + jnp.dot(cand_grad.T, query, preferred_element_type=jnp.float32)
        grad_w_in = grad_w_in + jnp.dot(feat_blk.T, d_pre, preferred_element_type=jnp.float32)
        grad_w_out = grad_w_out + jnp.dot(act_b.T, d_query, preferred_element_type=jnp.float32)
        loss_sum = loss_sum + jnp.sum(log_norm - tgt_logit)
        return (grad_cand, grad_w_in, grad_w_out, loss_sum), grad_tgt[:, None] * query_f

    start_carry = (jnp.zeros((NUM_CANDS, EMB_DIM), jnp.float32), jnp.zeros((IN_DIM, HID_DIM), jnp.float32), jnp.zeros((HID_DIM, EMB_DIM), jnp.float32), jnp.zeros((), jnp.float32))
    end_carry, tgt_grad = lax.scan(block_step, start_carry, (feat_blocks, tgt_blocks))
    grad_cand, grad_w_in, grad_w_out, loss_sum = end_carry
    grad_table = jnp.zeros((NUM_ITEMS, EMB_DIM), jnp.float32).at[cand_ids].add(grad_cand).at[targets].add(tgt_grad.reshape(TOKENS, EMB_DIM))
    return loss_sum / TOKENS, grad_table, grad_w_in, grad_w_out
```

```python
import functools
import jax
import jax.numpy as jnp
from jax import lax
from jax.experimental import pallas as pl
from jax.experimental.pallas import tpu as pltpu
from jax.sharding import PartitionSpec as P

NZ, NY, NX = 8, 4, 4
LANES = 128
CHIP_TOK = 32
DEV_TOK = 16
MIB = 1 << 20
MESH = pl.DeviceIdType.MESH


def coords():
    me = lax.axis_index("dp")
    return me // (NY * NX * 2), (me // (NX * 2)) % NY, (me // 2) % NX, me % 2


def dev(z, y, x, c):
    return (((z * NY + y) * NX + x) * 2 + c,)


def rcopy(src, dst, ssem, rsem, to):
    return pltpu.make_async_remote_copy(src_ref=src, dst_ref=dst, send_sem=ssem, recv_sem=rsem, device_id=to, device_id_type=MESH)


def entry_barrier(z, y, x, c):
    bar = pltpu.get_barrier_semaphore()
    peers = [dev(z, y, x, 1 - c)]
    peers += [dev(z, y, (x + k) % NX, c) for k in range(1, NX)]
    peers += [dev(z, (y + k) % NY, x, c) for k in range(1, NY)]
    peers += [dev((z + k) % NZ, y, x, c) for k in range(1, NZ)]
    for p in peers:
        pl.semaphore_signal(bar, inc=1, device_id=p, device_id_type=MESH)
    pl.semaphore_wait(bar, len(peers))


def ag_tail(out_ref, z, y, x, c, s1, r1, s2, r2, s3, r3, sd, rd):
    blk = out_ref.at[c, z, y, x]
    to_c = dev(z, y, x, 1 - c)
    c1 = [rcopy(blk, blk, s1.at[k - 1], r1.at[k - 1], dev((z + k) % NZ, y, x, c)) for k in range(1, NZ)]
    for cp in c1:
        cp.start()
    for cp in c1:
        cp.wait()
    col = out_ref.at[c, :, y, x]
    c2 = [rcopy(col, col, s2.at[k - 1], r2.at[k - 1], dev(z, (y + k * (1 - c)) % NY, (x + k * c) % NX, c)) for k in range(1, 4)]
    for cp in c2:
        cp.start()
    dc = [rcopy(col, col, sd.at[0], rd.at[0], to_c)]
    dc[0].start()
    for cp in c2:
        cp.wait()

    def last(sl, to, got):
        c3 = [rcopy(sl, sl, s3.at[k - 1], r3.at[k - 1], to(k)) for k in range(1, 4)]
        for cp in c3:
            cp.start()
        dd = []
        for k in range(1, 4):
            g = got(k, 2)
            dd.append(rcopy(g, g, sd.at[k], rd.at[k], to_c))
            dd[-1].start()
        for k in (1, 3, 2):
            c3[k - 1].wait()
            g = got(k, 3)
            dd.append(rcopy(g, g, sd.at[3 + k], rd.at[3 + k], to_c))
            dd[-1].start()
        for cp in dd:
            cp.wait_send()

    @pl.when(c == 0)
    def _():
        last(out_ref.at[0, :, :, x], lambda k: dev(z, y, (x + k) % NX, c),
             lambda k, ph: out_ref.at[0, :, (y + NY - k) % NY, x] if ph == 2 else out_ref.at[0, :, :, (x + NX - k) % NX])

    @pl.when(c == 1)
    def _():
        last(out_ref.at[1, :, y, :], lambda k: dev(z, (y + k) % NY, x, c),
             lambda k, ph: out_ref.at[1, :, y, (x + NX - k) % NX] if ph == 2 else out_ref.at[1, :, (y + NY - k) % NY, :])

    dc[0].wait()
    for k in range(1, 4):
        rcopy(col, col, sd.at[k], rd.at[k], to_c).wait_recv()
        pln = out_ref.at[0, :, :, 0]
        rcopy(pln, pln, sd.at[3 + k], rd.at[3 + k], to_c).wait_recv()


def ag_start(src_ref, out_ref, z, y, x, c, loc_sem, ssem, rsem):
    half = out_ref.shape[-1]
    mine = pl.ds(pl.multiple_of(c * half, half), half)
    other = pl.ds(pl.multiple_of((1 - c) * half, half), half)
    rows = pl.ds(pl.multiple_of(c * DEV_TOK, DEV_TOK), DEV_TOK)
    cp0 = rcopy(src_ref.at[:, other], out_ref.at[1 - c, z, y, x, rows, :], ssem, rsem, dev(z, y, x, 1 - c))
    cp0.start()
    cl = pltpu.make_async_copy(src_ref.at[:, mine], out_ref.at[c, z, y, x, rows, :], loc_sem)
    cl.start()
    cl.wait()
    cp0.wait()


def ag_kernel(src_ref, out_ref, loc_sem, ssem, rsem, *sems):
    z, y, x, c = coords()
    entry_barrier(z, y, x, c)
    ag_start(src_ref, out_ref, z, y, x, c, loc_sem, ssem, rsem)
    ag_tail(out_ref, z, y, x, c, *sems)


def ag_y_kernel(src_ref, y_ref, out_ref, yout_ref, ytmp, loc_sem, ssem, rsem, t1, q1, t2, q2, t3, q3, t4, q4, *sems):
    z, y, x, c = coords()
    entry_barrier(z, y, x, c)
    cy = rcopy(y_ref, ytmp, t1, q1, dev(z, y, x, 1 - c))
    cy.start()
    ag_start(src_ref, out_ref, z, y, x, c, loc_sem, ssem, rsem)
    cy.wait()
    yout_ref[z, y, x] = y_ref[...] + ytmp[...]
    for axis, to, sl, ts, qs in (
        (NX, lambda k: dev(z, y, (x + k) % NX, c), yout_ref.at[z, y, x], t2, q2),
        (NY, lambda k: dev(z, (y + k) % NY, x, c), yout_ref.at[z, y], t3, q3),
        (NZ, lambda k: dev((z + k) % NZ, y, x, c), yout_ref.at[z], t4, q4),
    ):
        cps = [rcopy(sl, sl, ts.at[k - 1], qs.at[k - 1], to(k)) for k in range(1, axis)]
        for cp in cps:
            cp.start()
        for cp in cps:
            cp.wait()
    ag_tail(out_ref, z, y, x, c, *sems)


_D = pltpu.SemaphoreType.DMA
_AG_SEMS = [_D((7,)), _D((7,)), _D((3,)), _D((3,)), _D((3,)), _D((3,)), _D((7,)), _D((7,))]


def all_gather(src, cid, name):
    cols = src.shape[1]
    return pl.pallas_call(
        ag_kernel, name=name,
        out_shape=jax.ShapeDtypeStruct((2, NZ, NY, NX, CHIP_TOK, cols // 2), src.dtype),
        in_specs=[pl.BlockSpec(memory_space=pl.ANY)],
        out_specs=pl.BlockSpec(memory_space=pltpu.VMEM),
        scratch_shapes=[_D, _D, _D] + _AG_SEMS,
        compiler_params=pltpu.CompilerParams(collective_id=cid, has_side_effects=True, vmem_limit_bytes=40 * MIB),
    )(src)


def all_gather_y(src, yrow, cid, name):
    cols = src.shape[1]
    V = pl.BlockSpec(memory_space=pltpu.VMEM)
    return pl.pallas_call(
        ag_y_kernel, name=name,
        out_shape=(jax.ShapeDtypeStruct((2, NZ, NY, NX, CHIP_TOK, cols // 2), src.dtype), jax.ShapeDtypeStruct((NZ, NY, NX, 1, LANES), jnp.int32)),
        in_specs=[pl.BlockSpec(memory_space=pl.ANY), V],
        out_specs=(V, V),
        scratch_shapes=[pltpu.VMEM((1, LANES), jnp.int32), _D, _D, _D, _D, _D, _D((3,)), _D((3,)), _D((3,)), _D((3,)), _D((7,)), _D((7,))] + _AG_SEMS,
        compiler_params=pltpu.CompilerParams(collective_id=cid, has_side_effects=True, vmem_limit_bytes=40 * MIB),
    )(src, yrow)


def ag_rows(full):
    return jnp.concatenate([full[0].reshape(-1, full.shape[-1]), full[1].reshape(-1, full.shape[-1])], axis=1)


NEG = -jnp.inf
CH = NY * NX * CHIP_TOK


def lane_row_to_col(row):
    return jnp.transpose(jnp.broadcast_to(row, (LANES, LANES)))


def logq_rows(cid_v, lq_v, lqr_ref, base):
    for blk in range(lqr_ref.shape[1] // LANES):
        rid = lax.broadcasted_iota(jnp.int32, (LANES, LANES), 0) + (base + blk * LANES)
        acc = jnp.zeros((LANES, LANES), jnp.float32)
        for q in range(DEV_TOK):
            acc += jnp.where(cid_v[q:q + 1, :] == rid, lq_v[q:q + 1, :], 0.0)
        col = jnp.broadcast_to(jnp.sum(acc, axis=1, keepdims=True), (LANES, LANES))
        lqr_ref[:, blk * LANES:(blk + 1) * LANES] = jnp.transpose(col)[:8]


def scores_chunk(h, emb_ref, lqr_ref, e_ref, d_ref, mcol_ref, zcol_ref, scol_ref):
    rows = emb_ref.shape[0]
    RB = 64
    for j in range(0, rows, 256):
        s = lax.dot_general(h, emb_ref[j:j + 256, :], (((1,), (1,)), ((), ())), preferred_element_type=jnp.float32)
        for rb in range(0, CH, RB):
            rs = slice(rb, rb + RB)
            m = mcol_ref[rs, :] if j else jnp.full((RB, LANES), NEG, jnp.float32)
            zc = zcol_ref[rs, :] if j else jnp.full((RB, LANES), NEG, jnp.float32)
            d = d_ref[rs, :]
            for k in (0, LANES):
                raw = s[rs, k:k + LANES]
                hit = d == float(j + k)
                zc = jnp.where(hit, raw, zc)
                v = jnp.where(hit, -1e9, raw - lqr_ref[:1, j + k:j + k + LANES])
                e_ref[rs, j + k:j + k + LANES] = v
                m = jnp.maximum(m, v)
            mcol_ref[rs, :] = m
            zcol_ref[rs, :] = zc
    for rb in range(0, CH, RB):
        rs = slice(rb, rb + RB)
        zc = jnp.max(zcol_ref[rs, :], axis=1, keepdims=True)
        m = jnp.maximum(jnp.max(mcol_ref[rs, :], axis=1, keepdims=True), zc)
        zcol_ref[rs, :] = jnp.broadcast_to(zc, (RB, LANES))
        mcol_ref[rs, :] = jnp.broadcast_to(m, (RB, LANES))

    def grp(g, _):
        rs = pl.ds(pl.multiple_of(g * CHIP_TOK, CHIP_TOK), CHIP_TOK)
        m = mcol_ref[rs, :]
        tot = jnp.zeros((CHIP_TOK, LANES), jnp.float32)
        for k in range(0, rows, LANES):
            ex = jnp.exp(e_ref[rs, k:k + LANES] - m)
            e_ref[rs, k:k + LANES] = ex
            tot += ex
        scol_ref[rs, :] = tot
        return 0
    lax.fori_loop(0, CH // CHIP_TOK, grp, 0)
    for rb in range(0, CH, RB):
        rs = slice(rb, rb + RB)
        tot = jnp.sum(scol_ref[rs, :], axis=1, keepdims=True)
        scol_ref[rs, :] = jnp.broadcast_to(tot, (RB, LANES)) + jnp.exp(zcol_ref[rs, :] - mcol_ref[rs, :])


def scores_kernel(h_ref, emb_ref, y_ref, cid_hbm, lq_hbm, e_ref, mcol_ref, mrow_ref, srow_ref, zrow_ref,
                  cid_v, lq_v, lqr_ref, d_ref, zcol_ref, scol_ref, sem):
    zi = pl.program_id(0)
    me = lax.axis_index("dp")
    rows = emb_ref.shape[0]
    base = me * rows

    @pl.when(zi == 0)
    def _():
        own = pl.ds(me * DEV_TOK, DEV_TOK)
        ca = pltpu.make_async_copy(cid_hbm.at[own], cid_v, sem.at[0])
        cb = pltpu.make_async_copy(lq_hbm.at[own], lq_v, sem.at[1])
        ca.start()
        cb.start()
        ca.wait()
        cb.wait()
        logq_rows(cid_v, lq_v, lqr_ref, base)

    lane = lax.broadcasted_iota(jnp.int32, (LANES, LANES), 1).astype(jnp.float32)
    for b in range(CH // LANES):
        yr = jnp.sum(y_ref[0, b, :, 0, :], axis=0, keepdims=True) - base
        d_ref[b * LANES:(b + 1) * LANES, :] = lane_row_to_col(yr.astype(jnp.float32)) - lane
    h = jnp.concatenate([h_ref[0, 0].reshape(CH, LANES), h_ref[1, 0].reshape(CH, LANES)], axis=1)
    scores_chunk(h, emb_ref, lqr_ref, e_ref, d_ref, mcol_ref, zcol_ref, scol_ref)
    for b in range(CH // LANES):
        bs = slice(b * LANES, (b + 1) * LANES)
        row = pl.ds(zi * (CH // LANES) + b, 1)
        mrow_ref[row, :] = jnp.transpose(mcol_ref[bs, :])[:1]
        srow_ref[row, :] = jnp.transpose(scol_ref[bs, :])[:1]
        zrow_ref[row, :] = jnp.transpose(zcol_ref[bs, :])[:1]


def scores(hfull, emb, yfull, cand_ids, log_q):
    rows = emb.shape[0]
    tok = NZ * CH
    whole = lambda *s: pl.BlockSpec(s, lambda i: (0,) * len(s))
    return pl.pallas_call(
        scores_kernel, name="scores", grid=(NZ,),
        out_shape=(jax.ShapeDtypeStruct((tok, rows), jnp.float32),
                   jax.ShapeDtypeStruct((tok, LANES), jnp.float32), jax.ShapeDtypeStruct((tok // LANES, LANES), jnp.float32),
                   jax.ShapeDtypeStruct((tok // LANES, LANES), jnp.float32), jax.ShapeDtypeStruct((tok // LANES, LANES), jnp.float32)),
        in_specs=[pl.BlockSpec((2, 1, NY, NX, CHIP_TOK, LANES), lambda i: (0, i, 0, 0, 0, 0)), whole(rows, 256),
                  pl.BlockSpec((1, NY, NX, 1, LANES), lambda i: (i, 0, 0, 0, 0)), pl.BlockSpec(memory_space=pl.ANY), pl.BlockSpec(memory_space=pl.ANY)],
        out_specs=(pl.BlockSpec((CH, rows), lambda i: (i, 0)),
                   pl.BlockSpec((CH, LANES), lambda i: (i, 0)), whole(tok // LANES, LANES), whole(tok // LANES, LANES), whole(tok // LANES, LANES)),
        scratch_shapes=[pltpu.VMEM((DEV_TOK, LANES), jnp.int32), pltpu.VMEM((DEV_TOK, LANES), jnp.float32), pltpu.VMEM((8, rows), jnp.float32),
                        pltpu.VMEM((CH, LANES), jnp.float32), pltpu.VMEM((CH, LANES), jnp.float32), pltpu.VMEM((CH, LANES), jnp.float32),
                        pltpu.SemaphoreType.DMA((2,))],
        compiler_params=pltpu.CompilerParams(vmem_limit_bytes=48 * MIB),
    )(hfull, emb, yfull, cand_ids.reshape(-1, LANES), log_q.reshape(-1, LANES))


HR = DEV_TOK


def merge_stats(parts):
    m = functools.reduce(jnp.maximum, [p[:HR] for p in parts])
    s = sum(p[HR:2 * HR] * jnp.exp(p[:HR] - m) for p in parts)
    t = sum(p[2 * HR:] for p in parts)
    return m, s, t


def put_stats(ref, parts):
    m, s, t = merge_stats(parts)
    ref[0:HR, :] = m
    ref[HR:2 * HR, :] = s
    ref[2 * HR:, :] = t


def stats_kernel(m_ref, s_ref, z_ref, l_ref, loss_ref, b0, bc, bx, by, bz, fin, sc, rc, sx, rx, sy, ry, sz, rz, sf, rf):
    z, y, x, c = coords()
    entry_barrier(z, y, x, c)
    for hf in range(2):
        hs = slice(hf * HR, (hf + 1) * HR)
        zz = z_ref[hs, :]
        zz = jnp.where(zz > NEG, zz, 0.0)
        b0[hf, 0:HR, :] = m_ref[hs, :]
        b0[hf, HR:2 * HR, :] = s_ref[hs, :]
        b0[hf, 2 * HR:, :] = zz[:8] + zz[8:]
    cp = rcopy(b0.at[1 - c], bc, sc, rc, dev(z, y, x, 1 - c))
    cp.start()
    cp.wait()
    here, there = b0[c], bc[...]
    even = c == 0
    put_stats(bx.at[x], [jnp.where(even, here, there), jnp.where(even, there, here)])
    cps = [rcopy(bx.at[x], bx.at[x], sx.at[k - 1], rx.at[k - 1], dev(z, y, (x + k) % NX, c)) for k in range(1, NX)]
    [cp.start() for cp in cps]
    [cp.wait() for cp in cps]
    put_stats(by.at[y], [bx[i] for i in range(NX)])
    cps = [rcopy(by.at[y], by.at[y], sy.at[k - 1], ry.at[k - 1], dev(z, (y + k) % NY, x, c)) for k in range(1, NY)]
    [cp.start() for cp in cps]
    [cp.wait() for cp in cps]
    put_stats(bz.at[z], [by[i] for i in range(NY)])
    cps = [rcopy(bz.at[z], bz.at[z], sz.at[k - 1], rz.at[k - 1], dev((z + k) % NZ, y, x, c)) for k in range(1, NZ)]
    [cp.start() for cp in cps]
    [cp.wait() for cp in cps]
    m, s, t = merge_stats([bz[i] for i in range(NZ)])
    fin[c, 0:HR, :] = m + jnp.log(s)
    fin[c, HR:, :] = t
    cp = rcopy(fin.at[c], fin.at[c], sf, rf, dev(z, y, x, 1 - c))
    cp.start()
    cp.wait()
    ls = fin[0, 0:HR, :] + fin[1, 0:HR, :]
    ls = ls[:8] + ls[8:] - (fin[0, HR:, :] + fin[1, HR:, :])
    l_ref[0:HR, :] = fin[0, 0:HR, :]
    l_ref[HR:, :] = fin[1, 0:HR, :]
    tot = jnp.sum(jnp.sum(ls, axis=0, keepdims=True), axis=1, keepdims=True)
    loss_ref[...] = jnp.broadcast_to(tot * (1.0 / (NZ * CH)), (8, LANES))


def stats(mrow, srow, zrow, cid):
    V = pl.BlockSpec(memory_space=pltpu.VMEM)
    D = pltpu.SemaphoreType.DMA
    buf = lambda n: pltpu.VMEM((n, 40, LANES), jnp.float32)
    return pl.pallas_call(
        stats_kernel, name="stats",
        out_shape=(jax.ShapeDtypeStruct(mrow.shape, jnp.float32), jax.ShapeDtypeStruct((8, LANES), jnp.float32)),
        in_specs=[V] * 3, out_specs=(V, V),
        scratch_shapes=[buf(2), pltpu.VMEM((40, LANES), jnp.float32), buf(NX), buf(NY), buf(NZ), pltpu.VMEM((2, 24, LANES), jnp.float32),
                        D, D, D((3,)), D((3,)), D((3,)), D((3,)), D((7,)), D((7,)), D, D],
        compiler_params=pltpu.CompilerParams(collective_id=cid, has_side_effects=True),
    )(mrow, srow, zrow)


def grad_kernel(e_hbm, mcol_hbm, h_ref, emb_ref, y_ref, l_ref, z_ref, dh_ref, de_ref,
                ebuf, mbuf, p_ref, d_ref, dq, rc, a0, ra, a1, rb, zb, esem, msem,
                sc, rcs, sa, ras, sb, rbs, sz, rzs, s1, r1, s2, r2, s3, r3, sd, rd):
    z, y, x, c = coords()
    me = lax.axis_index("dp")
    rows = emb_ref.shape[0]
    base = me * rows
    ax1 = x * (1 - c) + y * c
    ax2 = y * (1 - c) + x * c
    to_c = dev(z, y, x, 1 - c)
    to_1 = lambda k: dev(z, (y + k * c) % NY, (x + k * (1 - c)) % NX, c)
    to_2 = lambda k: dev(z, (y + k * (1 - c)) % NY, (x + k * c) % NX, c)

    def chunk(k):
        return (z + 1 + k) % NZ

    def load(k, slot):
        ch = chunk(k)
        return (pltpu.make_async_copy(e_hbm.at[pl.ds(pl.multiple_of(ch * CH, CH), CH)], ebuf.at[slot], esem.at[slot]),
                pltpu.make_async_copy(mcol_hbm.at[pl.ds(pl.multiple_of(ch * CH, CH), CH)], mbuf.at[slot], msem.at[slot]))

    for cp in load(0, 0):
        cp.start()
    entry_barrier(z, y, x, c)
    de_ref[...] = jnp.zeros_like(de_ref)
    lane = lax.broadcasted_iota(jnp.int32, (LANES, LANES), 1).astype(jnp.float32)
    c_copy = lambda k: rcopy(dq.at[k, 1 - c], rc.at[k], sc.at[k], rcs.at[k], to_c)
    a_copy = lambda k, j: rcopy(a0.at[k, (ax1 + j) % 4], ra.at[k, ax1], sa.at[k, j - 1], ras.at[k, j - 1], to_1(j))
    b_copy = lambda k, j: rcopy(a1.at[k, (ax2 + j) % 4], rb.at[k, ax2], sb.at[k, j - 1], rbs.at[k, j - 1], to_2(j))
    z_copy = lambda k: rcopy(zb.at[NZ + k], zb.at[z], sz.at[k], rzs.at[k], dev(chunk(k), y, x, c))

    def body(k, _):
        @pl.when(k < NZ)
        def _():
            slot = lax.rem(k, 2)
            ch = chunk(k)

            @pl.when(k + 1 < NZ)
            def _():
                for cp in load(k + 1, 1 - slot):
                    cp.start()
            for cp in load(k, slot):
                cp.wait()
            for b in range(CH // LANES):
                bs = slice(b * LANES, (b + 1) * LANES)
                row = pl.ds(ch * (CH // LANES) + b, 1)
                lcol = lane_row_to_col(l_ref[row, :])
                sc_col = jnp.exp(mbuf[slot, bs, :] - lcol) * (1.0 / (NZ * CH))
                yr = jnp.sum(y_ref[ch, b, :, 0, :], axis=0, keepdims=True) - base
                d_ref[bs, :] = lane_row_to_col(yr.astype(jnp.float32)) - lane
                for q in range(0, rows, LANES):
                    p_ref[bs, q:q + LANES] = (ebuf[slot, bs, q:q + LANES] * sc_col).astype(jnp.bfloat16)
            h = jnp.concatenate([h_ref[0, ch].reshape(CH, LANES), h_ref[1, ch].reshape(CH, LANES)], axis=1)
            for q in range(0, rows, 512):
                de_ref[q:q + 512, :] += lax.dot_general(p_ref[:, q:q + 512], h, (((0,), (0,)), ((), ())), preferred_element_type=jnp.float32)
            dqv = jnp.dot(p_ref[...], emb_ref[...], preferred_element_type=jnp.float32)
            for q in range(0, rows, LANES):
                p_ref[:, q:q + LANES] = jnp.where(d_ref[...] == float(q), 1.0, 0.0).astype(jnp.bfloat16)
            tgt = jnp.dot(p_ref[...], emb_ref[...], preferred_element_type=jnp.float32)
            for b in range(CH // LANES):
                bs = slice(b * LANES, (b + 1) * LANES)
                row = pl.ds(ch * (CH // LANES) + b, 1)
                zr = z_ref[row, :]
                g = jnp.where(zr > NEG, (jnp.exp(zr - l_ref[row, :]) - 1.0) * (1.0 / (NZ * CH)), 0.0)
                gc = lane_row_to_col(g)
                for hf in range(2):
                    v = dqv[bs, hf * LANES:hf * LANES + LANES] + gc * tgt[bs, hf * LANES:hf * LANES + LANES]
                    dq[k, hf, b] = v.reshape(NX, CHIP_TOK, LANES)
            c_copy(k).start()

        @pl.when((k >= 1) & (k <= NZ))
        def _():
            q = k - 1
            c_copy(q).wait()
            for yy in range(NY):
                for xx in range(NX):
                    i1 = xx * (1 - c) + yy * c
                    i2 = yy * (1 - c) + xx * c
                    a0[q, i1, i2] = dq[q, c, yy, xx] + rc[q, yy, xx]
            for j in range(1, 4):
                a_copy(q, j).start()

        @pl.when((k >= 2) & (k <= NZ + 1))
        def _():
            q = k - 2
            for j in range(1, 4):
                a_copy(q, j).wait()
            ra[q, ax1] = a0[q, ax1]
            a1[q] = (ra[q, 0] + ra[q, 1]) + (ra[q, 2] + ra[q, 3])
            for j in range(1, 4):
                b_copy(q, j).start()

        @pl.when((k >= 3) & (k <= NZ + 2))
        def _():
            q = k - 3
            for j in range(1, 4):
                b_copy(q, j).wait()
            rb[q, ax2] = a1[q, ax2]
            v = (rb[q, 0] + rb[q, 1]) + (rb[q, 2] + rb[q, 3])

            @pl.when(q < NZ - 1)
            def _():
                zb[NZ + q] = v
                z_copy(q).start()

            @pl.when(q == NZ - 1)
            def _():
                zb[z] = v
        return 0

    lax.fori_loop(0, NZ + 3, body, 0)
    for k in range(NZ - 1):
        z_copy(k).wait()
    tot = ((zb[0] + zb[1]) + (zb[2] + zb[3])) + ((zb[4] + zb[5]) + (zb[6] + zb[7]))
    dh_ref[c, z, y, x] = tot.astype(jnp.bfloat16)
    ag_tail(dh_ref, z, y, x, c, s1, r1, s2, r2, s3, r3, sd, rd)


def grads(e, mcol, hfull, emb, yfull, lrow, zrow, cid):
    V = pl.BlockSpec(memory_space=pltpu.VMEM)
    A = pl.BlockSpec(memory_space=pl.ANY)
    D = pltpu.SemaphoreType.DMA
    F = jnp.float32
    rows = emb.shape[0]
    return pl.pallas_call(
        grad_kernel, name="grads",
        out_shape=(jax.ShapeDtypeStruct((2, NZ, NY, NX, CHIP_TOK, LANES), jnp.bfloat16), jax.ShapeDtypeStruct((rows, 256), F)),
        in_specs=[A, A, V, V, V, V, V], out_specs=(V, V),
        scratch_shapes=[pltpu.VMEM((2, CH, rows), F), pltpu.VMEM((2, CH, LANES), F), pltpu.VMEM((CH, rows), jnp.bfloat16), pltpu.VMEM((CH, LANES), F),
                        pltpu.VMEM((NZ, 2, NY, NX, CHIP_TOK, LANES), F), pltpu.VMEM((NZ, NY, NX, CHIP_TOK, LANES), F),
                        pltpu.VMEM((NZ, 4, 4, CHIP_TOK, LANES), F), pltpu.VMEM((NZ, 4, 4, CHIP_TOK, LANES), F),
                        pltpu.VMEM((NZ, 4, CHIP_TOK, LANES), F), pltpu.VMEM((NZ, 4, CHIP_TOK, LANES), F), pltpu.VMEM((2 * NZ, CHIP_TOK, LANES), F),
                        D((2,)), D((2,)), D((NZ,)), D((NZ,)), D((NZ, 3)), D((NZ, 3)), D((NZ, 3)), D((NZ, 3)), D((NZ - 1,)), D((NZ - 1,)),
                        D((7,)), D((7,)), D((3,)), D((3,)), D((3,)), D((3,)), D((7,)), D((7,))],
        compiler_params=pltpu.CompilerParams(collective_id=cid, has_side_effects=True, vmem_limit_bytes=60 * MIB),
    )(e, mcol, hfull, emb, yfull, lrow, zrow)


def fix_kernel(de_ref, h_ref, y_ref, l_ref, z_ref, out_ref, lst_i, lst_g, si, sg, sem):
    me = lax.axis_index("dp")
    rows = out_ref.shape[0]
    n_row = l_ref.shape[0]
    base = me * rows
    out_ref[...] = de_ref[...]
    yl = jnp.concatenate([jnp.sum(y_ref[r // NY, r % NY, :, 0, :], axis=0, keepdims=True) for r in range(n_row)], axis=0) - base
    own = (yl >= 0) & (yl < rows)
    g = jnp.where(own, (jnp.exp(jnp.where(own, z_ref[...], 0.0) - l_ref[...]) - 1.0) * (1.0 / (NZ * CH)), 0.0)
    of = jnp.where(own, 1.0, 0.0)
    tri = jnp.where(lax.broadcasted_iota(jnp.int32, (LANES, LANES), 0) < lax.broadcasted_iota(jnp.int32, (LANES, LANES), 1), 1.0, 0.0).astype(jnp.bfloat16)
    pre = jnp.dot(of.astype(jnp.bfloat16), tri, preferred_element_type=jnp.float32)
    tot = jnp.broadcast_to(jnp.sum(of, axis=1, keepdims=True), (n_row, LANES))
    low = jnp.where(lax.broadcasted_iota(jnp.int32, (n_row, n_row), 1) < lax.broadcasted_iota(jnp.int32, (n_row, n_row), 0), 1.0, 0.0).astype(jnp.bfloat16)
    off = jnp.dot(low, tot.astype(jnp.bfloat16), preferred_element_type=jnp.float32)
    rank = jnp.where(own, pre + off, -1.0)
    n = jnp.sum(of).astype(jnp.int32)
    lane = lax.broadcasted_iota(jnp.int32, (1, LANES), 1)

    def page(p, _):
        slot = (lax.broadcasted_iota(jnp.int32, (LANES, LANES), 0) + p * LANES).astype(jnp.float32)
        code = jnp.zeros((LANES, LANES), jnp.float32)
        gg = jnp.zeros((LANES, LANES), jnp.float32)
        tt = jnp.zeros((LANES, LANES), jnp.float32)
        for r in range(n_row):
            hit = rank[r:r + 1] == slot
            code += jnp.where(hit, yl[r:r + 1].astype(jnp.float32), 0.0)
            tt += jnp.where(hit, (lane + r * LANES).astype(jnp.float32), 0.0)
            gg += jnp.where(hit, g[r:r + 1], 0.0)
        row = lambda a: jnp.transpose(jnp.broadcast_to(jnp.sum(a, axis=1, keepdims=True), (LANES, LANES)))[:8]
        lst_i[0] = row(code).astype(jnp.int32)
        lst_i[1] = row(tt).astype(jnp.int32)
        lst_g[...] = row(gg)
        ca = pltpu.make_async_copy(lst_i, si, sem.at[0])
        cb = pltpu.make_async_copy(lst_g, sg, sem.at[1])
        ca.start()
        cb.start()
        ca.wait()
        cb.wait()

        def one(i, _):
            r, t, gv = si[0, 0, i], si[1, 0, i], sg[0, i]
            q, w = t // CHIP_TOK, t % CHIP_TOK
            hs = pl.ds(pl.multiple_of((w // DEV_TOK) * DEV_TOK, DEV_TOK), DEV_TOK)
            zz, yy, xx = q // (NY * NX), (q // NX) % NY, q % NX
            ht = jnp.concatenate([h_ref[0, zz, yy, xx, hs, :], h_ref[1, zz, yy, xx, hs, :]], axis=1).astype(jnp.float32)
            hr = jnp.sum(jnp.where(lax.broadcasted_iota(jnp.int32, (DEV_TOK, 1), 0) == w % DEV_TOK, ht, 0.0), axis=0, keepdims=True)
            out_ref[pl.ds(r, 1), :] += gv * hr
            return 0
        lax.fori_loop(0, jnp.minimum(n - p * LANES, LANES), one, 0)
        return 0
    lax.fori_loop(0, (n + 127) // LANES, page, 0)


def fix(de, hfull, yfull, lrow, zrow):
    V = pl.BlockSpec(memory_space=pltpu.VMEM)
    return pl.pallas_call(
        fix_kernel, name="fix", out_shape=jax.ShapeDtypeStruct(de.shape, jnp.float32),
        in_specs=[V] * 5, out_specs=V,
        scratch_shapes=[pltpu.VMEM((2, 8, LANES), jnp.int32), pltpu.VMEM((8, LANES), jnp.float32), pltpu.SMEM((2, 8, LANES), jnp.int32),
                        pltpu.SMEM((8, LANES), jnp.float32), pltpu.SemaphoreType.DMA((2,))],
        compiler_params=pltpu.CompilerParams(vmem_limit_bytes=40 * MIB),
    )(de, hfull, yfull, lrow, zrow)


def solution(mesh):
    def local_step(features, w_in, w_out, table_blk, cand_ids, log_q, targets):
        z, y, x, c = coords()
        pre_act = jnp.dot(features, w_in, preferred_element_type=jnp.float32)
        act_b = jax.nn.gelu(pre_act).astype(jnp.bfloat16)
        query = jnp.dot(act_b, w_out, preferred_element_type=jnp.float32).astype(jnp.bfloat16)
        yrow = lax.dynamic_update_slice(jnp.zeros((1, LANES), jnp.int32), targets[None, :], (0, CHIP_TOK * x + DEV_TOK * c))
        hfull, yfull = all_gather_y(query, yrow, 0, "ag_query")
        e, mcol, mrow, srow, zrow = scores(hfull, table_blk, yfull, cand_ids, log_q)
        lrow, loss = stats(mrow, srow, zrow, 1)
        dhfull, de = grads(e, mcol, hfull, table_blk, yfull, lrow, zrow, 2)
        grad_blk = fix(de, hfull, yfull, lrow, zrow)
        xfull = all_gather(features, 3, "ag_feat")
        dh = ag_rows(dhfull)
        feat = ag_rows(xfull)
        pre, = [jnp.dot(feat, w_in, preferred_element_type=jnp.float32)]
        act, back = jax.vjp(jax.nn.gelu, pre)
        act_all = act.astype(jnp.bfloat16)
        d_act = jnp.einsum("td,fd->tf", dh, w_out, preferred_element_type=jnp.float32)
        d_pre = back(d_act)[0].astype(jnp.bfloat16)
        grad_w_out = jnp.einsum("tf,td->fd", act_all, dh, preferred_element_type=jnp.float32)
        grad_w_in = jnp.einsum("ti,tf->if", feat, d_pre, preferred_element_type=jnp.float32)
        return loss[0, 0], grad_blk, grad_w_in, grad_w_out

    return jax.shard_map(local_step, mesh=mesh, in_specs=(P("dp", None), P(), P(), P("dp", None), P(), P(), P("dp")), out_specs=(P(), P("dp", None), P(), P()), check_vma=False)
```

```python
import functools
import math
import jax
import jax.numpy as jnp
from jax import lax
from jax.experimental import pallas as pl
from jax.experimental.pallas import tpu as pltpu
from jax.sharding import PartitionSpec as P

NZ, NY, NX = 8, 4, 4
NA = 4
LN = 128
TD = 16
NC = 2 * NA
CH = NZ * NA * TD
NT = NC * CH
PZ = NA * TD
SR = NT // LN
GR = CH // LN
F32, BF16 = jnp.float32, jnp.bfloat16
NEG = -jnp.inf
MESH = pl.DeviceIdType.MESH
DMA = pltpu.SemaphoreType.DMA


def coords():
    me = lax.axis_index("dp")
    z, y, x, c = me // (NY * NX * 2), (me // (NX * 2)) % NY, (me // 2) % NX, me % 2
    return z, y, x, c, x * (1 - c) + y * c, y * (1 - c) + x * c


def dev(z, y, x, c):
    return (((z * NY + y) * NX + x) * 2 + c,)


def peers():
    z, y, x, c, v, a = coords()
    return (dev(z, y, x, 1 - c), lambda k: dev((z + k) % NZ, y, x, c), lambda k: dev(z, (y + k * c) % NY, (x + k * (1 - c)) % NX, c),
            lambda k: dev(z, (y + k * (1 - c)) % NY, (x + k * c) % NX, c))


def rcopy(src, dst, ssem, rsem, to):
    return pltpu.make_async_remote_copy(src_ref=src, dst_ref=dst, send_sem=ssem, recv_sem=rsem, device_id=to, device_id_type=MESH)


def run(copies):
    for cp in copies:
        cp.start()
    for cp in copies:
        cp.wait()


def signal_peers():
    bar = pltpu.get_barrier_semaphore()
    to_c, to_z, to_1, to_2 = peers()
    everyone = [to_c] + [to_1(k) for k in range(1, NA)] + [to_2(k) for k in range(1, NA)] + [to_z(k) for k in range(1, NZ)]
    for p in everyone:
        pl.semaphore_signal(bar, inc=1, device_id=p, device_id_type=MESH)
    return bar, len(everyone)


NEAR = (1, 3, 2)


class Gather:
    SEMS = [DMA((NZ - 1,)), DMA((NZ - 1,)), DMA((NA,)), DMA((NA,)), DMA((NA, NA)), DMA((NA, NA)), DMA((NA,)), DMA((NA,))]

    def __init__(self, buf, sems, src=None):
        z, y, x, c, v, a = coords()
        sz, rz, s2, r2, s1, r1, sd, rd = sems
        to_c, to_z, to_1, to_2 = peers()
        self.c, self.v, self.a = c, v, a
        own = buf.at[c, v, z, a]
        col = lambda j: buf.at[c, v, :, (a + NA - j) % NA]
        chunk = lambda j: buf.at[c, (v + NA - j) % NA]
        self.zc = lambda k: rcopy(own if src is None else src, own, sz.at[k - 1], rz.at[k - 1], to_z(k))
        self.ac = lambda k: rcopy(col(0), col(0), s2.at[k], r2.at[k], to_2(k))
        self.vc = lambda k, p: rcopy(col(p), col(p), s1.at[k, p], r1.at[k, p], to_1(k))
        self.dc = lambda j: rcopy(chunk(j), chunk(j), sd.at[j], rd.at[j], to_c)

    def start(self):
        @pl.loop(1, NZ)
        def _(k):
            self.zc(k).start()

    def second(self):
        @pl.loop(1, NZ)
        def _(k):
            self.zc(k).wait()
        for k in NEAR:
            self.ac(k).start()

    def first(self):
        for k in NEAR:
            self.vc(k, 0).start()
        for j in NEAR:
            self.ac(j).wait()
            for k in NEAR:
                self.vc(k, j).start()
        self.dc(0).start()

    def take(self, n):
        i, p = n // 2, n % 2
        j = i + (i // 2) * (1 - 2 * (i % 2))

        @pl.when((p == 0) & (i > 0))
        def _():
            for q in range(NA):
                self.vc(j, q).wait()
            self.dc(j).start()

        @pl.when(p == 1)
        def _():
            self.dc(j).wait()
        return self.c + p * (1 - 2 * self.c), (self.v * (1 - p) + self.a * p + NA - j) % NA


def to_col(row):
    return jnp.transpose(jnp.broadcast_to(row, (LN, LN)))


def logq_rows(cid_v, lq_v, lqr_ref, base):
    @pl.loop(0, lqr_ref.shape[1] // LN)
    def _(i):
        blk = pl.multiple_of(i * LN, LN)
        rid = lax.broadcasted_iota(jnp.int32, (LN, LN), 0) + (base + blk)
        acc = jnp.zeros((LN, LN), F32)
        for q in range(cid_v.shape[0]):
            acc += jnp.where(cid_v[q:q + 1, :] == rid, lq_v[q:q + 1, :], 0.0)
        lqr_ref[:, pl.ds(blk, LN)] = jnp.transpose(jnp.broadcast_to(jnp.sum(acc, axis=1, keepdims=True), (LN, LN)))[:8]


def target_cols(yblk, base, yl_ref, row, d_ref):
    lane = lax.broadcasted_iota(jnp.int32, (LN, LN), 1).astype(F32)
    group = lax.broadcasted_iota(jnp.int32, (1, LN), 1) // TD
    for g in range(GR):
        yr = sum(jnp.where(group == b, yblk(g * 8 + b), 0) for b in range(8)) - base
        yl_ref[pl.ds(row + g, 1), :] = yr
        d_ref[g * LN:(g + 1) * LN, :] = to_col(yr.astype(F32)) - lane


def scores_chunk(h, emb_ref, lqr_ref, e_ref, d_ref, mcol_ref, zcol_ref, scol_ref):
    rows = emb_ref.shape[0]
    RB = PZ
    for j in range(0, rows, 2 * LN):
        s = lax.dot_general(h, emb_ref[j:j + 2 * LN, :], (((1,), (1,)), ((), ())), preferred_element_type=F32)
        for rb in range(0, CH, RB):
            rs = slice(rb, rb + RB)
            m = mcol_ref[rs, :] if j else jnp.full((RB, LN), NEG, F32)
            zc = zcol_ref[rs, :] if j else jnp.full((RB, LN), NEG, F32)
            d = d_ref[rs, :]
            for k in (0, LN):
                raw = s[rs, k:k + LN]
                hit = d == float(j + k)
                zc = jnp.where(hit, raw, zc)
                val = jnp.where(hit, -1e9, raw - lqr_ref[:1, j + k:j + k + LN])
                e_ref[rs, j + k:j + k + LN] = val
                m = jnp.maximum(m, val)
            mcol_ref[rs, :] = m
            zcol_ref[rs, :] = zc
    for rb in range(0, CH, RB):
        rs = slice(rb, rb + RB)
        zc = jnp.max(zcol_ref[rs, :], axis=1, keepdims=True)
        m = jnp.maximum(jnp.max(mcol_ref[rs, :], axis=1, keepdims=True), zc)
        zcol_ref[rs, :] = jnp.broadcast_to(zc, (RB, LN))
        mcol_ref[rs, :] = jnp.broadcast_to(m, (RB, LN))

    def grp(g, _):
        rs = pl.ds(pl.multiple_of(g * 2 * TD, 2 * TD), 2 * TD)
        m = mcol_ref[rs, :]
        tot = jnp.zeros((2 * TD, LN), F32)
        for k in range(0, rows, LN):
            ex = jnp.exp(e_ref[rs, k:k + LN] - m)
            e_ref[rs, k:k + LN] = ex
            tot += ex
        scol_ref[rs, :] = tot
        return 0
    lax.fori_loop(0, CH // (2 * TD), grp, 0)
    for rb in range(0, CH, RB):
        rs = slice(rb, rb + RB)
        tot = jnp.sum(scol_ref[rs, :], axis=1, keepdims=True)
        scol_ref[rs, :] = jnp.broadcast_to(tot, (RB, LN)) + jnp.exp(zcol_ref[rs, :] - mcol_ref[rs, :])


HR = SR // 2


def merge_stats(parts):
    m = functools.reduce(jnp.maximum, [p[:HR] for p in parts])
    s = sum(p[HR:2 * HR] * jnp.exp(p[:HR] - m) for p in parts)
    return m, s, sum(p[2 * HR:] for p in parts)


def put_stats(ref, parts):
    m, s, t = merge_stats(parts)
    ref[:HR, :] = m
    ref[HR:2 * HR, :] = s
    ref[2 * HR:, :] = t


def reduce_stats(mr, sr, zr, lr, b0, bc, b1, bs, b2, bz, fin, sems, fill):
    z, y, x, c, v, a = coords()
    to_c, to_z, to_1, to_2 = peers()
    sc, rc, s1, r1, ss, rs, s2, r2, sz, rz, sf, rf = sems

    def step(copies, lo=0, hi=0):
        for cp in copies:
            cp.start()
        if hi:
            fill(lo, hi)
        for cp in copies:
            cp.wait()
    for hf in range(2):
        hs = slice(hf * HR, (hf + 1) * HR)
        zz = zr[hs, :]
        zz = jnp.where(zz > NEG, zz, 0.0)
        b0[hf, :HR, :] = mr[hs, :]
        b0[hf, HR:2 * HR, :] = sr[hs, :]
        b0[hf, 2 * HR:, :] = zz[:8] + zz[8:]
    step([rcopy(b0.at[1 - c], bc, sc, rc, to_c)])
    here, there = b0[c], bc[...]
    even = c == 0
    put_stats(b1.at[a], [jnp.where(even, here, there), jnp.where(even, there, here)])
    step([rcopy(b1.at[a], b1.at[a], s1.at[k], r1.at[k], to_2(k)) for k in NEAR], 0, 2)
    put_stats(b0.at[c], [b1[i] for i in range(NA)])
    step([rcopy(b0.at[c], bs, ss, rs, to_c)])
    b2[a] = bs[...]
    step([rcopy(bs, b2.at[a], s2.at[k], r2.at[k], to_2(k)) for k in NEAR], 2, 5)
    put_stats(bz.at[z], [b2[i] for i in range(NA)])
    step([rcopy(bz.at[z], bz.at[z], sz.at[k - 1], rz.at[k - 1], to_z(k)) for k in range(1, NZ)], 5, NC)
    m, s, t = merge_stats([bz[i] for i in range(NZ)])
    fin[1 - c, :HR, :] = m + jnp.log(s)
    fin[1 - c, HR:, :] = t
    step([rcopy(fin.at[1 - c], fin.at[1 - c], sf, rf, to_c)])
    tot = fin[0, :HR, :] + fin[1, :HR, :]
    tot = tot[:8] + tot[8:] - (fin[0, HR:, :] + fin[1, HR:, :])
    lr[:HR, :] = fin[0, :HR, :]
    lr[HR:, :] = fin[1, :HR, :]
    return jnp.sum(tot) * (1.0 / NT)


def gelu_both(u):
    k0, k1 = math.sqrt(2.0 / math.pi), 0.044715
    sq = u * u
    t = jnp.tanh(k0 * (u + k1 * (sq * u)))
    cdf = 0.5 * (1.0 + t)
    return u * cdf, cdf + (0.5 * k0) * u * ((1.0 - t * t) * (1.0 + (3.0 * k1) * sq))


def step_kernel(x_hbm, win_hbm, wout_hbm, emb_hbm, cid_hbm, lq_hbm, y_s,
                loss_ref, de_hbm, gwi_hbm, gwo_hbm, h_hbm, yl_out, l_out, z_out, xg,
                xv, win, wout, emb, cid_v, lq_v, lqr, hb, yb, dh,
                eb, pb, de, te, dcol, mcol, zcol, scol, mr, sr, zr, yl,
                b0, bc, b1, bs, b2, bz, fin,
                dq, rc, a0, ra, a1, rb, zb,
                lsem, osem, fsem, xsem, *sems):
    z, y, x, c, v, a = coords()
    to_c, to_z, to_1, to_2 = peers()
    rows = emb.shape[0]
    hid = win.shape[1]
    half = hid // 2
    me = lax.axis_index("dp")
    base = me * rows
    gh, gy, gx, gd, sems = sems[:8], sems[8:16], sems[16:24], sems[24:32], sems[32:]
    own16 = pl.ds(me * TD, TD)
    loads = [pltpu.make_async_copy(s, d, lsem.at[i]) for i, (s, d) in enumerate((
        (x_hbm, xv), (win_hbm, win), (wout_hbm, wout), (emb_hbm, emb), (cid_hbm.at[own16], cid_v), (lq_hbm.at[own16], lq_v)))]
    for cp in loads:
        cp.start()
    bar, n_peers = signal_peers()

    for cp in loads[:3]:
        cp.wait()
    pre = jnp.dot(xv[...], win[...], preferred_element_type=F32)
    act = gelu_both(pre)[0].astype(BF16)
    hb[c, v, z, a] = jnp.dot(act, wout[...], preferred_element_type=F32).astype(BF16)
    lane16 = lax.broadcasted_iota(jnp.int32, (1, LN), 1) % TD
    yb[c, v, z, a] = sum(jnp.where(lane16 == i, y_s[i], 0) for i in range(TD))
    xown = pltpu.make_async_copy(xv, xg.at[c, v, z, a], xsem.at[0])
    xown.start()
    pl.semaphore_wait(bar, n_peers)

    gath, gaty, gatx, gatd = Gather(hb, gh), Gather(yb, gy), Gather(xg, gx, xv), Gather(dh, gd)
    gath.start()
    gaty.start()
    gatx.start()
    for cp in loads[3:]:
        cp.wait()
    logq_rows(cid_v, lq_v, lqr, base)
    de[...] = jnp.zeros_like(de)
    for g in (gath, gaty):
        g.second()
    for g in (gath, gaty):
        g.first()
    xown.wait()
    gatx.second()

    def score(cc, vv):
        ci = cc * NA + vv
        target_cols(lambda b: yb[cc, vv, b // NA, b % NA], base, yl, ci * GR, dcol.at[ci])
        scores_chunk(hb[cc, vv].reshape(CH, 2 * LN), emb, lqr, eb.at[ci], dcol.at[ci], mcol.at[ci], zcol.at[ci], scol)
        for b in range(GR):
            bs_ = slice(b * LN, (b + 1) * LN)
            row = pl.ds(ci * GR + b, 1)
            mr[row, :] = jnp.transpose(mcol[ci, bs_, :])[:1]
            sr[row, :] = jnp.transpose(scol[bs_, :])[:1]
            zr[row, :] = jnp.transpose(zcol[ci, bs_, :])[:1]

    @pl.loop(0, NC)
    def _(n):
        gaty.take(n)
        score(*gath.take(n))
        pl.when(n == NA - 1)(gatx.first)

    def target_rows(lo, hi):
        @pl.loop(lo, hi)
        def _(ci):
            for q in range(0, rows, LN):
                pb[:, q:q + LN] = jnp.where(dcol[ci] == float(q), 1.0, 0.0).astype(BF16)
            te[ci] = jnp.dot(pb[...], emb[...], preferred_element_type=F32).astype(BF16)

    lr = l_out
    loss_ref[0, 0] = reduce_stats(mr, sr, zr, lr, b0, bc, b1, bs, b2, bz, fin, sems[:12], target_rows)
    @pl.loop(0, NC)
    def _(ci):
        for b in range(GR):
            bs_ = slice(b * LN, (b + 1) * LN)
            lc = to_col(lr[pl.ds(ci * GR + b, 1), :])
            mcol[ci, bs_, :] = jnp.exp(mcol[ci, bs_, :] - lc) * (1.0 / NT)
            zc = zcol[ci, bs_, :]
            zcol[ci, bs_, :] = jnp.where(zc > NEG, (jnp.exp(zc - lc) - 1.0) * (1.0 / NT), 0.0)
    yl_out[...] = yl[...]
    z_out[...] = zr[...]

    sc, rcs, sa, ras, sb, rbs, sz, rzs = sems[12:20]
    ring = a0.shape[0]
    c_copy = lambda k: rcopy(dq.at[k % 2, 1 - c], rc.at[k], sc.at[k], rcs.at[k], to_c)
    a_copy = lambda k, j: rcopy(a0.at[k % ring, (v + j) % NA], ra.at[k, v], sa.at[k, j], ras.at[k, j], to_1(j))
    b_copy = lambda k, j: rcopy(a1.at[k % ring, (a + j) % NA], rb.at[k, a], sb.at[k, j], rbs.at[k, j], to_2(j))

    def off(k):
        s = (k + 1) // 2
        return NA + s - 2 * s * (k % 2)

    z_copy = lambda k: rcopy(zb.at[NZ + k], zb.at[z], sz.at[k], rzs.at[k], to_z(off(k)))

    def compute(k):
        zz = (z + off(k)) % NZ
        piece = pl.ds(pl.multiple_of(zz * PZ, PZ), PZ)
        for ci in range(NC):
            ps = slice(ci * PZ, (ci + 1) * PZ)
            f = mcol[ci, piece, :]
            for q in range(0, rows, LN):
                pb[ps, q:q + LN] = (eb[ci, piece, q:q + LN] * f).astype(BF16)
        h = jnp.concatenate([hb[ci // NA, ci % NA, zz].reshape(PZ, 2 * LN) for ci in range(NC)], axis=0)
        for q in range(0, rows, CH):
            de[q:q + CH, :] += lax.dot_general(pb[:, q:q + CH], h, (((0,), (0,)), ((), ())), preferred_element_type=F32)
        out = jnp.dot(pb[...], emb[...], preferred_element_type=F32)
        for ci in range(NC):
            g = zcol[ci, piece, :]
            t = te[ci, piece, :].astype(F32)
            for hf in (0, LN):
                dq[k % 2, ci // NA, ci % NA, :, hf:hf + LN] = out[ci * PZ:(ci + 1) * PZ, hf:hf + LN] + g * t[:, hf:hf + LN]
        c_copy(k).start()

    def sum_core(k):
        c_copy(k).wait()
        a0[k % ring] = dq[k % 2, c] + rc[k]
        for j in NEAR:
            a_copy(k, j).start()

    def sum_first(k):
        for j in NEAR:
            a_copy(k, j).wait()
        ra[k, v] = a0[k % ring, v]
        a1[k % ring] = ((ra[k, 0] + ra[k, 1]) + (ra[k, 2] + ra[k, 3])).reshape(NA, TD, 2 * LN)
        for j in NEAR:
            b_copy(k, j).start()

    def sum_second(k, last=False):
        for j in NEAR:
            b_copy(k, j).wait()
        rb[k, a] = a1[k % ring, a]
        val = (rb[k, 0] + rb[k, 1]) + (rb[k, 2] + rb[k, 3])
        if last:
            zb[z] = val
        else:
            zb[NZ + k] = val
            z_copy(k).start()

    def body(k, _):
        compute(k)
        for lag, f in ((1, sum_core), (3, sum_first), (5, sum_second)):
            pl.when(k >= lag)(functools.partial(f, k - lag))
        return 0

    lax.fori_loop(0, NZ, body, 0)
    outs = [pltpu.make_async_copy(de, de_hbm, osem.at[0]), pltpu.make_async_copy(hb, h_hbm, osem.at[1])]
    for cp in outs:
        cp.start()

    cols = pl.ds(pl.multiple_of(c * half, half), half)
    xs = lambda ci, slot: pltpu.make_async_copy(xg.at[ci // NA, ci % NA].reshape(CH, hid), pb.at[:, pl.ds(pl.multiple_of(slot * hid, hid), hid)], fsem.at[slot])

    def tower(ci, slot):
        pre = jnp.dot(pb[:, pl.ds(pl.multiple_of(slot * hid, hid), hid)], win[:, cols], preferred_element_type=F32)
        act, der = gelu_both(pre)
        eb[ci, :, :half] = der
        eb[ci, :, half:2 * half] = act.astype(BF16).astype(F32)

    sum_core(7)
    sum_first(5)
    sum_second(3)
    sum_first(6)
    sum_second(4)
    sum_second(5)
    sum_first(7)
    sum_second(6)
    sum_second(7, last=True)
    for k in range(NZ - 1):
        z_copy(k).wait()
    tot = ((zb[0] + zb[1]) + (zb[2] + zb[3])) + ((zb[4] + zb[5]) + (zb[6] + zb[7]))
    dh[c, v, z, a] = tot.astype(BF16)
    gatd.start()
    pl.loop(0, NC)(lambda n: gatx.take(n) and None)
    xs(0, 0).start()

    def towers(lo, hi):
        @pl.loop(lo, hi)
        def _(ci):
            @pl.when(ci + 1 < NC)
            def _():
                xs(ci + 1, (ci + 1) % 2).start()
            xs(ci, ci % 2).wait()
            tower(ci, ci % 2)

    towers(0, 3)
    gatd.second()
    towers(3, 5)
    gatd.first()
    towers(5, NC)

    acc_i, acc_o = eb.at[pl.ds(0, 2), :, pl.ds(2 * half, half)], eb.at[2, :, pl.ds(2 * half, 2 * LN)]
    acc_i[...] = jnp.zeros(acc_i.shape, F32)
    acc_o[...] = jnp.zeros(acc_o.shape, F32)

    def weights(ci, slot):
        g = dh[ci // NA, ci % NA].reshape(CH, 2 * LN)
        back = lax.dot_general(g, wout[cols, :], (((1,), (1,)), ((), ())), preferred_element_type=F32)
        da = (eb[ci, :, :half] * back).astype(BF16)
        act = eb[ci, :, half:2 * half].astype(BF16)
        acc_o[...] += lax.dot_general(act, g, (((0,), (0,)), ((), ())), preferred_element_type=F32)
        for r in range(2):
            xr = pb[:, pl.ds(pl.multiple_of(slot * hid + r * half, half), half)]
            acc_i[r] += lax.dot_general(xr, da, (((0,), (0,)), ((), ())), preferred_element_type=F32)

    @pl.loop(0, NC)
    def _(n):
        cc, vv = gatd.take(n)
        cp = xs(cc * NA + vv, n % 2)
        cp.start()
        cp.wait()
        weights(cc * NA + vv, n % 2)

    so, ro = sems[20:22]
    mine = [(acc_i.at[r], gwi_hbm.at[pl.ds(r * half, half), cols]) for r in range(2)] + [(acc_o, gwo_hbm.at[cols])]
    ends = [rcopy(s, d, so.at[i], ro.at[i], to_c) for i, (s, d) in enumerate(mine)]
    outs += [pltpu.make_async_copy(s, d, osem.at[2 + i]) for i, (s, d) in enumerate(mine)]
    for cp in ends + outs[2:]:
        cp.start()
    for cp in ends + outs:
        cp.wait()


def step(features, w_in, w_out, table, cand_ids, log_q, targets):
    rows, dim = table.shape
    hid = w_in.shape[1]
    V, A, S = (pl.BlockSpec(memory_space=m) for m in (pltpu.VMEM, pl.ANY, pltpu.SMEM))
    sds = jax.ShapeDtypeStruct
    vm = pltpu.VMEM
    tokens = (2, NA, NZ, NA, TD)
    stat = lambda *n: vm(n + (2 * HR + 8, LN), F32)
    col = vm((NC, CH, LN), F32)
    row = vm((SR, LN), F32)
    return pl.pallas_call(
        step_kernel, name="step",
        out_shape=(sds((1, 1), F32), sds((rows, dim), F32), sds((w_in.shape[0], hid), F32), sds((hid, dim), F32), sds(tokens + (dim,), BF16),
                   sds((SR, LN), jnp.int32), sds((SR, LN), F32), sds((SR, LN), F32), sds(tokens + (w_in.shape[0],), BF16)),
        in_specs=[A] * 6 + [S], out_specs=(S, A, A, A, A, V, V, V, A),
        scratch_shapes=[
            vm(features.shape, BF16), vm(w_in.shape, BF16), vm(w_out.shape, BF16), vm(table.shape, BF16), vm((TD, LN), jnp.int32), vm((TD, LN), F32),
            vm((8, rows), F32), vm(tokens + (dim,), BF16), vm((2, NA, NZ, NA, 1, LN), jnp.int32), vm(tokens + (dim,), BF16),
            vm((NC, CH, rows), F32), vm((CH, rows), BF16), vm((rows, dim), F32), vm((NC, CH, dim), BF16), col, col, col, vm((CH, LN), F32),
            row, row, row, vm((SR, LN), jnp.int32),
            stat(2), stat(), stat(NA), stat(), stat(NA), stat(NZ), vm((2, HR + 8, LN), F32),
            vm((2, 2, NA, PZ, dim), F32), vm((NZ, NA, PZ, dim), F32), vm((4, NA, PZ, dim), F32), vm((NZ, NA, PZ, dim), F32),
            vm((4, NA, TD, dim), F32), vm((NZ, NA, TD, dim), F32), vm((2 * NZ, TD, dim), F32),
            DMA((6,)), DMA((5,)), DMA((2,)), DMA((1,))] + Gather.SEMS * 4 + [
            DMA, DMA, DMA((NA,)), DMA((NA,)), DMA, DMA, DMA((NA,)), DMA((NA,)), DMA((NZ - 1,)), DMA((NZ - 1,)), DMA, DMA,
            DMA((NZ,)), DMA((NZ,)), DMA((NZ, NA)), DMA((NZ, NA)), DMA((NZ, NA)), DMA((NZ, NA)), DMA((NZ,)), DMA((NZ,)),
            DMA((3,)), DMA((3,))],
        compiler_params=pltpu.CompilerParams(collective_id=0, has_side_effects=True, vmem_limit_bytes=67043328),
    )(features, w_in, w_out, table, cand_ids.reshape(-1, LN), log_q.reshape(-1, LN), targets)


def fix_kernel(de_ref, h_ref, yl_ref, l_ref, z_ref, out_ref, lst_i, lst_g, si, sg, sem):
    rows = out_ref.shape[0]
    out_ref[...] = de_ref[...]
    yl = yl_ref[...]
    own = (yl >= 0) & (yl < rows)
    g = jnp.where(own, (jnp.exp(jnp.where(own, z_ref[...], 0.0) - l_ref[...]) - 1.0) * (1.0 / NT), 0.0)
    of = jnp.where(own, 1.0, 0.0)
    before = lambda n, i, j: jnp.where(lax.broadcasted_iota(jnp.int32, (n, n), i) < lax.broadcasted_iota(jnp.int32, (n, n), j), 1.0, 0.0).astype(BF16)
    pre = jnp.dot(of.astype(BF16), before(LN, 0, 1), preferred_element_type=F32)
    tot = jnp.broadcast_to(jnp.sum(of, axis=1, keepdims=True), (SR, LN))
    rank = jnp.where(own, pre + jnp.dot(before(SR, 1, 0), tot.astype(BF16), preferred_element_type=F32), -1.0)
    n = jnp.sum(of).astype(jnp.int32)
    lane = lax.broadcasted_iota(jnp.int32, (1, LN), 1)

    def page(p, _):
        slot = (lax.broadcasted_iota(jnp.int32, (LN, LN), 0) + p * LN).astype(F32)
        rr, tt, gg = (jnp.zeros((LN, LN), F32) for _ in range(3))
        for r in range(SR):
            rw = slice(r, r + 1)
            hit = rank[rw] == slot
            rr += jnp.where(hit, yl[rw].astype(F32), 0.0)
            tt += jnp.where(hit, (lane + r * LN).astype(F32), 0.0)
            gg += jnp.where(hit, g[rw], 0.0)
        row = lambda m: jnp.transpose(jnp.broadcast_to(jnp.sum(m, axis=1, keepdims=True), (LN, LN)))[:8]
        lst_i[0] = row(rr).astype(jnp.int32)
        lst_i[1] = row(tt).astype(jnp.int32)
        lst_g[...] = row(gg)
        run([pltpu.make_async_copy(lst_i, si, sem.at[0]), pltpu.make_async_copy(lst_g, sg, sem.at[1])])

        def one(i, _):
            r, t, gv = si[0, 0, i], si[1, 0, i], sg[0, i]
            blk, w = t // TD, t % TD
            ht = h_ref[blk // (NA * NZ * NA), (blk // (NZ * NA)) % NA, (blk // NA) % NZ, blk % NA].astype(F32)
            hr = jnp.sum(jnp.where(lax.broadcasted_iota(jnp.int32, (TD, 1), 0) == w, ht, 0.0), axis=0, keepdims=True)
            out_ref[pl.ds(r, 1), :] += gv * hr
            return 0
        lax.fori_loop(0, jnp.minimum(n - p * LN, LN), one, 0)
        return 0
    lax.fori_loop(0, (n + LN - 1) // LN, page, 0)


def fix(de, h, yl, lr, zr):
    V = pl.BlockSpec(memory_space=pltpu.VMEM)
    return pl.pallas_call(
        fix_kernel, name="fix", out_shape=jax.ShapeDtypeStruct(de.shape, F32), in_specs=[V] * 5, out_specs=V,
        scratch_shapes=[pltpu.VMEM((2, 8, LN), jnp.int32), pltpu.VMEM((8, LN), F32), pltpu.SMEM((2, 8, LN), jnp.int32),
                        pltpu.SMEM((8, LN), F32), DMA((2,))],
        compiler_params=pltpu.CompilerParams(vmem_limit_bytes=20 << 20),
    )(de, h, yl, lr, zr)


def solution(mesh):
    def local_step(*args):
        loss, de, gwi, gwo, h, yl, lr, zr, _ = step(*args)
        return loss.reshape(()), fix(de, h, yl, lr, zr), gwi, gwo

    return jax.shard_map(local_step, mesh=mesh, in_specs=(P("dp", None), P(), P(), P("dp", None), P(), P(), P("dp")), out_specs=(P(), P("dp", None), P(), P()), check_vma=False)
```

```python
import functools
import math
import jax
import jax.numpy as jnp
from jax import lax
from jax.experimental import pallas as pl
from jax.experimental.pallas import tpu as pltpu
from jax.sharding import PartitionSpec as P

NZ, NY, NX = 8, 4, 4
NA = 4
LN = 128
TD = 16
NC = 2 * NA
CH = NZ * NA * TD
NT = NC * CH
PZ = NA * TD
SR = NT // LN
GR = CH // LN
F32, BF16 = jnp.float32, jnp.bfloat16
NEG = -jnp.inf
VMEM_ALL = 67043328
MESH = pl.DeviceIdType.MESH
DMA = pltpu.SemaphoreType.DMA


def coords():
    me = lax.axis_index("dp")
    z, y, x, c = me // (NY * NX * 2), (me // (NX * 2)) % NY, (me // 2) % NX, me % 2
    return z, y, x, c, x * (1 - c) + y * c, y * (1 - c) + x * c


def dev(z, y, x, c):
    return (((z * NY + y) * NX + x) * 2 + c,)


def peers():
    z, y, x, c, v, a = coords()
    return (dev(z, y, x, 1 - c), lambda k: dev((z + k) % NZ, y, x, c), lambda k: dev(z, (y + k * c) % NY, (x + k * (1 - c)) % NX, c),
            lambda k: dev(z, (y + k * (1 - c)) % NY, (x + k * c) % NX, c))


def rcopy(src, dst, ssem, rsem, to):
    return pltpu.make_async_remote_copy(src_ref=src, dst_ref=dst, send_sem=ssem, recv_sem=rsem, device_id=to, device_id_type=MESH)


def run(copies):
    for cp in copies:
        cp.start()
    for cp in copies:
        cp.wait()


def signal_peers():
    bar = pltpu.get_barrier_semaphore()
    to_c, to_z, to_1, to_2 = peers()
    everyone = [to_c] + [to_1(k) for k in range(1, NA)] + [to_2(k) for k in range(1, NA)] + [to_z(k) for k in range(1, NZ)]
    for p in everyone:
        pl.semaphore_signal(bar, inc=1, device_id=p, device_id_type=MESH)
    return bar, len(everyone)


NEAR = (1, 3, 2)


class Gather:
    SEMS = [DMA] * 5 + [DMA((NA - 1,)), DMA, DMA((NA,))]

    def __init__(self, buf, sems, src=None):
        z, y, x, c, v, a = coords()
        sz, rz, s2, r2, s1, r1, sd, rd = sems
        to_c, to_z, to_1, to_2 = peers()
        self.c, self.v, self.a = c, v, a
        own = buf.at[c, v, z, a]
        col = lambda j: buf.at[c, v, :, (a + NA - j) % NA]
        chunk = lambda j: buf.at[c, (v + NA - j) % NA]
        self.zc = lambda k: rcopy(own if src is None else src, own, sz, rz, to_z(k))
        self.ac = lambda k: rcopy(col(0), col(0), s2, r2, to_2(k))
        self.vc = lambda k, p: rcopy(col(p), col(p), s1, r1.at[k - 1], to_1(k))
        self.dc = lambda j: rcopy(chunk(j), chunk(j), sd, rd.at[j], to_c)
        self.z_all = rcopy(buf.at[c, v, pl.ds(0, NZ - 1), a], buf.at[c, v, pl.ds(0, NZ - 1), a], sz, rz, to_c)
        self.a_all = rcopy(buf.at[c, v, :, pl.ds(0, NA - 1)], buf.at[c, v, :, pl.ds(0, NA - 1)], s2, r2, to_c)
        self.v_one = lambda k: rcopy(chunk(k), chunk(k), s1, r1.at[k - 1], to_c)
        self.d_all = rcopy(buf.at[c], buf.at[c], sd, rd.at[0], to_c)

    def start(self):
        @pl.loop(1, NZ)
        def _(k):
            self.zc(k).start()

    def second(self):
        self.z_all.wait()
        for k in NEAR:
            self.ac(k).start()

    def first(self):
        for k in NEAR:
            self.vc(k, 0).start()
        self.a_all.wait()
        for j in NEAR:
            for k in NEAR:
                self.vc(k, j).start()
        self.dc(0).start()

    def finish(self):
        for k in NEAR:
            self.v_one(k).wait_send()
        self.d_all.wait_send()

    def place(self, n):
        i, p = n // 2, n % 2
        j = i + (i // 2) * (1 - 2 * (i % 2))
        return i, p, j, (self.c + p * (1 - 2 * self.c), (self.v * (1 - p) + self.a * p + NA - j) % NA)

    def hand(self, i):
        j = self.place(2 * i)[2]
        self.v_one(j).wait_recv()
        self.dc(j).start()

    def take(self, n, hand=True):
        i, p, j, cv = self.place(n)
        if hand:
            pl.when((p == 0) & (i > 0))(lambda: self.hand(i))
        pl.when(p == 1)(lambda: self.dc(j).wait_recv())
        return cv


def to_col(row):
    return jnp.transpose(jnp.broadcast_to(row, (LN, LN)))


def logq_rows(cid_v, lq_v, lqr_ref, base):
    @pl.loop(0, lqr_ref.shape[1] // LN)
    def _(i):
        blk = pl.multiple_of(i * LN, LN)
        rid = lax.broadcasted_iota(jnp.int32, (LN, LN), 0) + (base + blk)
        acc = jnp.zeros((LN, LN), F32)
        for q in range(cid_v.shape[0]):
            acc += jnp.where(cid_v[q:q + 1, :] == rid, lq_v[q:q + 1, :], 0.0)
        lqr_ref[:, pl.ds(blk, LN)] = jnp.transpose(jnp.broadcast_to(jnp.sum(acc, axis=1, keepdims=True), (LN, LN)))[:8]


def target_cols(yblk, base, yl_ref, row, d_ref):
    lane = lax.broadcasted_iota(jnp.int32, (LN, LN), 1).astype(F32)
    group = lax.broadcasted_iota(jnp.int32, (1, LN), 1) // TD
    for g in range(GR):
        yr = sum(jnp.where(group == b, yblk(g * 8 + b), 0) for b in range(8)) - base
        yl_ref[pl.ds(row + g, 1), :] = yr
        d_ref[g * LN:(g + 1) * LN, :] = to_col(yr.astype(F32)) - lane


def scores_chunk(h, emb_ref, lqr_ref, e_ref, d_ref, mcol_ref, zcol_ref, scol_ref):
    rows = emb_ref.shape[0]
    RB = PZ
    for j in range(0, rows, 2 * LN):
        s = lax.dot_general(h, emb_ref[j:j + 2 * LN, :], (((1,), (1,)), ((), ())), preferred_element_type=F32)
        for rb in range(0, CH, RB):
            rs = slice(rb, rb + RB)
            m = mcol_ref[rs, :] if j else jnp.full((RB, LN), NEG, F32)
            zc = zcol_ref[rs, :] if j else jnp.full((RB, LN), NEG, F32)
            d = d_ref[rs, :]
            for k in (0, LN):
                raw = s[rs, k:k + LN]
                hit = d == float(j + k)
                zc = jnp.where(hit, raw, zc)
                val = jnp.where(hit, -1e9, raw - lqr_ref[:1, j + k:j + k + LN])
                e_ref[rs, j + k:j + k + LN] = val
                m = jnp.maximum(m, val)
            mcol_ref[rs, :] = m
            zcol_ref[rs, :] = zc
    for rb in range(0, CH, RB):
        rs = slice(rb, rb + RB)
        zc = jnp.max(zcol_ref[rs, :], axis=1, keepdims=True)
        m = jnp.maximum(jnp.max(mcol_ref[rs, :], axis=1, keepdims=True), zc)
        zcol_ref[rs, :] = jnp.broadcast_to(zc, (RB, LN))
        mcol_ref[rs, :] = jnp.broadcast_to(m, (RB, LN))

    def grp(g, _):
        rs = pl.ds(pl.multiple_of(g * 2 * TD, 2 * TD), 2 * TD)
        m = mcol_ref[rs, :]
        tot = jnp.zeros((2 * TD, LN), F32)
        for k in range(0, rows, LN):
            ex = jnp.exp(e_ref[rs, k:k + LN] - m)
            e_ref[rs, k:k + LN] = ex
            tot += ex
        scol_ref[rs, :] = tot
        return 0
    lax.fori_loop(0, CH // (2 * TD), grp, 0)
    for rb in range(0, CH, RB):
        rs = slice(rb, rb + RB)
        tot = jnp.sum(scol_ref[rs, :], axis=1, keepdims=True)
        scol_ref[rs, :] = jnp.broadcast_to(tot, (RB, LN)) + jnp.exp(zcol_ref[rs, :] - mcol_ref[rs, :])


HR = SR // 2


def merge_stats(parts):
    m = functools.reduce(jnp.maximum, [p[:HR] for p in parts])
    s = sum(p[HR:2 * HR] * jnp.exp(p[:HR] - m) for p in parts)
    return m, s, sum(p[2 * HR:] for p in parts)


def put_stats(ref, parts):
    m, s, t = merge_stats(parts)
    ref[:HR, :] = m
    ref[HR:2 * HR, :] = s
    ref[2 * HR:, :] = t


def reduce_stats(mr, sr, zr, lr, b0, bc, b1, bs, b2, bz, fin, sems, fill):
    z, y, x, c, v, a = coords()
    to_c, to_z, to_1, to_2 = peers()
    sc, rc, s1, r1, ss, rs, s2, r2, sz, rz, sf, rf = sems

    all3 = lambda b, ss_, rs_: rcopy(b.at[pl.ds(0, NA - 1)], b.at[pl.ds(0, NA - 1)], ss_, rs_, to_c)

    def step(copies, lo=0, hi=0, every=None):
        for cp in copies:
            cp.start()
        if hi:
            fill(lo, hi)
        for cp in copies if every is None else [every]:
            cp.wait()
    for hf in range(2):
        hs = slice(hf * HR, (hf + 1) * HR)
        zz = zr[hs, :]
        zz = jnp.where(zz > NEG, zz, 0.0)
        b0[hf, :HR, :] = mr[hs, :]
        b0[hf, HR:2 * HR, :] = sr[hs, :]
        b0[hf, 2 * HR:, :] = zz[:8] + zz[8:]
    step([rcopy(b0.at[1 - c], bc, sc, rc, to_c)])
    here, there = b0[c], bc[...]
    even = c == 0
    put_stats(b1.at[a], [jnp.where(even, here, there), jnp.where(even, there, here)])
    step([rcopy(b1.at[a], b1.at[a], s1, r1, to_2(k)) for k in NEAR], 0, 2, all3(b1, s1, r1))
    put_stats(b0.at[c], [b1[i] for i in range(NA)])
    step([rcopy(b0.at[c], bs, ss, rs, to_c)])
    b2[a] = bs[...]
    step([rcopy(bs, b2.at[a], s2, r2, to_2(k)) for k in NEAR], 2, 5, all3(b2, s2, r2))
    put_stats(bz.at[z], [b2[i] for i in range(NA)])
    step([rcopy(bz.at[z], bz.at[z], sz, rz, to_z(k)) for k in range(1, NZ)], 5, NC, rcopy(bz.at[pl.ds(0, NZ - 1)], bz.at[pl.ds(0, NZ - 1)], sz, rz, to_c))
    m, s, t = merge_stats([bz[i] for i in range(NZ)])
    fin[1 - c, :HR, :] = m + jnp.log(s)
    fin[1 - c, HR:, :] = t
    step([rcopy(fin.at[1 - c], fin.at[1 - c], sf, rf, to_c)])
    tot = fin[0, :HR, :] + fin[1, :HR, :]
    tot = tot[:8] + tot[8:] - (fin[0, HR:, :] + fin[1, HR:, :])
    lr[:HR, :] = fin[0, :HR, :]
    lr[HR:, :] = fin[1, :HR, :]
    return jnp.sum(tot) * (1.0 / NT)


def gelu_both(u):
    k0, k1 = math.sqrt(2.0 / math.pi), 0.044715
    sq = u * u
    t = jnp.tanh(k0 * (u + k1 * (sq * u)))
    cdf = 0.5 * (1.0 + t)
    return u * cdf, cdf + (0.5 * k0) * u * ((1.0 - t * t) * (1.0 + (3.0 * k1) * sq))


def step_kernel(x_hbm, win_hbm, wout_hbm, emb_hbm, cid_hbm, lq_hbm, y_s,
                loss_ref, de_hbm, gwi_hbm, gwo_hbm, h_hbm, st_hbm, lh_hbm, li_hbm, lg_hbm, xg,
                xv, win, wout, emb, cid_v, lq_v, lqr, hb, yb, dh,
                eb, pb, de, te, dcol, mcol, zcol, scol, mr, sr, zr, yl, st, lh, li, lg,
                b0, bc, b1, bs, b2, bz, fin,
                dq, rc, a0, ra, a1, rb, zb,
                lsem, osem, fsem, xsem, *sems):
    z, y, x, c, v, a = coords()
    to_c, to_z, to_1, to_2 = peers()
    rows = emb.shape[0]
    hid = win.shape[1]
    half = hid // 2
    me = lax.axis_index("dp")
    base = me * rows
    gh, gy, gx, gd, sems = sems[:8], sems[8:16], sems[16:24], sems[24:32], sems[32:]
    own16 = pl.ds(me * TD, TD)
    loads = [pltpu.make_async_copy(s, d, lsem.at[i]) for i, (s, d) in enumerate((
        (x_hbm, xv), (win_hbm, win), (wout_hbm, wout), (emb_hbm, emb), (cid_hbm.at[own16], cid_v), (lq_hbm.at[own16], lq_v)))]
    for cp in loads:
        cp.start()
    bar, n_peers = signal_peers()

    for cp in loads[:3]:
        cp.wait()
    pre = jnp.dot(xv[...], win[...], preferred_element_type=F32)
    act = gelu_both(pre)[0].astype(BF16)
    hb[c, v, z, a] = jnp.dot(act, wout[...], preferred_element_type=F32).astype(BF16)
    lane16 = lax.broadcasted_iota(jnp.int32, (1, LN), 1) % TD
    yb[c, v, z, a] = sum(jnp.where(lane16 == i, y_s[i], 0) for i in range(TD))
    xown = pltpu.make_async_copy(xv, xg.at[c, v, z, a], xsem.at[0])
    xown.start()
    pl.semaphore_wait(bar, n_peers)

    gath, gaty, gatx, gatd = Gather(hb, gh), Gather(yb, gy), Gather(xg, gx, xv), Gather(dh, gd)
    gath.start()
    gaty.start()
    for cp in loads[3:]:
        cp.wait()
    logq_rows(cid_v, lq_v, lqr, base)
    de[...] = jnp.zeros_like(de)
    for g in (gath, gaty):
        g.second()
    xown.wait()
    gatx.start()
    for g in (gath, gaty):
        g.first()
    def score(cc, vv):
        ci = cc * NA + vv
        target_cols(lambda b: yb[cc, vv, b // NA, b % NA], base, yl, ci * GR, dcol.at[ci])
        scores_chunk(hb[cc, vv].reshape(CH, 2 * LN), emb, lqr, eb.at[ci], dcol.at[ci], mcol.at[ci], zcol.at[ci], scol)
        for b in range(GR):
            bs_ = slice(b * LN, (b + 1) * LN)
            row = pl.ds(ci * GR + b, 1)
            mr[row, :] = jnp.transpose(mcol[ci, bs_, :])[:1]
            sr[row, :] = jnp.transpose(scol[bs_, :])[:1]
            zr[row, :] = jnp.transpose(zcol[ci, bs_, :])[:1]

    @pl.loop(0, NC)
    def _(n):
        gaty.take(n)
        cv = gath.take(n)
        score(*cv)
        pl.when(n == NA - 1)(gatx.second)
        pl.when(n == NC - 1)(gatx.first)

    def target_rows(lo, hi):
        @pl.loop(lo, hi)
        def _(ci):
            for q in range(0, rows, LN):
                pb[:, q:q + LN] = jnp.where(dcol[ci] == float(q), 1.0, 0.0).astype(BF16)
            te[ci] = jnp.dot(pb[...], emb[...], preferred_element_type=F32).astype(BF16)

    lr = st.at[1]
    loss_ref[0, 0] = reduce_stats(mr, sr, zr, lr, b0, bc, b1, bs, b2, bz, fin, sems[:12], target_rows)
    @pl.loop(0, NC)
    def _(ci):
        for b in range(GR):
            bs_ = slice(b * LN, (b + 1) * LN)
            lc = to_col(lr[pl.ds(ci * GR + b, 1), :])
            mcol[ci, bs_, :] = jnp.exp(mcol[ci, bs_, :] - lc) * (1.0 / NT)
            zc = zcol[ci, bs_, :]
            zcol[ci, bs_, :] = jnp.where(zc > NEG, (jnp.exp(zc - lc) - 1.0) * (1.0 / NT), 0.0)
    st[0] = yl[...].astype(F32)
    st[2] = zr[...]

    sc, rcs, sa, ras, sb, rbs, sz, rzs = sems[12:20]
    ring = a0.shape[0]
    c_copy = lambda k: rcopy(dq.at[k % 2, 1 - c], rc.at[k], sc.at[k % 2], rcs.at[k], to_c)
    a_copy = lambda k, j: rcopy(a0.at[k % ring, (v + j) % NA], ra.at[k, v], sa.at[k % ring], ras.at[k], to_1(j))
    a_all = lambda k: rcopy(ra.at[k, pl.ds(0, NA - 1)], ra.at[k, pl.ds(0, NA - 1)], sa.at[k % ring], ras.at[k], to_c)
    b_copy = lambda k, j: rcopy(a1.at[k % ring, (a + j) % NA], rb.at[k, a], sb.at[k % ring], rbs.at[k], to_2(j))
    b_all = lambda k: rcopy(rb.at[k, pl.ds(0, NA - 1)], rb.at[k, pl.ds(0, NA - 1)], sb.at[k % ring], rbs.at[k], to_c)

    def off(k):
        s = (k + 1) // 2
        return NA + s - 2 * s * (k % 2)

    z_copy = lambda k: rcopy(zb.at[NZ + k], zb.at[z], sz, rzs, to_z(off(k)))

    def compute(k):
        zz = (z + off(k)) % NZ
        piece = pl.ds(pl.multiple_of(zz * PZ, PZ), PZ)
        for ci in range(NC):
            ps = slice(ci * PZ, (ci + 1) * PZ)
            f = mcol[ci, piece, :]
            for q in range(0, rows, LN):
                pb[ps, q:q + LN] = (eb[ci, piece, q:q + LN] * f).astype(BF16)
        h = jnp.concatenate([hb[ci // NA, ci % NA, zz].reshape(PZ, 2 * LN) for ci in range(NC)], axis=0)
        for q in range(0, rows, CH):
            de[q:q + CH, :] += lax.dot_general(pb[:, q:q + CH], h, (((0,), (0,)), ((), ())), preferred_element_type=F32)
        out = jnp.dot(pb[...], emb[...], preferred_element_type=F32)
        for ci in range(NC):
            g = zcol[ci, piece, :]
            t = te[ci, piece, :].astype(F32)
            for hf in (0, LN):
                dq[k % 2, ci // NA, ci % NA, :, hf:hf + LN] = out[ci * PZ:(ci + 1) * PZ, hf:hf + LN] + g * t[:, hf:hf + LN]
        c_copy(k).start()

    def sum_core(k):
        c_copy(k).wait()
        a0[k % ring] = dq[k % 2, c] + rc[k]
        for j in NEAR:
            a_copy(k, j).start()

    def sum_first(k):
        a_all(k).wait()
        ra[k, v] = a0[k % ring, v]
        a1[k % ring] = ((ra[k, 0] + ra[k, 1]) + (ra[k, 2] + ra[k, 3])).reshape(NA, TD, 2 * LN)
        for j in NEAR:
            b_copy(k, j).start()

    def sum_second(k, last=False):
        b_all(k).wait()
        rb[k, a] = a1[k % ring, a]
        val = (rb[k, 0] + rb[k, 1]) + (rb[k, 2] + rb[k, 3])
        if last:
            zb[z] = val
        else:
            zb[NZ + k] = val
            z_copy(k).start()

    def body(k, _):
        compute(k)
        for lag, f in ((1, sum_core), (3, sum_first), (5, sum_second)):
            pl.when(k >= lag)(functools.partial(f, k - lag))
        pl.when(k >= NZ - NA + 1)(lambda: gatx.hand(k - (NZ - NA)))
        return 0

    lax.fori_loop(0, NZ, body, 0)
    outs = [pltpu.make_async_copy(s, d, osem.at[i]) for i, (s, d) in enumerate(((de, de_hbm), (hb, h_hbm), (st, st_hbm), (lh, lh_hbm), (li, li_hbm), (lg, lg_hbm)))]
    for cp in outs[:3]:
        cp.start()

    cols = pl.ds(pl.multiple_of(c * half, half), half)
    xs = lambda ci, slot: pltpu.make_async_copy(xg.at[ci // NA, ci % NA].reshape(CH, hid), pb.at[:, pl.ds(pl.multiple_of(slot * hid, hid), hid)], fsem.at[slot])

    def tower(ci, slot):
        pre = jnp.dot(pb[:, pl.ds(pl.multiple_of(slot * hid, hid), hid)], win[:, cols], preferred_element_type=F32)
        act, der = gelu_both(pre)
        eb[ci, :, :half] = der
        eb[ci, :, half:2 * half] = act.astype(BF16).astype(F32)

    ordinal = lambda n: gatx.place(n)[3][0] * NA + gatx.place(n)[3][1]

    def towers(lo, hi):
        @pl.loop(lo, hi)
        def _(n):
            @pl.when(n + 1 < NC)
            def _():
                gatx.take(n + 1, hand=False)
                xs(ordinal(n + 1), (n + 1) % 2).start()
            xs(ordinal(n), n % 2).wait()
            tower(ordinal(n), n % 2)

    xs(ordinal(0), 0).start()
    towers(0, 1)
    sum_core(7)
    sum_first(5)
    sum_second(3)
    towers(1, 2)
    sum_first(6)
    sum_second(4)
    sum_second(5)
    towers(2, 4)
    sum_first(7)
    sum_second(6)
    towers(4, 6)
    sum_second(7, last=True)
    rcopy(zb.at[pl.ds(0, NZ - 1)], zb.at[pl.ds(0, NZ - 1)], sz, rzs, to_c).wait()
    tot = ((zb[0] + zb[1]) + (zb[2] + zb[3])) + ((zb[4] + zb[5]) + (zb[6] + zb[7]))
    dh[c, v, z, a] = tot.astype(BF16)
    gatd.start()
    towers(6, NC)
    xs(ordinal(0), 0).start()
    gatd.second()
    rank, gfac, _ = target_ranks(st, rows)
    target_page(0, st, rank, gfac, lambda r: token_rows(hb, r), lh, li, lg)
    for cp in outs[3:6]:
        cp.start()
    gatd.first()
    acc_i, acc_o = eb.at[pl.ds(0, 2), :, pl.ds(2 * half, half)], eb.at[2, :, pl.ds(2 * half, 2 * LN)]
    acc_i[...] = jnp.zeros(acc_i.shape, F32)
    acc_o[...] = jnp.zeros(acc_o.shape, F32)

    def weights(ci, slot):
        g = dh[ci // NA, ci % NA].reshape(CH, 2 * LN)
        back = lax.dot_general(g, wout[cols, :], (((1,), (1,)), ((), ())), preferred_element_type=F32)
        da = (eb[ci, :, :half] * back).astype(BF16)
        act = eb[ci, :, half:2 * half].astype(BF16)
        acc_o[...] += lax.dot_general(act, g, (((0,), (0,)), ((), ())), preferred_element_type=F32)
        for r in range(2):
            xr = pb[:, pl.ds(pl.multiple_of(slot * hid + r * half, half), half)]
            acc_i[r] += lax.dot_general(xr, da, (((0,), (0,)), ((), ())), preferred_element_type=F32)

    @pl.loop(0, NC)
    def _(n):
        gatd.take(n)
        pl.when(n + 1 < NC)(lambda: xs(ordinal(n + 1), (n + 1) % 2).start())
        xs(ordinal(n), n % 2).wait()
        weights(ordinal(n), n % 2)

    for g in (gath, gaty, gatx, gatd):
        g.finish()
    so, ro = sems[20:22]
    mine = [(acc_i.at[r], gwi_hbm.at[pl.ds(r * half, half), cols]) for r in range(2)] + [(acc_o, gwo_hbm.at[cols])]
    ends = [rcopy(s, d, so.at[i], ro.at[i], to_c) for i, (s, d) in enumerate(mine)]
    outs += [pltpu.make_async_copy(s, d, osem.at[6 + i]) for i, (s, d) in enumerate(mine)]
    for cp in ends + outs[6:]:
        cp.start()
    for cp in ends + outs:
        cp.wait()


def step(features, w_in, w_out, table, cand_ids, log_q, targets):
    rows, dim = table.shape
    hid = w_in.shape[1]
    A, S = (pl.BlockSpec(memory_space=m) for m in (pl.ANY, pltpu.SMEM))
    sds = jax.ShapeDtypeStruct
    vm = pltpu.VMEM
    tokens = (2, NA, NZ, NA, TD)
    stat = lambda *n: vm(n + (2 * HR + 8, LN), F32)
    col = vm((NC, CH, LN), F32)
    row = vm((SR, LN), F32)
    return pl.pallas_call(
        step_kernel, name="step",
        out_shape=(sds((1, 1), F32), sds((rows, dim), F32), sds((w_in.shape[0], hid), F32), sds((hid, dim), F32), sds(tokens + (dim,), BF16),
                   sds((3, SR, LN), F32), sds((LN, dim), F32), sds((8, LN), jnp.int32), sds((8, LN), F32), sds(tokens + (w_in.shape[0],), BF16)),
        in_specs=[A] * 6 + [S], out_specs=(S,) + (A,) * 9,
        scratch_shapes=[
            vm(features.shape, BF16), vm(w_in.shape, BF16), vm(w_out.shape, BF16), vm(table.shape, BF16), vm((TD, LN), jnp.int32), vm((TD, LN), F32),
            vm((8, rows), F32), vm(tokens + (dim,), BF16), vm((2, NA, NZ, NA, 1, LN), jnp.int32), vm(tokens + (dim,), BF16),
            vm((NC, CH, rows), F32), vm((CH, rows), BF16), vm((rows, dim), F32), vm((NC, CH, dim), BF16), col, col, col, vm((CH, LN), F32),
            row, row, row, vm((SR, LN), jnp.int32), vm((3, SR, LN), F32), vm((LN, dim), F32), vm((8, LN), jnp.int32), vm((8, LN), F32),
            stat(2), stat(), stat(NA), stat(), stat(NA), stat(NZ), vm((2, HR + 8, LN), F32),
            vm((2, 2, NA, PZ, dim), F32), vm((NZ, NA, PZ, dim), F32), vm((4, NA, PZ, dim), F32), vm((NZ, NA, PZ, dim), F32),
            vm((4, NA, TD, dim), F32), vm((NZ, NA, TD, dim), F32), vm((2 * NZ, TD, dim), F32),
            DMA((6,)), DMA((9,)), DMA((2,)), DMA((1,))] + Gather.SEMS * 4 + [
            DMA] * 12 + [DMA((2,)), DMA((NZ,)), DMA((4,)), DMA((NZ,)), DMA((4,)), DMA((NZ,)), DMA, DMA, DMA((3,)), DMA((3,))],
        compiler_params=pltpu.CompilerParams(collective_id=0, has_side_effects=True, vmem_limit_bytes=VMEM_ALL),
    )(features, w_in, w_out, table, cand_ids.reshape(-1, LN), log_q.reshape(-1, LN), targets)


def target_ranks(st, rows):
    own = (st[0] >= 0) & (st[0] < rows)
    g = jnp.where(own, (jnp.exp(jnp.where(own, st[2], 0.0) - st[1]) - 1.0) * (1.0 / NT), 0.0)
    of = jnp.where(own, 1.0, 0.0)
    before = lambda n, i, j: jnp.where(lax.broadcasted_iota(jnp.int32, (n, n), i) < lax.broadcasted_iota(jnp.int32, (n, n), j), 1.0, 0.0).astype(BF16)
    pre = jnp.dot(of.astype(BF16), before(LN, 0, 1), preferred_element_type=F32)
    tot = jnp.broadcast_to(jnp.sum(of, axis=1, keepdims=True), (SR, LN))
    return jnp.where(own, pre + jnp.dot(before(SR, 1, 0), tot.astype(BF16), preferred_element_type=F32), -1.0), g, jnp.sum(of)


def target_page(p, st, rank, g, h_row, out_h, out_i, out_g):
    slot = (lax.broadcasted_iota(jnp.int32, (LN, LN), 0) + p * LN).astype(F32)
    rr, gg = jnp.zeros((LN, LN), F32), jnp.zeros((LN, LN), F32)
    hh = jnp.zeros((LN, 2 * LN), F32)
    for r in range(SR):
        rw = slice(r, r + 1)
        hit = rank[rw] == slot
        rr += jnp.where(hit, st[0, rw], 0.0)
        gg += jnp.where(hit, g[rw], 0.0)
        hh += jnp.dot(jnp.where(hit, 1.0, 0.0).astype(BF16), h_row(r), preferred_element_type=F32)
    row = lambda m: jnp.transpose(jnp.broadcast_to(jnp.sum(m, axis=1, keepdims=True), (LN, LN)))[:8]
    out_i[...] = row(rr).astype(jnp.int32)
    out_g[...] = row(gg)
    out_h[...] = hh


def token_rows(h, r):
    ci, g = r // GR, r % GR
    return h[ci // NA, ci % NA, 2 * g:2 * g + 2].reshape(LN, 2 * LN)


def fix_kernel(de_hbm, h_hbm, st_hbm, lh_hbm, li_hbm, lg_hbm, gwi_hbm, gwo_hbm, out_hbm, wi_hbm, wo_hbm,
               de, h, st, wi, wo, lh, li, lg, si, sg, sem):
    rows = de.shape[0]
    pairs = ((st_hbm, st), (li_hbm, si), (lg_hbm, sg), (lh_hbm, lh), (de_hbm, de), (gwi_hbm, wi), (gwo_hbm, wo), (de, out_hbm), (wi, wi_hbm), (wo, wo_hbm))
    ins = [pltpu.make_async_copy(s, d, sem.at[i]) for i, (s, d) in enumerate(pairs)]
    outs = ins[7:]
    for cp in ins[:7]:
        cp.start()
    ins[0].wait()
    own = (st[0] >= 0) & (st[0] < rows)
    n = jnp.sum(jnp.where(own, 1.0, 0.0)).astype(jnp.int32)
    for i in (6, 5):
        ins[i].wait()
        ins[i + 3].start()
    for cp in ins[1:5]:
        cp.wait()

    def page(p, _):
        @pl.when(p > 0)
        def _():
            run([pltpu.make_async_copy(h_hbm, h, sem.at[0])])
            rank, g, _ = target_ranks(st, rows)
            target_page(p, st, rank, g, lambda r: token_rows(h, r), lh, li, lg)
            run([pltpu.make_async_copy(li, si, sem.at[1]), pltpu.make_async_copy(lg, sg, sem.at[2])])

        @pl.loop(0, jnp.minimum(n - p * LN, LN))
        def _(i):
            de[pl.ds(si[0, i], 1), :] += sg[0, i] * lh[pl.ds(i, 1), :]
        return 0
    lax.fori_loop(0, (n + LN - 1) // LN, page, 0)
    outs[0].start()
    for cp in outs:
        cp.wait()


def fix(de, h, st, lh, li, lg, gwi, gwo):
    A = pl.BlockSpec(memory_space=pl.ANY)
    vm = lambda m: pltpu.VMEM(m.shape, m.dtype)
    like = lambda m: jax.ShapeDtypeStruct(m.shape, F32)
    return pl.pallas_call(
        fix_kernel, name="fix", out_shape=(like(de), like(gwi), like(gwo)), in_specs=[A] * 8, out_specs=(A,) * 3,
        scratch_shapes=[vm(de), vm(h), vm(st), vm(gwi), vm(gwo), vm(lh), vm(li), vm(lg), pltpu.SMEM(li.shape, jnp.int32), pltpu.SMEM(lg.shape, F32), DMA((10,))],
        compiler_params=pltpu.CompilerParams(vmem_limit_bytes=VMEM_ALL),
    )(de, h, st, lh, li, lg, gwi, gwo)


def solution(mesh):
    def local_step(*args):
        loss, de, gwi, gwo, *rest, _ = step(*args)
        return loss.reshape(()), *fix(de, *rest, gwi, gwo)

    return jax.shard_map(local_step, mesh=mesh, in_specs=(P("dp", None), P(), P(), P("dp", None), P(), P(), P("dp")), out_specs=(P(), P("dp", None), P(), P()), check_vma=False)
```

```python
import functools
import math
import jax
import jax.numpy as jnp
from jax import lax
from jax.experimental import pallas as pl
from jax.experimental.pallas import tpu as pltpu
from jax.sharding import PartitionSpec as P

NZ, NY, NX = 8, 4, 4
NA = 4
LN = 128
TD = 16
NC = 2 * NA
CH = NZ * NA * TD
NT = NC * CH
PZ = NA * TD
SR = NT // LN
GR = CH // LN
F32, BF16 = jnp.float32, jnp.bfloat16
NEG = -jnp.inf
PER_TOKEN = 1.0 / NT
ZO, AO, PO = NZ - 1, NA - 1, SR - 1
DIM = 2 * LN
NC_LAST = NC - 1
VMEM_ALL = 67043328
MESH = pl.DeviceIdType.MESH
ROWS, COLS = (((0,), (0,)), ((), ())), (((1,), (1,)), ((), ()))
DMA = pltpu.SemaphoreType.DMA


def coords():
    me = lax.axis_index("dp")
    z, y, x, c = me // (NY * NX * 2), (me // (NX * 2)) % NY, (me // 2) % NX, me % 2
    return z, y, x, c, x * (1 - c) + y * c, y * (1 - c) + x * c


def dev(z, y, x, c):
    return (((z * NY + y) * NX + x) * 2 + c,)


def peers():
    z, y, x, c, v, a = coords()
    return (dev(z, y, x, 1 - c), lambda k: dev((z + k) % NZ, y, x, c), lambda k: dev(z, (y + k * c) % NY, (x + k * (1 - c)) % NX, c),
            lambda k: dev(z, (y + k * (1 - c)) % NY, (x + k * c) % NX, c))


def in_plane(k):
    z, y, x, c, v, a = coords()
    p = ((y * NX + x) * 2 + c + k) % SR
    return dev(z, p // (NX * 2), (p // 2) % NX, p % 2)


def rcopy(src, dst, ssem, rsem, to):
    return pltpu.make_async_remote_copy(src_ref=src, dst_ref=dst, send_sem=ssem, recv_sem=rsem, device_id=to, device_id_type=MESH)


def run(copies):
    for cp in copies:
        cp.start()
    for cp in copies:
        cp.wait()


def signal_peers():
    bar = pltpu.get_barrier_semaphore()
    to_c, to_z, to_1, to_2 = peers()
    z, y, x, c, v, a = coords()
    tell = lambda p: pl.semaphore_signal(bar, inc=1, device_id=p, device_id_type=MESH)
    pl.loop(1, NZ)(lambda k: tell(to_z(k)))
    pl.loop(1, SR)(lambda k: tell(in_plane(k)))
    return bar, NZ + SR - 2


NEAR = (1, 3, 2)


class Gather:
    SEMS = [DMA, DMA((2,)), DMA, DMA((3,)), DMA, DMA((AO,)), DMA, DMA((NA,))]
    WAVE = (1, 4, 3)

    def __init__(self, buf, sems):
        z, y, x, c, v, a = coords()
        sz, rz, s2, r2, s1, r1, sd, rd = sems
        to_c, to_z, to_1, to_2 = peers()
        self.c, self.v, self.a = c, v, a
        blk = lambda d, j: buf.at[c, v, (z + NZ - d) % NZ, (a + NA - j) % NA]
        chunk = lambda j: buf.at[c, (v + NA - j) % NA]
        self.to_z = lambda k: rcopy(blk(0, 0), blk(0, 0), sz, rz.at[jnp.minimum(k, NZ - k) // 3], to_z(k)).start()
        self.to_2 = lambda w, d: [rcopy(blk(d, 0), blk(d, 0), s2, r2.at[w], to_2(k)).start() for k in NEAR]
        self.to_1 = lambda d, j: [rcopy(blk(d, j), blk(d, j), s1, r1.at[k - 1], to_1(k)).start() for k in NEAR]
        self.to_c = lambda j: rcopy(chunk(j), chunk(j), sd, rd.at[j], to_c)
        every = lambda ref, ss, rs: rcopy(ref, ref, ss, rs, to_c)
        self.z_in = lambda w: every(buf.at[c, v, pl.ds(0, self.WAVE[w]), a], sz, rz.at[w - 1]).wait_recv()
        self.two_in = lambda w: every(buf.at[c, v, pl.ds(0, (1, AO, AO)[w]), pl.ds(0, (AO, NA, AO)[w])], s2, r2.at[w]).wait_recv()
        self.one_in = lambda k: every(chunk(k), s1, r1.at[k - 1]).wait_recv()
        self.sent = [every(buf.at[c, v, pl.ds(0, ZO), a], sz, rz.at[0]), every(buf.at[c, v, :, pl.ds(0, AO)], s2, r2.at[0]),
                     every(buf.at[c, pl.ds(0, AO)], s1, r1.at[0]), every(buf.at[c], sd, rd.at[0])]

    def each(self, w, f):
        if w == 0:
            f(0)
        else:
            pl.loop(0, self.WAVE[w])(lambda i: f((2 * w - 1 + i // 2) * (1 - 2 * (i % 2))) and None)

    def start(self):
        pl.loop(1, NZ)(self.to_z)
        self.to_2(0, 0)
        self.to_1(0, 0)

    def column(self, w):
        self.z_in(w)
        self.each(w, lambda d: self.to_2(w, d) + self.to_1(d, 0))

    def rest(self, w):
        self.two_in(w)
        self.each(w, lambda d: sum((self.to_1(d, j) for j in NEAR), []))

    def finish(self):
        for cp in self.sent:
            cp.wait_send()

    def place(self, n):
        i, p = n // 2, n % 2
        j = i + (i // 2) * (1 - 2 * (i % 2))
        return i, p, j, (self.c + p * (1 - 2 * self.c), (self.v * (1 - p) + self.a * p + NA - j) % NA)

    def take(self, n):
        i, p, j, cv = self.place(n)

        @pl.when((p == 0) & (i > 0))
        def _():
            self.one_in(j)
            self.to_c(j).start()
        pl.when(p == 1)(lambda: self.to_c(j).wait_recv())
        return cv


class GatherFeatures:
    SEMS = [DMA] * 4 + [DMA, DMA((ZO,)), DMA, DMA((ZO,)), DMA, DMA]

    def __init__(self, buf, sems, src):
        z, y, x, c, v, a = coords()
        s2, r2, s1, r1, sr, rr, sl, rl, sd, rd = sems
        to_c, to_z, to_1, to_2 = peers()
        at = lambda d: buf.at[c, (z + 2 * NZ + d) % NZ]
        own = at(0).at[v // 2, v % 2]
        self.own = own.at[a]
        self.two = lambda: [rcopy(src, own.at[a], s2, r2, to_2(k)).start() for k in NEAR]
        self.one = lambda: [rcopy(own, own, s1, r1, to_1(k)).start() for k in NEAR]
        every = lambda ref, ss, rs: rcopy(ref, ref, ss, rs, to_c)
        self.two_all = every(own.at[pl.ds(0, AO)], s2, r2)
        self.one_all = every(buf.at[c, pl.ds(0, AO), 0, 0], s1, r1)
        self.right = lambda s, h: rcopy(at(1 - s).at[h], at(1 - s).at[h], sr, rr.at[2 * s - 2 + (h if s < NA else 0)], to_z(1))
        self.left = lambda s, h: rcopy(at(s - 1).at[h], at(s - 1).at[h], sl, rl.at[2 * s - 2 + (h if s < NA else 0)], to_z(ZO))
        self.share = lambda ref: rcopy(ref, ref, sd, rd, to_c).start()
        self.at = at
        halves = buf.at[c].reshape((2 * NZ,) + buf.shape[3:])
        self.sent = [every(halves.at[pl.ds(0, ZO)], m, rd) for m in (sr, sl)] + [every(buf.at[c], sd, rd)]
        self.shared = every(buf.at[c], sd, rd)

    def plane(self):
        self.two_all.wait()
        self.one()

    def ring(self):
        self.one_all.wait()
        self.share(self.at(0))
        for h in range(2):
            self.right(1, h).start()
            self.left(1, h).start()

    def move(self, s, h):
        self.right(s, h).wait_recv()
        self.left(s, h).wait_recv()
        if s < 3 or h == 0:
            self.right(s + 1, h).start()
        if s < 3 or h == 1:
            self.left(s + 1, h).start()
        self.share(self.at(-s).at[h])
        self.share(self.at(s).at[h])

    def last(self):
        self.right(NA, 0).wait_recv()
        self.left(NA, 1).wait_recv()
        self.share(self.at(NA))

    def finish(self):
        for cp in self.sent:
            cp.wait_send()


def tree(parts):
    while len(parts) > 1:
        parts = [p + q for p, q in zip(parts[::2], parts[1::2])]
    return parts.pop()


def iota(shape, dim):
    return lax.broadcasted_iota(jnp.int32, shape, dim)


def lane_sum(m):
    return jnp.sum(m, axis=1, keepdims=True)


def lane_max(m):
    return jnp.max(m, axis=1, keepdims=True)


def ones_at(hit):
    return jnp.where(hit, 1.0, 0.0)


def to_col(row):
    return jnp.transpose(jnp.broadcast_to(row, (LN, LN)))


def logq_rows(cid_v, lq_v, lqr_ref, base):
    @pl.loop(0, lqr_ref.shape[1] // LN, unroll=4)
    def _(i):
        blk = pl.multiple_of(i * LN, LN)
        rid = iota((LN, LN), 0) + (base + blk)
        acc = jnp.zeros((LN, LN), F32)
        for q in range(cid_v.shape[0]):
            acc += jnp.where(cid_v[q:q + 1, :] == rid, lq_v[q:q + 1, :], 0.0)
        lqr_ref[:, pl.ds(blk, LN)] = jnp.transpose(jnp.broadcast_to(lane_sum(acc), (LN, LN)))[:8]


def target_cols(yblk, base, yl_ref, row, d_ref):
    lane = iota((LN, LN), 1).astype(F32)
    group = iota((1, LN), 1) // TD
    for g in range(GR):
        yr = sum(jnp.where(group == b, yblk(g * 8 + b), 0) for b in range(8)) - base
        yl_ref[pl.ds(row + g, 1), :] = yr
        d_ref[g * LN:(g + 1) * LN, :] = to_col(yr.astype(F32)) - lane


def scores_chunk(h, emb_ref, lqr_ref, e_ref, d_ref, mcol_ref, zcol_ref, scol_ref):
    rows = emb_ref.shape[0]
    RB = PZ
    for j in range(0, rows, DIM):
        s = lax.dot_general(h, emb_ref[j:j + DIM, :], COLS, preferred_element_type=F32)
        for rb in range(0, CH, RB):
            rs = slice(rb, rb + RB)
            m = mcol_ref[rs, :] if j else jnp.full((RB, LN), NEG, F32)
            zc = zcol_ref[rs, :] if j else jnp.full((RB, LN), NEG, F32)
            d = d_ref[rs, :]
            for k in (0, LN):
                raw = s[rs, k:k + LN]
                hit = d == float(j + k)
                zc = jnp.where(hit, raw, zc)
                val = jnp.where(hit, -1e9, raw - lqr_ref[:1, j + k:j + k + LN])
                e_ref[rs, j + k:j + k + LN] = val
                m = jnp.maximum(m, val)
            mcol_ref[rs, :] = m
            zcol_ref[rs, :] = zc
    for rb in range(0, CH, RB):
        rs = slice(rb, rb + RB)
        zc = lane_max(zcol_ref[rs, :])
        m = jnp.maximum(lane_max(mcol_ref[rs, :]), zc)
        zcol_ref[rs, :] = jnp.broadcast_to(zc, (RB, LN))
        mcol_ref[rs, :] = jnp.broadcast_to(m, (RB, LN))

    def grp(g, _):
        rs = pl.ds(pl.multiple_of(g * RB, RB), RB)
        m = mcol_ref[rs, :]
        tot = jnp.zeros((RB, LN), F32)
        for k in range(0, rows, LN):
            ex = jnp.exp(e_ref[rs, k:k + LN] - m)
            e_ref[rs, k:k + LN] = ex
            tot += ex
        scol_ref[rs, :] = tot
        return 0
    lax.fori_loop(0, CH // RB, grp, 0)
    for rb in range(0, CH, RB):
        rs = slice(rb, rb + RB)
        tot = lane_sum(scol_ref[rs, :])
        scol_ref[rs, :] = jnp.broadcast_to(tot, (RB, LN)) + jnp.exp(zcol_ref[rs, :] - mcol_ref[rs, :])


def reduce_stats(pb, rb, zb, ab, st, sems, fill):
    z, y, x, c, v, a = coords()
    to_c, to_z, to_1, to_2 = peers()
    sp, rp, sz, rz, sa, ra = sems
    me = (y * NX + x) * 2 + c

    def merge(ref):
        m, s = ref[:, 0, :], ref[:, 1, :]
        top = jnp.max(m, axis=0, keepdims=True)
        return top, jnp.sum(s * jnp.exp(m - top), axis=0, keepdims=True), jnp.max(ref[:, 2, :], axis=0, keepdims=True)

    rb[me] = pb[me]
    pl.loop(1, SR)(lambda k: rcopy(pb.at[(me + k) % SR], rb.at[me], sp, rp, in_plane(k)).start())
    fill(0)
    rcopy(rb.at[pl.ds(0, PO)], rb.at[pl.ds(0, PO)], sp, rp, to_c).wait()
    for i, val in enumerate(merge(rb)):
        zb[z, i:i + 1, :] = val
    pl.loop(1, NZ)(lambda k: rcopy(zb.at[z], zb.at[z], sz, rz, to_z(k)).start())
    fill(1)
    rcopy(zb.at[pl.ds(0, ZO)], zb.at[pl.ds(0, ZO)], sz, rz, to_c).wait()
    m, s, t = merge(zb)
    ab[me, 0:1, :] = m + jnp.log(s)
    ab[me, 1:2, :] = t
    pl.loop(1, SR)(lambda k: rcopy(ab.at[me], ab.at[me], sa, ra, in_plane(k)).start())
    fill(2)
    rcopy(ab.at[pl.ds(0, PO)], ab.at[pl.ds(0, PO)], sa, ra, to_c).wait()
    st[1] = ab[:, 0, :]
    st[2] = ab[:, 1, :]
    return jnp.sum(ab[:, 0, :] - ab[:, 1, :]) * PER_TOKEN


def gelu_both(u):
    k0, k1 = math.sqrt(2.0 / math.pi), 0.044715
    sq = u * u
    t = jnp.tanh(k0 * (u + k1 * (sq * u)))
    cdf = 0.5 * (1.0 + t)
    return u * cdf, cdf + (0.5 * k0) * u * ((1.0 - t * t) * (1.0 + (3.0 * k1) * sq))


def step_kernel(x_hbm, win_hbm, wout_hbm, emb_hbm, cid_hbm, lq_hbm, y_s,
                loss_ref, de_hbm, gwi_hbm, gwo_hbm, h_hbm, st_hbm, lh_hbm, li_hbm, lg_hbm, xg,
                xv, win, wout, emb, cid_v, lq_v, lqr, hb, yb, dh,
                eb, pb, de, te, dcol, mcol, zcol, scol, yl, st, lh, li, lg, pst, rst, zst, ast,
                dq, rc, a0, ra, a1, rb, zb,
                lsem, osem, fsem, xsem, *sems):
    z, y, x, c, v, a = coords()
    to_c, to_z, to_1, to_2 = peers()
    rows = emb.shape[0]
    hid = win.shape[1]
    half = hid // 2
    me = lax.axis_index("dp")
    base = me * rows
    take = lambda n, it=iter(sems): [next(it) for _ in range(n)]
    gh, gy, gd = (take(len(Gather.SEMS)) for _ in range(3))
    gx = take(len(GatherFeatures.SEMS))
    own16 = pl.ds(me * TD, TD)
    loads = [pltpu.make_async_copy(s, d, lsem.at[i]) for i, (s, d) in enumerate((
        (x_hbm, xv), (win_hbm, win), (wout_hbm, wout), (emb_hbm, emb), (cid_hbm.at[own16], cid_v), (lq_hbm.at[own16], lq_v)))]
    for cp in loads:
        cp.start()
    bar, n_peers = signal_peers()

    for cp in loads[:3]:
        cp.wait()
    pre = jnp.dot(xv[...], win[...], preferred_element_type=F32)
    act = gelu_both(pre)[0].astype(BF16)
    hb[c, v, z, a] = jnp.dot(act, wout[...], preferred_element_type=F32).astype(BF16)
    lane16 = iota((1, LN), 1) % TD
    yb[c, v, z, a] = sum(jnp.where(lane16 == i, y_s[i], 0) for i in range(TD))
    pl.semaphore_wait(bar, n_peers)

    gath, gaty, gatx, gatd = Gather(hb, gh), Gather(yb, gy), GatherFeatures(xg, gx, xv), Gather(dh, gd)
    xown = pltpu.make_async_copy(xv, gatx.own, xsem.at[0])
    gath.start()
    gaty.start()
    xown.start()
    gatx.two()
    for cp in loads[3:]:
        cp.wait()
    logq_rows(cid_v, lq_v, lqr, base)
    de[...] = jnp.zeros_like(de)
    gath.column(1)
    gaty.column(1)
    gath.rest(0)
    gaty.rest(0)
    xown.wait()
    gatx.plane()
    gath.column(2)
    gaty.column(2)
    gath.rest(1)
    gath.rest(2)
    gath.to_c(0).start()
    gaty.rest(1)
    gaty.rest(2)
    gaty.to_c(0).start()

    lane = iota((LN, LN), 1)

    def score(cc, vv):
        ci = cc * NA + vv
        target_cols(lambda b: yb[cc, vv, b // NA, b % NA], base, yl, ci * GR, dcol.at[ci])
        scores_chunk(hb[cc, vv].reshape(CH, DIM), emb, lqr, eb.at[ci], dcol.at[ci], mcol.at[ci], zcol.at[ci], scol)
        for b in range(GR):
            bs_ = slice(b * LN, (b + 1) * LN)
            three = jnp.where(lane == 0, mcol[ci, bs_, :], jnp.where(lane == 1, scol[bs_, :], zcol[ci, bs_, :]))
            pst[ci * GR + b] = jnp.transpose(three)[:NA]

    @pl.loop(0, NC)
    def _(n):
        gaty.take(n)
        cv = gath.take(n)
        pl.when(n == 1)(gatx.ring)
        pl.when(n == 4)(lambda: gatx.move(1, 0))
        pl.when(n == NC_LAST)(lambda: gatx.move(1, 1))
        score(*cv)

    def target_rows(lo, hi):
        @pl.loop(lo, hi)
        def _(ci):
            for q in range(0, rows, LN):
                pb[:, q:q + LN] = ones_at(dcol[ci] == float(q)).astype(BF16)
            te[ci] = jnp.dot(pb[...], emb[...], preferred_element_type=F32).astype(BF16)

    def fill(n):
        if n:
            gatx.move(2, n - 1)
        target_rows(*((0, 3), (3, 6), (6, NC))[n])

    lr = st.at[1]
    loss_ref[0, 0] = reduce_stats(pst, rst, zst, ast, st, take(6), fill)
    @pl.loop(0, NC)
    def _(ci):
        for b in range(GR):
            bs_ = slice(b * LN, (b + 1) * LN)
            lc = to_col(lr[pl.ds(ci * GR + b, 1), :])
            mcol[ci, bs_, :] = jnp.exp(mcol[ci, bs_, :] - lc) * PER_TOKEN
            zc = zcol[ci, bs_, :]
            zcol[ci, bs_, :] = jnp.where(zc > NEG, (jnp.exp(zc - lc) - 1.0) * PER_TOKEN, 0.0)
    st[0] = yl[...].astype(F32)

    sc, rcs, sa, ras, sb, rbs, sz, rzs = take(8)
    ring = a0.shape[0]
    c_copy = lambda k: rcopy(dq.at[k % 2, 1 - c], rc.at[k], sc.at[k % 2], rcs.at[k], to_c)
    a_copy = lambda k, j: rcopy(a0.at[k % ring, (v + j) % NA], ra.at[k, v], sa.at[k % ring], ras.at[k], to_1(j))
    a_all = lambda k: rcopy(ra.at[k, pl.ds(0, AO)], ra.at[k, pl.ds(0, AO)], sa.at[k % ring], ras.at[k], to_c)
    b_copy = lambda k, j: rcopy(a1.at[k % ring, (a + j) % NA], rb.at[k, a], sb.at[k % ring], rbs.at[k], to_2(j))
    b_all = lambda k: rcopy(rb.at[k, pl.ds(0, AO)], rb.at[k, pl.ds(0, AO)], sb.at[k % ring], rbs.at[k], to_c)

    def off(k):
        s = (k + 1) // 2
        return NA + s - 2 * s * (k % 2)

    z_copy = lambda k: rcopy(zb.at[NZ + k], zb.at[z], sz, rzs, to_z(off(k)))

    def compute(k):
        zz = (z + off(k)) % NZ
        piece = pl.ds(pl.multiple_of(zz * PZ, PZ), PZ)
        for ci in range(NC):
            ps = slice(ci * PZ, (ci + 1) * PZ)
            f = mcol[ci, piece, :]
            for q in range(0, rows, LN):
                pb[ps, q:q + LN] = (eb[ci, piece, q:q + LN] * f).astype(BF16)
        h = jnp.concatenate([hb[ci // NA, ci % NA, zz].reshape(PZ, DIM) for ci in range(NC)], axis=0)
        for q in range(0, rows, CH):
            de[q:q + CH, :] += lax.dot_general(pb[:, q:q + CH], h, ROWS, preferred_element_type=F32)
        out = jnp.dot(pb[...], emb[...], preferred_element_type=F32)
        for ci in range(NC):
            g = zcol[ci, piece, :]
            t = te[ci, piece, :].astype(F32)
            for hf in (0, LN):
                dq[k % 2, ci // NA, ci % NA, :, hf:hf + LN] = out[ci * PZ:(ci + 1) * PZ, hf:hf + LN] + g * t[:, hf:hf + LN]
        c_copy(k).start()

    def sum_core(k):
        c_copy(k).wait()
        a0[k % ring] = dq[k % 2, c] + rc[k]
        for j in NEAR:
            a_copy(k, j).start()

    def sum_first(k):
        a_all(k).wait()
        ra[k, v] = a0[k % ring, v]
        a1[k % ring] = tree([ra[k, i] for i in range(NA)]).reshape(NA, TD, DIM)
        for j in NEAR:
            b_copy(k, j).start()

    def sum_second(k, last=False):
        b_all(k).wait()
        rb[k, a] = a1[k % ring, a]
        val = tree([rb[k, i] for i in range(NA)])
        if last:
            zb[z] = val
        else:
            zb[NZ + k] = val
            z_copy(k).start()

    def body(k, _):
        compute(k)
        for lag, f in ((1, sum_core), (3, sum_first), (5, sum_second)):
            pl.when(k >= lag)(functools.partial(f, k - lag))
        pl.when(k == 1)(lambda: gatx.move(3, 0))
        pl.when(k == 2)(lambda: gatx.move(3, 1))
        pl.when(k == 6)(gatx.last)
        return 0

    lax.fori_loop(0, NZ, body, 0)
    outs = [pltpu.make_async_copy(s, d, osem.at[i]) for i, (s, d) in enumerate(((de, de_hbm), (hb, h_hbm), (st, st_hbm), (lh, lh_hbm), (li, li_hbm), (lg, lg_hbm)))]
    for cp in outs[:3]:
        cp.start()

    cols = pl.ds(pl.multiple_of(c * half, half), half)
    def xs(ci, slot, go):
        to = pl.ds(pl.multiple_of(slot * hid, hid), hid)
        if go:
            @pl.loop(0, NZ)
            def _(zz):
                src = xg.at[ci // NA, zz, (ci % NA) // 2, ci % 2].reshape(PZ, hid)
                pltpu.make_async_copy(src, pb.at[pl.ds(pl.multiple_of(zz * PZ, PZ), PZ), to], fsem.at[slot]).start()
        else:
            pltpu.make_async_copy(pb.at[:, to], pb.at[:, to], fsem.at[slot]).wait()

    def tower(ci, slot):
        pre = jnp.dot(pb[:, pl.ds(pl.multiple_of(slot * hid, hid), hid)], win[:, cols], preferred_element_type=F32)
        act, der = gelu_both(pre)
        eb[ci, :, :half] = der
        eb[ci, :, half:2 * half] = act.astype(BF16).astype(F32)

    ordinal = lambda n: gatd.place(n)[3][0] * NA + gatd.place(n)[3][1]

    def towers(lo, hi):
        @pl.loop(lo, hi)
        def _(n):
            pl.when(n + 1 < NC)(lambda: xs(ordinal(n + 1), (n + 1) % 2, True))
            xs(ordinal(n), n % 2, False)
            tower(ordinal(n), n % 2)

    sum_core(7)
    sum_second(3)
    gatx.shared.wait_recv()
    xs(ordinal(0), 0, True)
    sum_first(5)
    sum_second(4)
    towers(0, 1)
    sum_first(6)
    towers(1, 2)
    sum_first(7)
    sum_second(5)
    towers(2, 3)
    sum_second(6)
    towers(3, 4)
    sum_second(7, last=True)
    rcopy(zb.at[pl.ds(0, ZO)], zb.at[pl.ds(0, ZO)], sz, rzs, to_c).wait()
    tot = tree([zb[i] for i in range(NZ)])
    dh[c, v, z, a] = tot.astype(BF16)
    gatd.start()
    towers(4, 6)
    gatd.column(1)
    gatd.rest(0)
    gatd.column(2)
    towers(6, 7)
    gatd.rest(1)
    towers(7, NC)
    xs(ordinal(0), 0, True)
    gatd.rest(2)
    gatd.to_c(0).start()
    rank, gfac, _ = target_ranks(st, rows)
    target_page(0, st, rank, gfac, lambda r: token_rows(hb, r), lh, li, lg)
    for cp in outs[3:6]:
        cp.start()
    acc_i, acc_o = eb.at[pl.ds(0, 2), :, pl.ds(2 * half, half)], eb.at[2, :, pl.ds(2 * half, DIM)]
    acc_i[...] = jnp.zeros(acc_i.shape, F32)
    acc_o[...] = jnp.zeros(acc_o.shape, F32)

    def weights(ci, slot):
        g = dh[ci // NA, ci % NA].reshape(CH, DIM)
        back = lax.dot_general(g, wout[cols, :], COLS, preferred_element_type=F32)
        da = (eb[ci, :, :half] * back).astype(BF16)
        act = eb[ci, :, half:2 * half].astype(BF16)
        acc_o[...] += lax.dot_general(act, g, ROWS, preferred_element_type=F32)
        for r in range(2):
            xr = pb[:, pl.ds(pl.multiple_of(slot * hid + r * half, half), half)]
            acc_i[r] += lax.dot_general(xr, da, ROWS, preferred_element_type=F32)

    @pl.loop(0, NC)
    def _(n):
        gatd.take(n)
        pl.when(n + 1 < NC)(lambda: xs(ordinal(n + 1), (n + 1) % 2, True))
        xs(ordinal(n), n % 2, False)
        weights(ordinal(n), n % 2)

    for g in (gath, gaty, gatx, gatd):
        g.finish()
    so, ro = take(2)
    mine = [(acc_i.at[r], gwi_hbm.at[pl.ds(r * half, half), cols]) for r in range(2)] + [(acc_o, gwo_hbm.at[cols])]
    ends = [rcopy(s, d, so.at[i], ro.at[i], to_c) for i, (s, d) in enumerate(mine)]
    outs += [pltpu.make_async_copy(s, d, osem.at[6 + i]) for i, (s, d) in enumerate(mine)]
    for cp in ends + outs[6:]:
        cp.start()
    for cp in ends + outs:
        cp.wait()


def step(features, w_in, w_out, table, cand_ids, log_q, targets):
    rows, dim = table.shape
    hid = w_in.shape[1]
    A, S = (pl.BlockSpec(memory_space=m) for m in (pl.ANY, pltpu.SMEM))
    sds = jax.ShapeDtypeStruct
    vm = pltpu.VMEM
    tokens = (2, NA, NZ, NA, TD)
    stat = lambda n: vm((n, NA, LN), F32)
    col = vm((NC, CH, LN), F32)
    return pl.pallas_call(
        step_kernel, name="step",
        out_shape=(sds((1, 1), F32), sds((rows, dim), F32), sds((w_in.shape[0], hid), F32), sds((hid, dim), F32), sds(tokens + (dim,), BF16),
                   sds((3, SR, LN), F32), sds((LN, dim), F32), sds((8, LN), jnp.int32), sds((8, LN), F32), sds((2, NZ, 2, 2, NA, TD, w_in.shape[0]), BF16)),
        in_specs=[A] * 6 + [S], out_specs=(S,) + (A,) * 9,
        scratch_shapes=[
            vm(features.shape, BF16), vm(w_in.shape, BF16), vm(w_out.shape, BF16), vm(table.shape, BF16), vm((TD, LN), jnp.int32), vm((TD, LN), F32),
            vm((8, rows), F32), vm(tokens + (dim,), BF16), vm((2, NA, NZ, NA, 1, LN), jnp.int32), vm(tokens + (dim,), BF16),
            vm((NC, CH, rows), F32), vm((CH, rows), BF16), vm((rows, dim), F32), vm((NC, CH, dim), BF16), col, col, col, vm((CH, LN), F32),
            vm((SR, LN), jnp.int32), vm((3, SR, LN), F32), vm((LN, dim), F32), vm((8, LN), jnp.int32), vm((8, LN), F32),
            stat(SR), stat(SR), stat(NZ), stat(SR),
            vm((2, 2, NA, PZ, dim), F32), vm((NZ, NA, PZ, dim), F32), vm((4, NA, PZ, dim), F32), vm((NZ, NA, PZ, dim), F32),
            vm((4, NA, TD, dim), F32), vm((NZ, NA, TD, dim), F32), vm((2 * NZ, TD, dim), F32),
            DMA((6,)), DMA((9,)), DMA((2,)), DMA((1,))] + Gather.SEMS * 3 + GatherFeatures.SEMS + [
            DMA] * 6 + [DMA((2,)), DMA((NZ,)), DMA((4,)), DMA((NZ,)), DMA((4,)), DMA((NZ,)), DMA, DMA, DMA((3,)), DMA((3,))],
        compiler_params=pltpu.CompilerParams(collective_id=0, has_side_effects=True, vmem_limit_bytes=VMEM_ALL),
    )(features, w_in, w_out, table, cand_ids.reshape(-1, LN), log_q.reshape(-1, LN), targets)


def target_ranks(st, rows):
    own = (st[0] >= 0) & (st[0] < rows)
    g = jnp.where(own, (jnp.exp(jnp.where(own, st[2], 0.0) - st[1]) - 1.0) * PER_TOKEN, 0.0)
    of = ones_at(own)
    before = lambda n, i, j: jnp.where(iota((n, n), i) < iota((n, n), j), 1.0, 0.0).astype(BF16)
    pre = jnp.dot(of.astype(BF16), before(LN, 0, 1), preferred_element_type=F32)
    tot = jnp.broadcast_to(lane_sum(of), (SR, LN))
    return jnp.where(own, pre + jnp.dot(before(SR, 1, 0), tot.astype(BF16), preferred_element_type=F32), -1.0), g, jnp.sum(of)


def target_page(p, st, rank, g, h_row, out_h, out_i, out_g):
    slot = (iota((LN, LN), 0) + p * LN).astype(F32)
    rr, gg = jnp.zeros((LN, LN), F32), jnp.zeros((LN, LN), F32)
    hh = jnp.zeros((LN, DIM), F32)
    for r in range(SR):
        rw = slice(r, r + 1)
        hit = rank[rw] == slot
        rr += jnp.where(hit, st[0, rw], 0.0)
        gg += jnp.where(hit, g[rw], 0.0)
        hh += jnp.dot(ones_at(hit).astype(BF16), h_row(r), preferred_element_type=F32)
    row = lambda m: jnp.transpose(jnp.broadcast_to(lane_sum(m), (LN, LN)))[:8]
    out_i[...] = row(rr).astype(jnp.int32)
    out_g[...] = row(gg)
    out_h[...] = hh


def token_rows(h, r):
    ci, g = r // GR, r % GR
    return h[ci // NA, ci % NA, 2 * g:2 * g + 2].reshape(LN, DIM)


def fix_kernel(de_hbm, h_hbm, st_hbm, lh_hbm, li_hbm, lg_hbm, gwi_hbm, gwo_hbm, out_hbm, wi_hbm, wo_hbm,
               de, h, st, wi, wo, lh, li, lg, si, sg, sem):
    rows = de.shape[0]
    pairs = ((st_hbm, st), (li_hbm, si), (lg_hbm, sg), (lh_hbm, lh), (de_hbm, de), (gwi_hbm, wi), (gwo_hbm, wo), (de, out_hbm), (wi, wi_hbm), (wo, wo_hbm))
    ins = [pltpu.make_async_copy(s, d, sem.at[i]) for i, (s, d) in enumerate(pairs)]
    outs = ins[7:]
    for cp in ins[:7]:
        cp.start()
    ins[0].wait()
    own = (st[0] >= 0) & (st[0] < rows)
    n = jnp.sum(ones_at(own)).astype(jnp.int32)
    for i in (6, 5):
        ins[i].wait()
        ins[i + 3].start()
    for cp in ins[1:5]:
        cp.wait()

    def page(p, _):
        @pl.when(p > 0)
        def _():
            run([pltpu.make_async_copy(h_hbm, h, sem.at[0])])
            rank, g, _ = target_ranks(st, rows)
            target_page(p, st, rank, g, lambda r: token_rows(h, r), lh, li, lg)
            run([pltpu.make_async_copy(li, si, sem.at[1]), pltpu.make_async_copy(lg, sg, sem.at[2])])

        @pl.loop(0, jnp.minimum(n - p * LN, LN))
        def _(i):
            de[pl.ds(si[0, i], 1), :] += sg[0, i] * lh[pl.ds(i, 1), :]
        return 0
    lax.fori_loop(0, (n + LN - 1) // LN, page, 0)
    outs[0].start()
    for cp in outs:
        cp.wait()


def fix(de, h, st, lh, li, lg, gwi, gwo):
    A = pl.BlockSpec(memory_space=pl.ANY)
    vm = lambda m: pltpu.VMEM(m.shape, m.dtype)
    like = lambda m: jax.ShapeDtypeStruct(m.shape, F32)
    return pl.pallas_call(
        fix_kernel, name="fix", out_shape=(like(de), like(gwi), like(gwo)), in_specs=[A] * 8, out_specs=(A,) * 3,
        scratch_shapes=[vm(de), vm(h), vm(st), vm(gwi), vm(gwo), vm(lh), vm(li), vm(lg), pltpu.SMEM(li.shape, jnp.int32), pltpu.SMEM(lg.shape, F32), DMA((10,))],
        compiler_params=pltpu.CompilerParams(vmem_limit_bytes=VMEM_ALL),
    )(de, h, st, lh, li, lg, gwi, gwo)


def solution(mesh):
    def local_step(*args):
        loss, de, gwi, gwo, *rest, _ = step(*args)
        return loss.reshape(()), *fix(de, *rest, gwi, gwo)

    return jax.shard_map(local_step, mesh=mesh, in_specs=(P("dp", None), P(), P(), P("dp", None), P(), P(), P("dp")), out_specs=(P(), P("dp", None), P(), P()), check_vma=False)
```

```python
import functools
import math
import jax
import jax.numpy as jnp
from jax import lax
from jax.experimental import pallas as pl
from jax.experimental.pallas import tpu as pltpu
from jax.sharding import PartitionSpec as P

NZ, NY, NX = 8, 4, 4
NA = 4
LN = 128
TD = 16
NC = 2 * NA
CH = NZ * NA * TD
NT = NC * CH
PZ = NA * TD
SR = NT // LN
GR = CH // LN
F32, BF16 = jnp.float32, jnp.bfloat16
NEG = -jnp.inf
PER_TOKEN = 1.0 / NT
ZO, AO, PO = NZ - 1, NA - 1, SR - 1
DIM = 2 * LN
NC_LAST = NC - 1
VMEM_ALL = 67043328
MESH = pl.DeviceIdType.MESH
ROWS, COLS = (((0,), (0,)), ((), ())), (((1,), (1,)), ((), ()))
DMA = pltpu.SemaphoreType.DMA


def coords():
    me = lax.axis_index("dp")
    z, y, x, c = me // (NY * NX * 2), (me // (NX * 2)) % NY, (me // 2) % NX, me % 2
    return z, y, x, c, x * (1 - c) + y * c, y * (1 - c) + x * c


def dev(z, y, x, c):
    return (((z * NY + y) * NX + x) * 2 + c,)


def peers():
    z, y, x, c, v, a = coords()
    me = lax.axis_index("dp")
    one = {k: dev(z, (y + k * c) % NY, (x + k * (1 - c)) % NX, c) for k in range(1, NA)}
    two = {k: dev(z, (y + k * (1 - c)) % NY, (x + k * c) % NX, c) for k in range(1, NA)}
    return (me + 1 - 2 * c,), lambda k: ((me + k * SR) % (NZ * SR),), one.get, two.get


def in_plane(k):
    me = lax.axis_index("dp")
    return (me // SR * SR + (me + k) % SR,)


def rcopy(src, dst, ssem, rsem, to):
    return pltpu.make_async_remote_copy(src_ref=src, dst_ref=dst, send_sem=ssem, recv_sem=rsem, device_id=to, device_id_type=MESH)


def run(copies):
    for cp in copies:
        cp.start()
    for cp in copies:
        cp.wait()


def signal_peers():
    bar = pltpu.get_barrier_semaphore()
    to_c, to_z, to_1, to_2 = peers()
    z, y, x, c, v, a = coords()
    tell = lambda p: pl.semaphore_signal(bar, inc=1, device_id=p, device_id_type=MESH)
    pl.loop(1, NZ)(lambda k: tell(to_z(k)))
    pl.loop(1, SR)(lambda k: tell(in_plane(k)))
    return bar, NZ + SR - 2


NEAR = (1, 3, 2)


class Arrivals:
    def finish(self):
        for cp in self.sent:
            cp.wait_send()

    def place(self, n):
        i, p = n // 2, n % 2
        j = i + (i // 2) * (1 - 2 * (i % 2))
        return i, p, j, (self.c + p * (1 - 2 * self.c), (self.v * (1 - p) + self.a * p + NA - j) % NA)

    def take(self, n):
        i, p, j, cv = self.place(n)

        @pl.when((p == 0) & (i > 0))
        def _():
            self.one_in(j)
            self.to_c(j).start()
        pl.when(p == 1)(lambda: self.to_c(j).wait_recv())
        return cv


class Gather(Arrivals):
    SEMS = [DMA, DMA((2,)), DMA, DMA((3,)), DMA, DMA((AO,)), DMA, DMA((NA,))]
    WAVE = (1, 4, 3)

    def __init__(self, buf, sems):
        z, y, x, c, v, a = coords()
        sz, rz, s2, r2, s1, r1, sd, rd = sems
        to_c, to_z, to_1, to_2 = peers()
        self.c, self.v, self.a = c, v, a
        blk = lambda d, j: buf.at[c, v, (z + NZ - d) % NZ, (a + NA - j) % NA]
        chunk = lambda j: buf.at[c, (v + NA - j) % NA]
        self.to_z = lambda k: rcopy(blk(0, 0), blk(0, 0), sz, rz.at[jnp.minimum(k, NZ - k) // 3], to_z(k)).start()
        self.to_2 = lambda w, d: [rcopy(blk(d, 0), blk(d, 0), s2, r2.at[w], to_2(k)).start() for k in NEAR]
        self.to_1 = lambda d, js: [rcopy(blk(d, j), blk(d, j), s1, r1.at[k - 1], to_1(k)).start() for j in js for k in NEAR]
        self.to_c = lambda j: rcopy(chunk(j), chunk(j), sd, rd.at[j], to_c)
        every = lambda ref, ss, rs: rcopy(ref, ref, ss, rs, to_c)
        self.z_in = lambda w: every(buf.at[c, v, pl.ds(0, self.WAVE[w]), a], sz, rz.at[w - 1]).wait_recv()
        self.two_in = lambda w: every(buf.at[c, v, pl.ds(0, (1, AO, AO)[w]), pl.ds(0, (AO, NA, AO)[w])], s2, r2.at[w]).wait_recv()
        self.one_in = lambda k: every(chunk(k), s1, r1.at[k - 1]).wait_recv()
        self.sent = [every(buf.at[c, v, pl.ds(0, ZO), a], sz, rz.at[0]), every(buf.at[c, v, :, pl.ds(0, AO)], s2, r2.at[0]),
                     every(buf.at[c, pl.ds(0, AO)], s1, r1.at[0]), every(buf.at[c], sd, rd.at[0])]

    def each(self, w, f):
        if w == 0:
            f(0)
        else:
            pl.loop(0, self.WAVE[w])(lambda i: f((2 * w - 1 + i // 2) * (1 - 2 * (i % 2))) and None)

    def start(self):
        pl.loop(1, NZ)(self.to_z)
        self.to_2(0, 0)
        self.to_1(0, (0,))

    def column(self, w):
        self.z_in(w)
        self.each(w, lambda d: self.to_2(w, d) + self.to_1(d, (0,)))

    def rest(self, w):
        self.two_in(w)
        self.each(w, lambda d: self.to_1(d, NEAR))


class GatherSmall(Arrivals):
    SEMS = [DMA] * 5 + [DMA((AO,)), DMA, DMA((NA,))]

    def __init__(self, buf, sems):
        z, y, x, c, v, a = coords()
        sz, rz, s2, r2, s1, r1, sd, rd = sems
        to_c, to_z, to_1, to_2 = peers()
        self.c, self.v, self.a = c, v, a
        own, col = buf.at[c, v, z, a], buf.at[c, v, :, a]
        chunk = lambda j: buf.at[c, (v + NA - j) % NA]
        every = lambda ref, ss, rs: rcopy(ref, ref, ss, rs, to_c)
        self.to_z = lambda k: rcopy(own, own, sz, rz, to_z(k)).start()
        self.to_2 = lambda: [rcopy(col, col, s2, r2, to_2(k)).start() for k in NEAR]
        self.to_1 = lambda: [rcopy(chunk(0), chunk(0), s1, r1.at[k - 1], to_1(k)).start() for k in NEAR]
        self.to_c = lambda j: rcopy(chunk(j), chunk(j), sd, rd.at[j], to_c)
        self.z_in = every(buf.at[c, v, pl.ds(0, ZO), a], sz, rz)
        self.two_in = every(buf.at[c, v, :, pl.ds(0, AO)], s2, r2)
        self.one_in = lambda k: every(chunk(k), s1, r1.at[k - 1]).wait_recv()
        self.sent = [every(buf.at[c, pl.ds(0, AO)], s1, r1.at[0]), every(buf.at[c], sd, rd.at[0])]

    def start(self):
        pl.loop(1, NZ)(self.to_z)

    def second(self):
        self.z_in.wait()
        self.to_2()

    def first(self):
        self.two_in.wait()
        self.to_1()
        self.to_c(0).start()


class GatherFeatures:
    SEMS = [DMA] * 4 + [DMA, DMA((ZO,)), DMA, DMA((ZO,)), DMA, DMA]

    def __init__(self, buf, sems, src):
        z, y, x, c, v, a = coords()
        s2, r2, s1, r1, sr, rr, sl, rl, sd, rd = sems
        to_c, to_z, to_1, to_2 = peers()
        at = lambda d: buf.at[c, (z + 2 * NZ + d) % NZ]
        own = at(0).at[v // 2, v % 2]
        self.own = own.at[a]
        self.two = lambda: [rcopy(src, own.at[a], s2, r2, to_2(k)).start() for k in NEAR]
        self.one = lambda: [rcopy(own, own, s1, r1, to_1(k)).start() for k in NEAR]
        every = lambda ref, ss, rs: rcopy(ref, ref, ss, rs, to_c)
        self.two_all = every(own.at[pl.ds(0, AO)], s2, r2)
        self.one_all = every(buf.at[c, pl.ds(0, AO), 0, 0], s1, r1)
        self.right = lambda s, h: rcopy(at(1 - s).at[h], at(1 - s).at[h], sr, rr.at[2 * s - 2 + (h if s < NA else 0)], to_z(1))
        self.left = lambda s, h: rcopy(at(s - 1).at[h], at(s - 1).at[h], sl, rl.at[2 * s - 2 + (h if s < NA else 0)], to_z(ZO))
        self.share = lambda ref: rcopy(ref, ref, sd, rd, to_c).start()
        self.at = at
        halves = buf.at[c].reshape((2 * NZ,) + buf.shape[3:])
        self.sent = [every(halves.at[pl.ds(0, ZO)], m, rd) for m in (sr, sl)] + [every(buf.at[c], sd, rd)]
        self.shared = every(buf.at[c], sd, rd)

    def plane(self):
        self.two_all.wait()
        self.one()

    def ring(self):
        self.one_all.wait()
        self.share(self.at(0))
        for h in range(2):
            self.right(1, h).start()
            self.left(1, h).start()

    def move(self, s, h):
        self.right(s, h).wait_recv()
        self.left(s, h).wait_recv()
        if s < 3 or h == 0:
            self.right(s + 1, h).start()
        if s < 3 or h == 1:
            self.left(s + 1, h).start()
        self.share(self.at(-s).at[h])
        self.share(self.at(s).at[h])

    def last(self):
        self.right(NA, 0).wait_recv()
        self.left(NA, 1).wait_recv()
        self.share(self.at(NA))

    def finish(self):
        for cp in self.sent:
            cp.wait_send()


def tree(parts):
    while len(parts) > 1:
        parts = [p + q for p, q in zip(parts[::2], parts[1::2])]
    return parts.pop()


def iota(shape, dim):
    return lax.broadcasted_iota(jnp.int32, shape, dim)


def lane_sum(m):
    return jnp.sum(m, axis=1, keepdims=True)


def lane_max(m):
    return jnp.max(m, axis=1, keepdims=True)


def ones_at(hit):
    return jnp.where(hit, 1.0, 0.0)


def to_col(row):
    return jnp.transpose(jnp.broadcast_to(row, (LN, LN)))


def logq_rows(cid_v, lq_v, lqr_ref, base):
    @pl.loop(0, lqr_ref.shape[1] // LN, unroll=4)
    def _(i):
        blk = pl.multiple_of(i * LN, LN)
        rid = iota((LN, LN), 0) + (base + blk)
        acc = jnp.zeros((LN, LN), F32)
        for q in range(cid_v.shape[0]):
            acc += jnp.where(cid_v[q:q + 1, :] == rid, lq_v[q:q + 1, :], 0.0)
        lqr_ref[:, pl.ds(blk, LN)] = jnp.transpose(jnp.broadcast_to(lane_sum(acc), (LN, LN)))[:8]


def target_cols(yblk, base, yl_ref, row, d_ref):
    lane = iota((LN, LN), 1).astype(F32)
    group = iota((1, LN), 1) // TD
    for g in range(GR):
        yr = sum(jnp.where(group == b, yblk(g * 8 + b), 0) for b in range(8)) - base
        yl_ref[pl.ds(row + g, 1), :] = yr
        d_ref[g * LN:(g + 1) * LN, :] = to_col(yr.astype(F32)) - lane


def scores_chunk(h, emb_ref, lqr_ref, e_ref, d_ref, mcol_ref, zcol_ref, scol_ref):
    rows = emb_ref.shape[0]
    RB = PZ
    for j in range(0, rows, DIM):
        s = lax.dot_general(h, emb_ref[j:j + DIM, :], COLS, preferred_element_type=F32)
        for rb in range(0, CH, RB):
            rs = slice(rb, rb + RB)
            m = mcol_ref[rs, :] if j else jnp.full((RB, LN), NEG, F32)
            zc = zcol_ref[rs, :] if j else jnp.full((RB, LN), NEG, F32)
            d = d_ref[rs, :]
            for k in (0, LN):
                raw = s[rs, k:k + LN]
                hit = d == float(j + k)
                zc = jnp.where(hit, raw, zc)
                val = jnp.where(hit, -1e9, raw - lqr_ref[:1, j + k:j + k + LN])
                e_ref[rs, j + k:j + k + LN] = val
                m = jnp.maximum(m, val)
            mcol_ref[rs, :] = m
            zcol_ref[rs, :] = zc
    for rb in range(0, CH, RB):
        rs = slice(rb, rb + RB)
        zc = lane_max(zcol_ref[rs, :])
        m = jnp.maximum(lane_max(mcol_ref[rs, :]), zc)
        zcol_ref[rs, :] = jnp.broadcast_to(zc, (RB, LN))
        mcol_ref[rs, :] = jnp.broadcast_to(m, (RB, LN))

    def grp(g, _):
        rs = pl.ds(pl.multiple_of(g * RB, RB), RB)
        m = mcol_ref[rs, :]
        tot = jnp.zeros((RB, LN), F32)
        for k in range(0, rows, LN):
            ex = jnp.exp(e_ref[rs, k:k + LN] - m)
            e_ref[rs, k:k + LN] = ex
            tot += ex
        scol_ref[rs, :] = tot
        return 0
    lax.fori_loop(0, CH // RB, grp, 0)
    for rb in range(0, CH, RB):
        rs = slice(rb, rb + RB)
        tot = lane_sum(scol_ref[rs, :])
        scol_ref[rs, :] = jnp.broadcast_to(tot, (RB, LN)) + jnp.exp(zcol_ref[rs, :] - mcol_ref[rs, :])


def reduce_stats(pb, rb, zb, ab, st, sems, fill):
    z, y, x, c, v, a = coords()
    to_c, to_z, to_1, to_2 = peers()
    sp, rp, sz, rz, sa, ra = sems
    me = (y * NX + x) * 2 + c

    def merge(ref):
        m, s = ref[:, 0, :], ref[:, 1, :]
        top = jnp.max(m, axis=0, keepdims=True)
        return top, jnp.sum(s * jnp.exp(m - top), axis=0, keepdims=True), jnp.max(ref[:, 2, :], axis=0, keepdims=True)

    rb[me] = pb[me]
    pl.loop(1, SR)(lambda k: rcopy(pb.at[(me + k) % SR], rb.at[me], sp, rp, in_plane(k)).start())
    fill(0)
    rcopy(rb.at[pl.ds(0, PO)], rb.at[pl.ds(0, PO)], sp, rp, to_c).wait()
    for i, val in enumerate(merge(rb)):
        zb[z, i:i + 1, :] = val
    pl.loop(1, NZ)(lambda k: rcopy(zb.at[z], zb.at[z], sz, rz, to_z(k)).start())
    fill(1)
    rcopy(zb.at[pl.ds(0, ZO)], zb.at[pl.ds(0, ZO)], sz, rz, to_c).wait()
    m, s, t = merge(zb)
    ab[me, 0:1, :] = m + jnp.log(s)
    ab[me, 1:2, :] = t
    pl.loop(1, SR)(lambda k: rcopy(ab.at[me], ab.at[me], sa, ra, in_plane(k)).start())
    fill(2)
    rcopy(ab.at[pl.ds(0, PO)], ab.at[pl.ds(0, PO)], sa, ra, to_c).wait()
    st[1] = ab[:, 0, :]
    st[2] = ab[:, 1, :]
    return jnp.sum(ab[:, 0, :] - ab[:, 1, :]) * PER_TOKEN


def gelu_both(u):
    k0, k1 = math.sqrt(2.0 / math.pi), 0.044715
    sq = u * u
    t = jnp.tanh(k0 * (u + k1 * (sq * u)))
    cdf = 0.5 * (1.0 + t)
    return u * cdf, cdf + (0.5 * k0) * u * ((1.0 - t * t) * (1.0 + (3.0 * k1) * sq))


def step_kernel(x_hbm, win_hbm, wout_hbm, emb_hbm, cid_hbm, lq_hbm, y_s,
                loss_ref, de_hbm, gwi_hbm, gwo_hbm, h_hbm, st_hbm, lh_hbm, li_hbm, lg_hbm, xg,
                xv, win, wout, emb, cid_v, lq_v, lqr, hb, yb, dh,
                eb, pb, det, te, dcol, mcol, zcol, scol, yl, st, lh, li, lg, pst, rst, zst, ast,
                dq, rc, a0, ra, a1, rb, zb,
                lsem, osem, fsem, xsem, *sems):
    z, y, x, c, v, a = coords()
    to_c, to_z, to_1, to_2 = peers()
    rows = emb.shape[0]
    hid = win.shape[1]
    half = hid // 2
    me = lax.axis_index("dp")
    base = me * rows
    take = lambda n, it=iter(sems): [next(it) for _ in range(n)]
    gh, gd, gy = (take(len(Gather.SEMS)) for _ in range(3))
    gx = take(len(GatherFeatures.SEMS))
    own16 = pl.ds(me * TD, TD)
    loads = [pltpu.make_async_copy(s, d, lsem.at[i]) for i, (s, d) in enumerate((
        (x_hbm, xv), (win_hbm, win), (wout_hbm, wout), (emb_hbm, emb), (cid_hbm.at[own16], cid_v), (lq_hbm.at[own16], lq_v)))]
    for cp in loads[:2]:
        cp.start()
    bar, n_peers = signal_peers()
    for cp in loads[2:]:
        cp.start()

    for cp in loads[:3]:
        cp.wait()
    pre = jnp.dot(xv[...], win[...], preferred_element_type=F32)
    act = gelu_both(pre)[0].astype(BF16)
    hb[c, v, z, a] = jnp.dot(act, wout[...], preferred_element_type=F32).astype(BF16)
    lane16 = iota((1, LN), 1) % TD
    yb[c, v, z, a] = sum(jnp.where(lane16 == i, y_s[i], 0) for i in range(TD))
    pl.semaphore_wait(bar, n_peers)

    gath, gaty, gatx, gatd = Gather(hb, gh), GatherSmall(yb, gy), GatherFeatures(xg, gx, xv), Gather(dh, gd)
    xown = pltpu.make_async_copy(xv, gatx.own, xsem.at[0])
    gath.start()
    gaty.start()
    xown.start()
    gatx.two()
    for cp in loads[3:]:
        cp.wait()
    logq_rows(cid_v, lq_v, lqr, base)
    det[...] = jnp.zeros_like(det)
    gath.column(1)
    gath.rest(0)
    xown.wait()
    gatx.plane()
    gath.column(2)
    gaty.second()
    gath.rest(1)
    gath.rest(2)
    gath.to_c(0).start()
    gaty.first()

    lane = iota((LN, LN), 1)

    def score(cc, vv):
        ci = cc * NA + vv
        target_cols(lambda b: yb[cc, vv, b // NA, b % NA], base, yl, ci * GR, dcol.at[ci])
        scores_chunk(hb[cc, vv].reshape(CH, DIM), emb, lqr, eb.at[ci], dcol.at[ci], mcol.at[ci], zcol.at[ci], scol)
        for b in range(GR):
            bs_ = slice(b * LN, (b + 1) * LN)
            three = jnp.where(lane == 0, mcol[ci, bs_, :], jnp.where(lane == 1, scol[bs_, :], zcol[ci, bs_, :]))
            pst[ci * GR + b] = jnp.transpose(three)[:NA]

    @pl.loop(0, NC)
    def _(n):
        gaty.take(n)
        cv = gath.take(n)
        pl.when(n == 1)(gatx.ring)
        pl.when(n == 4)(lambda: gatx.move(1, 0))
        pl.when(n == NC_LAST)(lambda: gatx.move(1, 1))
        score(*cv)

    def target_rows(lo, hi):
        @pl.loop(lo, hi)
        def _(ci):
            for q in range(0, rows, LN):
                pb[:, q:q + LN] = ones_at(dcol[ci] == float(q)).astype(BF16)
            te[ci] = jnp.dot(pb[...], emb[...], preferred_element_type=F32).astype(BF16)

    def fill(n):
        if n:
            gatx.move(2, n - 1)
        target_rows(*((0, 3), (3, 6), (6, NC))[n])

    lr = st.at[1]
    loss_ref[0, 0] = reduce_stats(pst, rst, zst, ast, st, take(6), fill)
    @pl.loop(0, NC)
    def _(ci):
        for b in range(GR):
            bs_ = slice(b * LN, (b + 1) * LN)
            lc = to_col(lr[pl.ds(ci * GR + b, 1), :])
            mcol[ci, bs_, :] = jnp.exp(mcol[ci, bs_, :] - lc) * PER_TOKEN
            zc = zcol[ci, bs_, :]
            zcol[ci, bs_, :] = jnp.where(zc > NEG, (jnp.exp(zc - lc) - 1.0) * PER_TOKEN, 0.0)
    st[0] = yl[...].astype(F32)

    sc, rcs, sa, ras, sb, rbs, sz, rzs = take(8)
    ring = a0.shape[0]
    c_copy = lambda k: rcopy(dq.at[k % 2, 1 - c], rc.at[k], sc.at[k % 2], rcs.at[k], to_c)
    a_copy = lambda k, j: rcopy(a0.at[k % ring, (v + j) % NA], ra.at[k, v], sa.at[k % ring], ras.at[k], to_1(j))
    a_all = lambda k: rcopy(ra.at[k, pl.ds(0, AO)], ra.at[k, pl.ds(0, AO)], sa.at[k % ring], ras.at[k], to_c)
    b_copy = lambda k, j: rcopy(a1.at[k % ring, (a + j) % NA], rb.at[k, a], sb.at[k % ring], rbs.at[k], to_2(j))
    b_all = lambda k: rcopy(rb.at[k, pl.ds(0, AO)], rb.at[k, pl.ds(0, AO)], sb.at[k % ring], rbs.at[k], to_c)

    def off(k):
        s = (k + 1) // 2
        return NA + s - 2 * s * (k % 2)

    z_copy = lambda k: rcopy(zb.at[NZ + k], zb.at[z], sz, rzs, to_z(off(k)))

    def compute(k):
        zz = (z + off(k)) % NZ
        piece = pl.ds(pl.multiple_of(zz * PZ, PZ), PZ)
        for ci in range(NC):
            ps = slice(ci * PZ, (ci + 1) * PZ)
            f = mcol[ci, piece, :]
            for q in range(0, rows, LN):
                pb[ps, q:q + LN] = (eb[ci, piece, q:q + LN] * f).astype(BF16)
        h = jnp.concatenate([hb[ci // NA, ci % NA, zz].reshape(PZ, DIM) for ci in range(NC)], axis=0)
        for q in range(0, rows, CH):
            det[:, q:q + CH] += lax.dot_general(h, pb[:, q:q + CH], ROWS, preferred_element_type=F32)
        out = jnp.dot(pb[...], emb[...], preferred_element_type=F32)
        for ci in range(NC):
            g = zcol[ci, piece, :]
            t = te[ci, piece, :].astype(F32)
            for hf in (0, LN):
                dq[k % 2, ci // NA, ci % NA, :, hf:hf + LN] = out[ci * PZ:(ci + 1) * PZ, hf:hf + LN] + g * t[:, hf:hf + LN]
        c_copy(k).start()

    def sum_core(k):
        c_copy(k).wait()
        a0[k % ring] = dq[k % 2, c] + rc[k]
        for j in NEAR:
            a_copy(k, j).start()

    def sum_first(k):
        a_all(k).wait()
        ra[k, v] = a0[k % ring, v]
        a1[k % ring] = tree([ra[k, i] for i in range(NA)]).reshape(NA, TD, DIM)
        for j in NEAR:
            b_copy(k, j).start()

    def sum_second(k, last=False):
        b_all(k).wait()
        rb[k, a] = a1[k % ring, a]
        val = tree([rb[k, i] for i in range(NA)])
        if last:
            zb[z] = val
        else:
            zb[NZ + k] = val
            z_copy(k).start()

    def body(k, _):
        compute(k)
        for lag, f in ((1, sum_core), (4, sum_first), (6, sum_second)):
            pl.when(k >= lag)(functools.partial(f, k - lag))
        pl.when(k == 0)(lambda: gatx.move(3, 0))
        pl.when(k == 1)(lambda: gatx.move(3, 1))
        pl.when(k == 7)(gatx.last)
        return 0

    lax.fori_loop(0, NZ, body, 0)
    de = eb.at[pl.ds(4, 4), :, pl.ds(DIM * 4, DIM)]
    for q in range(0, rows, LN):
        for w in (0, LN):
            de[q // CH, q % CH:q % CH + LN, w:w + LN] = jnp.transpose(det[w:w + LN, q:q + LN])
    outs = [pltpu.make_async_copy(s, d, osem.at[i]) for i, (s, d) in enumerate(((de, de_hbm.reshape(4, CH, DIM)), (hb, h_hbm), (st, st_hbm), (lh, lh_hbm), (li, li_hbm), (lg, lg_hbm)))]
    for cp in outs[:3]:
        cp.start()

    cols = pl.ds(pl.multiple_of(c * half, half), half)
    def xs(ci, slot, go):
        to = pl.ds(pl.multiple_of(slot * hid, hid), hid)
        if go:
            for zz in range(NZ):
                src = xg.at[ci // NA, zz, (ci % NA) // 2, ci % 2].reshape(PZ, hid)
                pltpu.make_async_copy(src, pb.at[pl.ds(zz * PZ, PZ), to], fsem.at[slot]).start()
        else:
            pltpu.make_async_copy(pb.at[:, to], pb.at[:, to], fsem.at[slot]).wait()

    def tower(ci, slot):
        pre = jnp.dot(pb[:, pl.ds(pl.multiple_of(slot * hid, hid), hid)], win[:, cols], preferred_element_type=F32)
        act, der = gelu_both(pre)
        eb[ci, :, :half] = der
        eb[ci, :, half:2 * half] = act.astype(BF16).astype(F32)

    ordinal = lambda n: gatd.place(n)[3][0] * NA + gatd.place(n)[3][1]

    def towers(lo, hi):
        @pl.loop(lo, hi)
        def _(n):
            pl.when(n + 1 < NC)(lambda: xs(ordinal(n + 1), (n + 1) % 2, True))
            xs(ordinal(n), n % 2, False)
            tower(ordinal(n), n % 2)

    sum_first(4)
    sum_core(7)
    sum_second(2)
    sum_second(3)
    gatx.shared.wait_recv()
    xs(ordinal(0), 0, True)
    sum_first(5)
    towers(0, 1)
    sum_first(6)
    sum_second(4)
    towers(1, 2)
    sum_first(7)
    sum_second(5)
    towers(2, 3)
    sum_second(6)
    sum_second(7, last=True)
    towers(3, 4)
    rcopy(zb.at[pl.ds(0, ZO)], zb.at[pl.ds(0, ZO)], sz, rzs, to_c).wait()
    tot = tree([zb[i] for i in range(NZ)])
    dh[c, v, z, a] = tot.astype(BF16)
    gatd.start()
    towers(4, 6)
    gatd.column(1)
    gatd.rest(0)
    gatd.column(2)
    towers(6, 7)
    gatd.rest(1)
    towers(7, NC)
    xs(ordinal(0), 0, True)
    gatd.rest(2)
    gatd.to_c(0).start()
    rank, gfac, _ = target_ranks(st, rows)
    target_page(0, st, rank, gfac, lambda r: token_rows(hb, r), lh, li, lg)
    for cp in outs[3:6]:
        cp.start()
    acc_i, acc_o = eb.at[pl.ds(0, 2), :, pl.ds(2 * half, half)], eb.at[2, :, pl.ds(2 * half, DIM)]
    acc_i[...] = jnp.zeros(acc_i.shape, F32)
    acc_o[...] = jnp.zeros(acc_o.shape, F32)

    so, ro = take(2)
    mine = [(acc_o, gwo_hbm.at[cols])] + [(acc_i.at[r], gwi_hbm.at[pl.ds(r * half, half), cols]) for r in range(2)]
    ends = [rcopy(s, d, so.at[i], ro.at[i], to_c) for i, (s, d) in enumerate(mine)]
    outs += [pltpu.make_async_copy(s, d, osem.at[6 + i]) for i, (s, d) in enumerate(mine)]
    early, late = ends[:2] + outs[6:8], ends[2:] + outs[8:]

    def weights(ci, slot, last=False):
        g = dh[ci // NA, ci % NA].reshape(CH, DIM)
        back = lax.dot_general(g, wout[cols, :], COLS, preferred_element_type=F32)
        da = (eb[ci, :, :half] * back).astype(BF16)
        act = eb[ci, :, half:2 * half].astype(BF16)
        acc_o[...] += lax.dot_general(act, g, ROWS, preferred_element_type=F32)
        for r in range(2):
            xr = pb[:, pl.ds(pl.multiple_of(slot * hid + r * half, half), half)]
            acc_i[r] += lax.dot_general(xr, da, ROWS, preferred_element_type=F32)
            if last and r == 0:
                for cp in early:
                    cp.start()

    @pl.loop(0, NC_LAST)
    def _(n):
        gatd.take(n)
        xs(ordinal(n + 1), (n + 1) % 2, True)
        xs(ordinal(n), n % 2, False)
        weights(ordinal(n), n % 2)

    gatd.take(NC_LAST)
    xs(ordinal(NC_LAST), NC_LAST % 2, False)
    weights(ordinal(NC_LAST), NC_LAST % 2, last=True)

    for g in (gath, gaty, gatx, gatd):
        g.finish()
    for cp in late:
        cp.start()
    for cp in ends + outs:
        cp.wait()


def step(features, w_in, w_out, table, cand_ids, log_q, targets):
    rows, dim = table.shape
    hid = w_in.shape[1]
    A, S = (pl.BlockSpec(memory_space=m) for m in (pl.ANY, pltpu.SMEM))
    sds = jax.ShapeDtypeStruct
    vm = pltpu.VMEM
    tokens = (2, NA, NZ, NA, TD)
    stat = lambda n: vm((n, NA, LN), F32)
    col = vm((NC, CH, LN), F32)
    return pl.pallas_call(
        step_kernel, name="step",
        out_shape=(sds((1, 1), F32), sds((rows, dim), F32), sds((w_in.shape[0], hid), F32), sds((hid, dim), F32), sds(tokens + (dim,), BF16),
                   sds((3, SR, LN), F32), sds((LN, dim), F32), sds((8, LN), jnp.int32), sds((8, LN), F32), sds((2, NZ, 2, 2, NA, TD, w_in.shape[0]), BF16)),
        in_specs=[A] * 6 + [S], out_specs=(S,) + (A,) * 9,
        scratch_shapes=[
            vm(features.shape, BF16), vm(w_in.shape, BF16), vm(w_out.shape, BF16), vm(table.shape, BF16), vm((TD, LN), jnp.int32), vm((TD, LN), F32),
            vm((8, rows), F32), vm(tokens + (dim,), BF16), vm((2, NA, NZ, NA, 1, LN), jnp.int32), vm(tokens + (dim,), BF16),
            vm((NC, CH, rows), F32), vm((CH, rows), BF16), vm((dim, rows), F32), vm((NC, CH, dim), BF16), col, col, col, vm((CH, LN), F32),
            vm((SR, LN), jnp.int32), vm((3, SR, LN), F32), vm((LN, dim), F32), vm((8, LN), jnp.int32), vm((8, LN), F32),
            stat(SR), stat(SR), stat(NZ), stat(SR),
            vm((2, 2, NA, PZ, dim), F32), vm((NZ, NA, PZ, dim), F32), vm((4, NA, PZ, dim), F32), vm((NZ, NA, PZ, dim), F32),
            vm((4, NA, TD, dim), F32), vm((NZ, NA, TD, dim), F32), vm((2 * NZ, TD, dim), F32),
            DMA((6,)), DMA((9,)), DMA((2,)), DMA((1,))] + Gather.SEMS * 2 + GatherSmall.SEMS + GatherFeatures.SEMS + [
            DMA] * 6 + [DMA((2,)), DMA((NZ,)), DMA((4,)), DMA((NZ,)), DMA((4,)), DMA((NZ,)), DMA, DMA, DMA((3,)), DMA((3,))],
        compiler_params=pltpu.CompilerParams(collective_id=0, has_side_effects=True, vmem_limit_bytes=VMEM_ALL),
    )(features, w_in, w_out, table, cand_ids.reshape(-1, LN), log_q.reshape(-1, LN), targets)


def target_ranks(st, rows):
    own = (st[0] >= 0) & (st[0] < rows)
    g = jnp.where(own, (jnp.exp(jnp.where(own, st[2], 0.0) - st[1]) - 1.0) * PER_TOKEN, 0.0)
    of = ones_at(own)
    before = lambda n, i, j: jnp.where(iota((n, n), i) < iota((n, n), j), 1.0, 0.0).astype(BF16)
    pre = jnp.dot(of.astype(BF16), before(LN, 0, 1), preferred_element_type=F32)
    tot = jnp.broadcast_to(lane_sum(of), (SR, LN))
    return jnp.where(own, pre + jnp.dot(before(SR, 1, 0), tot.astype(BF16), preferred_element_type=F32), -1.0), g, jnp.sum(of)


def target_page(p, st, rank, g, h_row, out_h, out_i, out_g):
    slot = (iota((LN, LN), 0) + p * LN).astype(F32)
    rr, gg = jnp.zeros((LN, LN), F32), jnp.zeros((LN, LN), F32)
    hh = jnp.zeros((LN, DIM), F32)
    for r in range(SR):
        rw = slice(r, r + 1)
        hit = rank[rw] == slot
        rr += jnp.where(hit, st[0, rw], 0.0)
        gg += jnp.where(hit, g[rw], 0.0)
        hh += jnp.dot(ones_at(hit).astype(BF16), h_row(r), preferred_element_type=F32)
    row = lambda m: jnp.transpose(jnp.broadcast_to(lane_sum(m), (LN, LN)))[:8]
    out_i[...] = row(rr).astype(jnp.int32)
    out_g[...] = row(gg)
    out_h[...] = hh


def token_rows(h, r):
    ci, g = r // GR, r % GR
    return h[ci // NA, ci % NA, 2 * g:2 * g + 2].reshape(LN, DIM)


def fix_kernel(de_hbm, h_hbm, st_hbm, lh_hbm, li_hbm, lg_hbm, gwi_hbm, gwo_hbm, out_hbm, wi_hbm, wo_hbm,
               de, h, st, wi, wo, lh, li, lg, si, sg, sem):
    rows = de.shape[0]
    pairs = ((st_hbm, st), (li_hbm, si), (lg_hbm, sg), (lh_hbm, lh), (de_hbm, de), (gwi_hbm, wi), (gwo_hbm, wo), (de, out_hbm), (wi, wi_hbm), (wo, wo_hbm))
    ins = [pltpu.make_async_copy(s, d, sem.at[i]) for i, (s, d) in enumerate(pairs)]
    outs = ins[7:]
    for cp in ins[:7]:
        cp.start()
    ins[0].wait()
    own = (st[0] >= 0) & (st[0] < rows)
    n = jnp.sum(ones_at(own)).astype(jnp.int32)
    for i in (6, 5):
        ins[i].wait()
        ins[i + 3].start()
    for cp in ins[1:5]:
        cp.wait()

    def page(p, _):
        @pl.when(p > 0)
        def _():
            run([pltpu.make_async_copy(h_hbm, h, sem.at[0])])
            rank, g, _ = target_ranks(st, rows)
            target_page(p, st, rank, g, lambda r: token_rows(h, r), lh, li, lg)
            run([pltpu.make_async_copy(li, si, sem.at[1]), pltpu.make_async_copy(lg, sg, sem.at[2])])

        @pl.loop(0, jnp.minimum(n - p * LN, LN))
        def _(i):
            de[pl.ds(si[0, i], 1), :] += sg[0, i] * lh[pl.ds(i, 1), :]
        return 0
    lax.fori_loop(0, (n + LN - 1) // LN, page, 0)
    outs[0].start()
    for cp in outs:
        cp.wait()


def fix(de, h, st, lh, li, lg, gwi, gwo):
    A = pl.BlockSpec(memory_space=pl.ANY)
    vm = lambda m: pltpu.VMEM(m.shape, m.dtype)
    like = lambda m: jax.ShapeDtypeStruct(m.shape, F32)
    return pl.pallas_call(
        fix_kernel, name="fix", out_shape=(like(de), like(gwi), like(gwo)), in_specs=[A] * 8, out_specs=(A,) * 3,
        scratch_shapes=[vm(de), vm(h), vm(st), vm(gwi), vm(gwo), vm(lh), vm(li), vm(lg), pltpu.SMEM(li.shape, jnp.int32), pltpu.SMEM(lg.shape, F32), DMA((10,))],
        compiler_params=pltpu.CompilerParams(vmem_limit_bytes=VMEM_ALL),
    )(de, h, st, lh, li, lg, gwi, gwo)


def solution(mesh):
    def local_step(*args):
        loss, de, gwi, gwo, *rest, _ = step(*args)
        return loss.reshape(()), *fix(de, *rest, gwi, gwo)

    return jax.shard_map(local_step, mesh=mesh, in_specs=(P("dp", None), P(), P(), P("dp", None), P(), P(), P("dp")), out_specs=(P(), P("dp", None), P(), P()), check_vma=False)
```

```python
import functools
import math
import jax
import jax.numpy as jnp
from jax import lax
from jax.experimental import pallas as pl
from jax.experimental.pallas import tpu as pltpu
from jax.sharding import PartitionSpec as P

NZ, NY, NX = 8, 4, 4
NA = 4
LN = 128
TD = 16
NC = 2 * NA
CH = NZ * NA * TD
NT = NC * CH
PZ = NA * TD
SR = NT // LN
GR = CH // LN
F32, BF16 = jnp.float32, jnp.bfloat16
NEG = -jnp.inf
PER_TOKEN = 1.0 / NT
ZO, AO, PO = NZ - 1, NA - 1, SR - 1
DIM = 2 * LN
NC_LAST = NC - 1
VMEM_ALL = 67043328
MESH = pl.DeviceIdType.MESH
ROWS, COLS = (((0,), (0,)), ((), ())), (((1,), (1,)), ((), ()))
DMA = pltpu.SemaphoreType.DMA


def coords():
    me = lax.axis_index("dp")
    z, y, x, c = me // (NY * NX * 2), (me // (NX * 2)) % NY, (me // 2) % NX, me % 2
    return z, y, x, c, x * (1 - c) + y * c, y * (1 - c) + x * c


def dev(z, y, x, c):
    return (((z * NY + y) * NX + x) * 2 + c,)


def peers():
    z, y, x, c, v, a = coords()
    me = lax.axis_index("dp")
    one = {k: dev(z, (y + k * c) % NY, (x + k * (1 - c)) % NX, c) for k in range(1, NA)}
    two = {k: dev(z, (y + k * (1 - c)) % NY, (x + k * c) % NX, c) for k in range(1, NA)}
    return (me + 1 - 2 * c,), lambda k: ((me + k * SR) % (NZ * SR),), one.get, two.get


def in_plane(k):
    me = lax.axis_index("dp")
    return (me // SR * SR + (me + k) % SR,)


def rcopy(src, dst, ssem, rsem, to):
    return pltpu.make_async_remote_copy(src_ref=src, dst_ref=dst, send_sem=ssem, recv_sem=rsem, device_id=to, device_id_type=MESH)


def run(copies):
    for cp in copies:
        cp.start()
    for cp in copies:
        cp.wait()


def signal_peers():
    bar = pltpu.get_barrier_semaphore()
    to_c, to_z, to_1, to_2 = peers()
    z, y, x, c, v, a = coords()
    tell = lambda p: pl.semaphore_signal(bar, inc=1, device_id=p, device_id_type=MESH)
    pl.loop(1, NZ)(lambda k: tell(to_z(k)))
    pl.loop(1, SR)(lambda k: tell(in_plane(k)))
    return bar, NZ + SR - 2


NEAR = (1, 3, 2)


class Arrivals:
    def finish(self):
        for cp in self.sent:
            cp.wait_send()

    def place(self, n):
        i, p = n // 2, n % 2
        j = i + (i // 2) * (1 - 2 * (i % 2))
        return i, p, j, (self.c + p * (1 - 2 * self.c), (self.v * (1 - p) + self.a * p + NA - j) % NA)

    def take(self, n):
        i, p, j, cv = self.place(n)

        @pl.when((p == 0) & (i > 0))
        def _():
            self.one_in(j)
            self.to_c(j).start()
        pl.when(p == 1)(lambda: self.to_c(j).wait_recv())
        return cv


class Gather(Arrivals):
    SEMS = [DMA, DMA((2,)), DMA, DMA((3,)), DMA, DMA((AO,)), DMA, DMA((NA,))]
    WAVE = (1, 4, 3)

    def __init__(self, buf, sems):
        z, y, x, c, v, a = coords()
        sz, rz, s2, r2, s1, r1, sd, rd = sems
        to_c, to_z, to_1, to_2 = peers()
        self.c, self.v, self.a = c, v, a
        blk = lambda d, j: buf.at[c, v, (z + NZ - d) % NZ, (a + NA - j) % NA]
        chunk = lambda j: buf.at[c, (v + NA - j) % NA]
        self.to_z = lambda k: rcopy(blk(0, 0), blk(0, 0), sz, rz.at[jnp.minimum(k, NZ - k) // 3], to_z(k)).start()
        self.to_2 = lambda w, d: [rcopy(blk(d, 0), blk(d, 0), s2, r2.at[w], to_2(k)).start() for k in NEAR]
        self.to_1 = lambda d, js: [rcopy(blk(d, j), blk(d, j), s1, r1.at[k - 1], to_1(k)).start() for j in js for k in NEAR]
        self.to_c = lambda j: rcopy(chunk(j), chunk(j), sd, rd.at[j], to_c)
        every = lambda ref, ss, rs: rcopy(ref, ref, ss, rs, to_c)
        self.z_in = lambda w: every(buf.at[c, v, pl.ds(0, self.WAVE[w]), a], sz, rz.at[w - 1]).wait_recv()
        self.two_in = lambda w: every(buf.at[c, v, pl.ds(0, (1, AO, AO)[w]), pl.ds(0, (AO, NA, AO)[w])], s2, r2.at[w]).wait_recv()
        self.one_in = lambda k: every(chunk(k), s1, r1.at[k - 1]).wait_recv()
        self.sent = [every(buf.at[c, v, pl.ds(0, ZO), a], sz, rz.at[0]), every(buf.at[c, v, :, pl.ds(0, AO)], s2, r2.at[0]),
                     every(buf.at[c, pl.ds(0, AO)], s1, r1.at[0]), every(buf.at[c], sd, rd.at[0])]

    def each(self, w, f):
        if w == 0:
            f(0)
        else:
            pl.loop(0, self.WAVE[w])(lambda i: f((2 * w - 1 + i // 2) * (1 - 2 * (i % 2))) and None)

    def start(self):
        pl.loop(1, NZ)(self.to_z)
        self.to_2(0, 0)
        self.to_1(0, (0,))

    def column(self, w):
        self.z_in(w)
        self.each(w, lambda d: self.to_2(w, d) + self.to_1(d, (0,)))

    def rest(self, w):
        self.two_in(w)
        self.each(w, lambda d: self.to_1(d, NEAR))


class GatherSmall(Arrivals):
    SEMS = [DMA] * 5 + [DMA((AO,)), DMA, DMA((NA,))]

    def __init__(self, buf, sems):
        z, y, x, c, v, a = coords()
        sz, rz, s2, r2, s1, r1, sd, rd = sems
        to_c, to_z, to_1, to_2 = peers()
        self.c, self.v, self.a = c, v, a
        own, col = buf.at[c, v, z, a], buf.at[c, v, :, a]
        chunk = lambda j: buf.at[c, (v + NA - j) % NA]
        every = lambda ref, ss, rs: rcopy(ref, ref, ss, rs, to_c)
        self.to_z = lambda k: rcopy(own, own, sz, rz, to_z(k)).start()
        self.to_2 = lambda: [rcopy(col, col, s2, r2, to_2(k)).start() for k in NEAR]
        self.to_1 = lambda: [rcopy(chunk(0), chunk(0), s1, r1.at[k - 1], to_1(k)).start() for k in NEAR]
        self.to_c = lambda j: rcopy(chunk(j), chunk(j), sd, rd.at[j], to_c)
        self.z_in = every(buf.at[c, v, pl.ds(0, ZO), a], sz, rz)
        self.two_in = every(buf.at[c, v, :, pl.ds(0, AO)], s2, r2)
        self.one_in = lambda k: every(chunk(k), s1, r1.at[k - 1]).wait_recv()
        self.sent = [every(buf.at[c, pl.ds(0, AO)], s1, r1.at[0]), every(buf.at[c], sd, rd.at[0])]

    def start(self):
        pl.loop(1, NZ)(self.to_z)

    def second(self):
        self.z_in.wait()
        self.to_2()

    def first(self):
        self.two_in.wait()
        self.to_1()
        self.to_c(0).start()


class GatherFeatures:
    SEMS = [DMA] * 4 + [DMA, DMA((ZO,)), DMA, DMA((ZO,)), DMA, DMA]

    def __init__(self, buf, sems, src):
        z, y, x, c, v, a = coords()
        s2, r2, s1, r1, sr, rr, sl, rl, sd, rd = sems
        to_c, to_z, to_1, to_2 = peers()
        at = lambda d: buf.at[c, (z + 2 * NZ + d) % NZ]
        own = at(0).at[v // 2, v % 2]
        self.own = own.at[a]
        self.two = lambda: [rcopy(src, own.at[a], s2, r2, to_2(k)).start() for k in NEAR]
        self.one = lambda: [rcopy(own, own, s1, r1, to_1(k)).start() for k in NEAR]
        every = lambda ref, ss, rs: rcopy(ref, ref, ss, rs, to_c)
        self.two_all = every(own.at[pl.ds(0, AO)], s2, r2)
        self.one_all = every(buf.at[c, pl.ds(0, AO), 0, 0], s1, r1)
        self.right = lambda s, h: rcopy(at(1 - s).at[h], at(1 - s).at[h], sr, rr.at[2 * s - 2 + (h if s < NA else 0)], to_z(1))
        self.left = lambda s, h: rcopy(at(s - 1).at[h], at(s - 1).at[h], sl, rl.at[2 * s - 2 + (h if s < NA else 0)], to_z(ZO))
        self.share = lambda ref: rcopy(ref, ref, sd, rd, to_c).start()
        self.at = at
        halves = buf.at[c].reshape((2 * NZ,) + buf.shape[3:])
        self.sent = [every(halves.at[pl.ds(0, ZO)], m, rd) for m in (sr, sl)] + [every(buf.at[c], sd, rd)]
        self.shared = every(buf.at[c], sd, rd)

    def plane(self):
        self.two_all.wait()
        self.one()

    def ring(self):
        self.one_all.wait()
        self.share(self.at(0))
        for h in range(2):
            self.right(1, h).start()
            self.left(1, h).start()

    def move(self, s, h):
        self.right(s, h).wait_recv()
        self.left(s, h).wait_recv()
        if s < 3 or h == 0:
            self.right(s + 1, h).start()
        if s < 3 or h == 1:
            self.left(s + 1, h).start()
        self.share(self.at(-s).at[h])
        self.share(self.at(s).at[h])

    def last(self):
        self.right(NA, 0).wait_recv()
        self.left(NA, 1).wait_recv()
        self.share(self.at(NA))

    def finish(self):
        for cp in self.sent:
            cp.wait_send()


def tree(parts):
    while len(parts) > 1:
        parts = [p + q for p, q in zip(parts[::2], parts[1::2])]
    return parts.pop()


def iota(shape, dim):
    return lax.broadcasted_iota(jnp.int32, shape, dim)


def lane_sum(m):
    return jnp.sum(m, axis=1, keepdims=True)


def lane_max(m):
    return jnp.max(m, axis=1, keepdims=True)


def ones_at(hit):
    return jnp.where(hit, 1.0, 0.0)


def to_col(row):
    return jnp.transpose(jnp.broadcast_to(row, (LN, LN)))


def logq_rows(cid_v, lq_v, lqr_ref, base):
    @pl.loop(0, lqr_ref.shape[1] // LN, unroll=4)
    def _(i):
        blk = pl.multiple_of(i * LN, LN)
        rid = iota((LN, LN), 0) + (base + blk)
        acc = jnp.zeros((LN, LN), F32)
        for q in range(cid_v.shape[0]):
            acc += jnp.where(cid_v[q:q + 1, :] == rid, lq_v[q:q + 1, :], 0.0)
        lqr_ref[:, pl.ds(blk, LN)] = jnp.transpose(jnp.broadcast_to(lane_sum(acc), (LN, LN)))[:8]


def target_cols(yblk, base, yl_ref, row, d_ref):
    lane = iota((LN, LN), 1).astype(F32)
    group = iota((1, LN), 1) // TD
    for g in range(GR):
        yr = sum(jnp.where(group == b, yblk(g * 8 + b), 0) for b in range(8)) - base
        yl_ref[pl.ds(row + g, 1), :] = yr
        d_ref[g * LN:(g + 1) * LN, :] = to_col(yr.astype(F32)) - lane


def scores_chunk(h, emb_ref, lqr_ref, e_ref, d_ref, mcol_ref, zcol_ref, scol_ref):
    rows = emb_ref.shape[0]
    RB = PZ
    for j in range(0, rows, DIM):
        s = lax.dot_general(h, emb_ref[j:j + DIM, :], COLS, preferred_element_type=F32)
        for rb in range(0, CH, RB):
            rs = slice(rb, rb + RB)
            m = mcol_ref[rs, :] if j else jnp.full((RB, LN), NEG, F32)
            zc = zcol_ref[rs, :] if j else jnp.full((RB, LN), NEG, F32)
            d = d_ref[rs, :]
            for k in (0, LN):
                raw = s[rs, k:k + LN]
                hit = d == float(j + k)
                zc = jnp.where(hit, raw, zc)
                val = jnp.where(hit, -1e9, raw - lqr_ref[:1, j + k:j + k + LN])
                e_ref[rs, j + k:j + k + LN] = val
                m = jnp.maximum(m, val)
            mcol_ref[rs, :] = m
            zcol_ref[rs, :] = zc
    for rb in range(0, CH, RB):
        rs = slice(rb, rb + RB)
        zc = lane_max(zcol_ref[rs, :])
        m = jnp.maximum(lane_max(mcol_ref[rs, :]), zc)
        zcol_ref[rs, :] = jnp.broadcast_to(zc, (RB, LN))
        mcol_ref[rs, :] = jnp.broadcast_to(m, (RB, LN))

    def grp(g, _):
        rs = pl.ds(pl.multiple_of(g * RB, RB), RB)
        m = mcol_ref[rs, :]
        tot = jnp.zeros((RB, LN), F32)
        for k in range(0, rows, LN):
            ex = jnp.exp(e_ref[rs, k:k + LN] - m)
            e_ref[rs, k:k + LN] = ex
            tot += ex
        scol_ref[rs, :] = tot
        return 0
    lax.fori_loop(0, CH // RB, grp, 0)
    for rb in range(0, CH, RB):
        rs = slice(rb, rb + RB)
        tot = lane_sum(scol_ref[rs, :])
        scol_ref[rs, :] = jnp.broadcast_to(tot, (RB, LN)) + jnp.exp(zcol_ref[rs, :] - mcol_ref[rs, :])


def reduce_stats(pb, rb, zb, ab, st, sems, fill):
    z, y, x, c, v, a = coords()
    to_c, to_z, to_1, to_2 = peers()
    sp, rp, sz, rz, sa, ra = sems
    me = (y * NX + x) * 2 + c

    def merge(ref):
        m, s = ref[:, 0, :], ref[:, 1, :]
        top = jnp.max(m, axis=0, keepdims=True)
        return top, jnp.sum(s * jnp.exp(m - top), axis=0, keepdims=True), jnp.max(ref[:, 2, :], axis=0, keepdims=True)

    rb[me] = pb[me]
    pl.loop(1, SR)(lambda k: rcopy(pb.at[(me + k) % SR], rb.at[me], sp, rp, in_plane(k)).start())
    fill(0)
    rcopy(rb.at[pl.ds(0, PO)], rb.at[pl.ds(0, PO)], sp, rp, to_c).wait()
    for i, val in enumerate(merge(rb)):
        zb[z, i:i + 1, :] = val
    pl.loop(1, NZ)(lambda k: rcopy(zb.at[z], zb.at[z], sz, rz, to_z(k)).start())
    fill(1)
    rcopy(zb.at[pl.ds(0, ZO)], zb.at[pl.ds(0, ZO)], sz, rz, to_c).wait()
    m, s, t = merge(zb)
    ab[me, 0:1, :] = m + jnp.log(s)
    ab[me, 1:2, :] = t
    pl.loop(1, SR)(lambda k: rcopy(ab.at[me], ab.at[me], sa, ra, in_plane(k)).start())
    fill(2)
    rcopy(ab.at[pl.ds(0, PO)], ab.at[pl.ds(0, PO)], sa, ra, to_c).wait()
    st[1] = ab[:, 0, :]
    st[2] = ab[:, 1, :]
    return jnp.sum(ab[:, 0, :] - ab[:, 1, :]) * PER_TOKEN


def gelu_both(u):
    k0, k1 = math.sqrt(2.0 / math.pi), 0.044715
    sq = u * u
    t = jnp.tanh(k0 * (u + k1 * (sq * u)))
    cdf = 0.5 * (1.0 + t)
    return u * cdf, cdf + (0.5 * k0) * u * ((1.0 - t * t) * (1.0 + (3.0 * k1) * sq))


def step_kernel(x_hbm, win_hbm, wout_hbm, emb_hbm, cid_hbm, lq_hbm, y_s,
                loss_ref, de_hbm, gwi_hbm, gwo_hbm, h_hbm, st_hbm, lh_hbm, li_hbm, lg_hbm, xg,
                xv, win, wout, emb, cid_v, lq_v, lqr, hb, yb, dh,
                eb, pb, det, te, dcol, mcol, zcol, scol, yl, st, lh, li, lg, pst, rst, zst, ast,
                dq, rc, a0, ra, a1, rb, zb,
                lsem, osem, fsem, xsem, *sems):
    z, y, x, c, v, a = coords()
    to_c, to_z, to_1, to_2 = peers()
    rows = emb.shape[0]
    hid = win.shape[1]
    half = hid // 2
    me = lax.axis_index("dp")
    base = me * rows
    take = lambda n, it=iter(sems): [next(it) for _ in range(n)]
    gh, gd, gy = (take(len(Gather.SEMS)) for _ in range(3))
    gx = take(len(GatherFeatures.SEMS))
    own16 = pl.ds(me * TD, TD)
    loads = [pltpu.make_async_copy(s, d, lsem.at[i]) for i, (s, d) in enumerate((
        (x_hbm, xv), (win_hbm, win), (wout_hbm, wout), (emb_hbm, emb), (cid_hbm.at[own16], cid_v), (lq_hbm.at[own16], lq_v)))]
    for cp in loads[:2]:
        cp.start()
    bar, n_peers = signal_peers()
    for cp in loads[2:]:
        cp.start()

    for cp in loads[:3]:
        cp.wait()
    pre = jnp.dot(xv[...], win[...], preferred_element_type=F32)
    act = gelu_both(pre)[0].astype(BF16)
    hb[c, v, z, a] = jnp.dot(act, wout[...], preferred_element_type=F32).astype(BF16)
    lane16 = iota((1, LN), 1) % TD
    yb[c, v, z, a] = sum(jnp.where(lane16 == i, y_s[i], 0) for i in range(TD))
    pl.semaphore_wait(bar, n_peers)

    gath, gaty, gatx, gatd = Gather(hb, gh), GatherSmall(yb, gy), GatherFeatures(xg, gx, xv), Gather(dh, gd)
    xown = pltpu.make_async_copy(xv, gatx.own, xsem.at[0])
    gath.start()
    gaty.start()
    xown.start()
    gatx.two()
    for cp in loads[3:]:
        cp.wait()
    logq_rows(cid_v, lq_v, lqr, base)
    det[...] = jnp.zeros_like(det)
    gath.column(1)
    gath.rest(0)
    xown.wait()
    gatx.plane()
    gath.column(2)
    gaty.second()
    gath.rest(1)
    gath.rest(2)
    gath.to_c(0).start()
    gaty.first()

    lane = iota((LN, LN), 1)

    def score(cc, vv):
        ci = cc * NA + vv
        target_cols(lambda b: yb[cc, vv, b // NA, b % NA], base, yl, ci * GR, dcol.at[ci])
        scores_chunk(hb[cc, vv].reshape(CH, DIM), emb, lqr, eb.at[ci], dcol.at[ci], mcol.at[ci], zcol.at[ci], scol)
        for b in range(GR):
            bs_ = slice(b * LN, (b + 1) * LN)
            three = jnp.where(lane == 0, mcol[ci, bs_, :], jnp.where(lane == 1, scol[bs_, :], zcol[ci, bs_, :]))
            pst[ci * GR + b] = jnp.transpose(three)[:NA]

    @pl.loop(0, NC)
    def _(n):
        gaty.take(n)
        cv = gath.take(n)
        pl.when(n == 1)(gatx.ring)
        pl.when(n == 5)(lambda: gatx.move(1, 0))
        pl.when(n == NC_LAST)(lambda: gatx.move(1, 1))
        score(*cv)

    def target_rows(lo, hi):
        @pl.loop(lo, hi)
        def _(ci):
            for q in range(0, rows, LN):
                pb[:, q:q + LN] = ones_at(dcol[ci] == float(q)).astype(BF16)
            te[ci] = jnp.dot(pb[...], emb[...], preferred_element_type=F32).astype(BF16)

    def fill(n):
        if n:
            gatx.move(2, n - 1)
        target_rows(*((0, 3), (3, 6), (6, NC))[n])

    lr = st.at[1]
    loss_ref[0, 0] = reduce_stats(pst, rst, zst, ast, st, take(6), fill)
    @pl.loop(0, NC)
    def _(ci):
        for b in range(GR):
            bs_ = slice(b * LN, (b + 1) * LN)
            lc = to_col(lr[pl.ds(ci * GR + b, 1), :])
            mcol[ci, bs_, :] = jnp.exp(mcol[ci, bs_, :] - lc) * PER_TOKEN
            dcol[ci, bs_, :] = lc
    st[0] = yl[...].astype(F32)

    sc, rcs, sa, ras, sb, rbs, sz, rzs = take(8)
    ring = a0.shape[0]
    c_copy = lambda k: rcopy(dq.at[k % 2, 1 - c], rc.at[k], sc.at[k % 2], rcs.at[k], to_c)
    a_copy = lambda k, j: rcopy(a0.at[k % ring, (v + j) % NA], ra.at[k, v], sa.at[k % ring], ras.at[k], to_1(j))
    a_all = lambda k: rcopy(ra.at[k, pl.ds(0, AO)], ra.at[k, pl.ds(0, AO)], sa.at[k % ring], ras.at[k], to_c)
    b_copy = lambda k, j: rcopy(a1.at[k % ring, (a + j) % NA], rb.at[k, a], sb.at[k % ring], rbs.at[k], to_2(j))
    b_all = lambda k: rcopy(rb.at[k, pl.ds(0, AO)], rb.at[k, pl.ds(0, AO)], sb.at[k % ring], rbs.at[k], to_c)

    def off(k):
        s = (k + 1) // 2
        return NA + s - 2 * s * (k % 2)

    z_copy = lambda k: rcopy(zb.at[NZ + k], zb.at[z], sz, rzs, to_z(off(k)))

    def compute(k):
        zz = (z + off(k)) % NZ
        piece = pl.ds(pl.multiple_of(zz * PZ, PZ), PZ)
        for ci in range(NC):
            ps = slice(ci * PZ, (ci + 1) * PZ)
            f = mcol[ci, piece, :]
            for q in range(0, rows, LN):
                pb[ps, q:q + LN] = (eb[ci, piece, q:q + LN] * f).astype(BF16)
        h = jnp.concatenate([hb[ci // NA, ci % NA, zz].reshape(PZ, DIM) for ci in range(NC)], axis=0)
        for q in range(0, rows, CH):
            det[:, q:q + CH] += lax.dot_general(h, pb[:, q:q + CH], ROWS, preferred_element_type=F32)
        out = jnp.dot(pb[...], emb[...], preferred_element_type=F32)
        for ci in range(NC):
            zc = zcol[ci, piece, :]
            g = jnp.where(zc > NEG, (jnp.exp(zc - dcol[ci, piece, :]) - 1.0) * PER_TOKEN, 0.0)
            t = te[ci, piece, :].astype(F32)
            for hf in (0, LN):
                dq[k % 2, ci // NA, ci % NA, :, hf:hf + LN] = out[ci * PZ:(ci + 1) * PZ, hf:hf + LN] + g * t[:, hf:hf + LN]
        c_copy(k).start()

    def sum_core(k):
        c_copy(k).wait()
        a0[k % ring] = dq[k % 2, c] + rc[k]
        for j in NEAR:
            a_copy(k, j).start()

    def sum_first(k):
        a_all(k).wait()
        ra[k, v] = a0[k % ring, v]
        a1[k % ring] = tree([ra[k, i] for i in range(NA)]).reshape(NA, TD, DIM)
        for j in NEAR:
            b_copy(k, j).start()

    def sum_second(k, last=False):
        b_all(k).wait()
        rb[k, a] = a1[k % ring, a]
        val = tree([rb[k, i] for i in range(NA)])
        if last:
            zb[z] = val
        else:
            zb[NZ + k] = val
            z_copy(k).start()

    def body(k, _):
        compute(k)
        for lag, f in ((1, sum_core), (4, sum_first), (6, sum_second)):
            pl.when(k >= lag)(functools.partial(f, k - lag))
        pl.when(k == 0)(lambda: gatx.move(3, 0))
        pl.when(k == 2)(lambda: gatx.move(3, 1))
        pl.when(k == 7)(gatx.last)
        return 0

    lax.fori_loop(0, NZ, body, 0)
    de = eb.at[pl.ds(4, 4), :, pl.ds(DIM * 4, DIM)]
    for q in range(0, rows, LN):
        for w in (0, LN):
            de[q // CH, q % CH:q % CH + LN, w:w + LN] = jnp.transpose(det[w:w + LN, q:q + LN])
    outs = [pltpu.make_async_copy(s, d, osem.at[i]) for i, (s, d) in enumerate(((de, de_hbm.reshape(4, CH, DIM)), (hb, h_hbm), (st, st_hbm), (lh, lh_hbm), (li, li_hbm), (lg, lg_hbm)))]
    for cp in outs[:3]:
        cp.start()

    cols = pl.ds(pl.multiple_of(c * half, half), half)
    def xs(ci, slot, go):
        to = pl.ds(pl.multiple_of(slot * hid, hid), hid)
        if go:
            for zz in range(NZ):
                src = xg.at[ci // NA, zz, (ci % NA) // 2, ci % 2].reshape(PZ, hid)
                pltpu.make_async_copy(src, pb.at[pl.ds(zz * PZ, PZ), to], fsem.at[slot]).start()
        else:
            pltpu.make_async_copy(pb.at[:, to], pb.at[:, to], fsem.at[slot]).wait()

    def tower(ci, slot):
        pre = jnp.dot(pb[:, pl.ds(pl.multiple_of(slot * hid, hid), hid)], win[:, cols], preferred_element_type=F32)
        act, der = gelu_both(pre)
        eb[ci, :, :half] = der
        eb[ci, :, half:2 * half] = act.astype(BF16).astype(F32)

    ordinal = lambda n: gatd.place(n)[3][0] * NA + gatd.place(n)[3][1]

    def towers(lo, hi):
        @pl.loop(lo, hi)
        def _(n):
            pl.when(n + 1 < NC)(lambda: xs(ordinal(n + 1), (n + 1) % 2, True))
            xs(ordinal(n), n % 2, False)
            tower(ordinal(n), n % 2)

    sum_first(4)
    sum_core(7)
    sum_second(2)
    sum_second(3)
    gatx.shared.wait_recv()
    xs(ordinal(0), 0, True)
    sum_first(5)
    towers(0, 1)
    sum_first(6)
    sum_second(4)
    towers(1, 2)
    sum_first(7)
    sum_second(5)
    towers(2, 3)
    sum_second(6)
    sum_second(7, last=True)
    towers(3, 4)
    rcopy(zb.at[pl.ds(0, ZO)], zb.at[pl.ds(0, ZO)], sz, rzs, to_c).wait()
    tot = tree([zb[i] for i in range(NZ)])
    dh[c, v, z, a] = tot.astype(BF16)
    gatd.start()
    towers(4, 6)
    gatd.column(1)
    gatd.rest(0)
    gatd.column(2)
    towers(6, 7)
    gatd.rest(1)
    towers(7, NC)
    xs(ordinal(0), 0, True)
    gatd.rest(2)
    gatd.to_c(0).start()
    rank, gfac, _ = target_ranks(st, rows)
    target_page(0, st, rank, gfac, lambda r: token_rows(hb, r), lh, li, lg)
    for cp in outs[3:6]:
        cp.start()
    acc_i, acc_o = eb.at[pl.ds(0, 2), :, pl.ds(2 * half, half)], eb.at[2, :, pl.ds(2 * half, DIM)]
    acc_i[...] = jnp.zeros(acc_i.shape, F32)
    acc_o[...] = jnp.zeros(acc_o.shape, F32)

    so, ro = take(2)
    mine = [(acc_o, gwo_hbm.at[cols])] + [(acc_i.at[r], gwi_hbm.at[pl.ds(r * half, half), cols]) for r in range(2)]
    ends = [rcopy(s, d, so.at[i], ro.at[i], to_c) for i, (s, d) in enumerate(mine)]
    outs += [pltpu.make_async_copy(s, d, osem.at[6 + i]) for i, (s, d) in enumerate(mine)]
    early, late = ends[:2] + outs[6:8], ends[2:] + outs[8:]

    def weights(ci, slot, last=False):
        g = dh[ci // NA, ci % NA].reshape(CH, DIM)
        back = lax.dot_general(g, wout[cols, :], COLS, preferred_element_type=F32)
        da = (eb[ci, :, :half] * back).astype(BF16)
        act = eb[ci, :, half:2 * half].astype(BF16)
        acc_o[...] += lax.dot_general(act, g, ROWS, preferred_element_type=F32)
        for r in range(2):
            xr = pb[:, pl.ds(pl.multiple_of(slot * hid + r * half, half), half)]
            acc_i[r] += lax.dot_general(xr, da, ROWS, preferred_element_type=F32)
            if last and r == 0:
                for cp in early:
                    cp.start()

    @pl.loop(0, NC_LAST)
    def _(n):
        gatd.take(n)
        xs(ordinal(n + 1), (n + 1) % 2, True)
        xs(ordinal(n), n % 2, False)
        weights(ordinal(n), n % 2)

    gatd.take(NC_LAST)
    xs(ordinal(NC_LAST), NC_LAST % 2, False)
    weights(ordinal(NC_LAST), NC_LAST % 2, last=True)

    for g in (gath, gaty, gatx, gatd):
        g.finish()
    for cp in late:
        cp.start()
    for cp in ends + outs:
        cp.wait()


def step(features, w_in, w_out, table, cand_ids, log_q, targets):
    rows, dim = table.shape
    hid = w_in.shape[1]
    A, S = (pl.BlockSpec(memory_space=m) for m in (pl.ANY, pltpu.SMEM))
    sds = jax.ShapeDtypeStruct
    vm = pltpu.VMEM
    tokens = (2, NA, NZ, NA, TD)
    stat = lambda n: vm((n, NA, LN), F32)
    col = vm((NC, CH, LN), F32)
    return pl.pallas_call(
        step_kernel, name="step",
        out_shape=(sds((1, 1), F32), sds((rows, dim), F32), sds((w_in.shape[0], hid), F32), sds((hid, dim), F32), sds(tokens + (dim,), BF16),
                   sds((3, SR, LN), F32), sds((LN, dim), F32), sds((8, LN), jnp.int32), sds((8, LN), F32), sds((2, NZ, 2, 2, NA, TD, w_in.shape[0]), BF16)),
        in_specs=[A] * 6 + [S], out_specs=(S,) + (A,) * 9,
        scratch_shapes=[
            vm(features.shape, BF16), vm(w_in.shape, BF16), vm(w_out.shape, BF16), vm(table.shape, BF16), vm((TD, LN), jnp.int32), vm((TD, LN), F32),
            vm((8, rows), F32), vm(tokens + (dim,), BF16), vm((2, NA, NZ, NA, 1, LN), jnp.int32), vm(tokens + (dim,), BF16),
            vm((NC, CH, rows), F32), vm((CH, rows), BF16), vm((dim, rows), F32), vm((NC, CH, dim), BF16), col, col, col, vm((CH, LN), F32),
            vm((SR, LN), jnp.int32), vm((3, SR, LN), F32), vm((LN, dim), F32), vm((8, LN), jnp.int32), vm((8, LN), F32),
            stat(SR), stat(SR), stat(NZ), stat(SR),
            vm((2, 2, NA, PZ, dim), F32), vm((NZ, NA, PZ, dim), F32), vm((4, NA, PZ, dim), F32), vm((NZ, NA, PZ, dim), F32),
            vm((4, NA, TD, dim), F32), vm((NZ, NA, TD, dim), F32), vm((2 * NZ, TD, dim), F32),
            DMA((6,)), DMA((9,)), DMA((2,)), DMA((1,))] + Gather.SEMS * 2 + GatherSmall.SEMS + GatherFeatures.SEMS + [
            DMA] * 6 + [DMA((2,)), DMA((NZ,)), DMA((4,)), DMA((NZ,)), DMA((4,)), DMA((NZ,)), DMA, DMA, DMA((3,)), DMA((3,))],
        compiler_params=pltpu.CompilerParams(collective_id=0, has_side_effects=True, vmem_limit_bytes=VMEM_ALL),
    )(features, w_in, w_out, table, cand_ids.reshape(-1, LN), log_q.reshape(-1, LN), targets)


def target_ranks(st, rows):
    own = (st[0] >= 0) & (st[0] < rows)
    g = jnp.where(own, (jnp.exp(jnp.where(own, st[2], 0.0) - st[1]) - 1.0) * PER_TOKEN, 0.0)
    of = ones_at(own)
    before = lambda n, i, j: jnp.where(iota((n, n), i) < iota((n, n), j), 1.0, 0.0).astype(BF16)
    pre = jnp.dot(of.astype(BF16), before(LN, 0, 1), preferred_element_type=F32)
    tot = jnp.broadcast_to(lane_sum(of), (SR, LN))
    return jnp.where(own, pre + jnp.dot(before(SR, 1, 0), tot.astype(BF16), preferred_element_type=F32), -1.0), g, jnp.sum(of)


def target_page(p, st, rank, g, h_row, out_h, out_i, out_g):
    slot = (iota((LN, LN), 0) + p * LN).astype(F32)
    rr, gg = jnp.zeros((LN, LN), F32), jnp.zeros((LN, LN), F32)
    hh = jnp.zeros((LN, DIM), F32)
    for r in range(SR):
        rw = slice(r, r + 1)
        hit = rank[rw] == slot
        rr += jnp.where(hit, st[0, rw], 0.0)
        gg += jnp.where(hit, g[rw], 0.0)
        hh += jnp.dot(ones_at(hit).astype(BF16), h_row(r), preferred_element_type=F32)
    row = lambda m: jnp.transpose(jnp.broadcast_to(lane_sum(m), (LN, LN)))[:8]
    out_i[...] = row(rr).astype(jnp.int32)
    out_g[...] = row(gg)
    out_h[...] = hh


def token_rows(h, r):
    ci, g = r // GR, r % GR
    return h[ci // NA, ci % NA, 2 * g:2 * g + 2].reshape(LN, DIM)


def fix_kernel(de_hbm, h_hbm, st_hbm, lh_hbm, li_hbm, lg_hbm, gwi_hbm, gwo_hbm, out_hbm, wi_hbm, wo_hbm,
               de, h, st, wi, wo, lh, li, lg, si, sg, sem):
    rows = de.shape[0]
    part = [pl.ds(q, CH // 2) for q in range(0, wi.shape[0], CH // 2)]
    pairs = [(st_hbm, st), (li_hbm, si), (lg_hbm, sg), (lh_hbm, lh), (de_hbm, de), (gwo_hbm, wo)] + [(gwi_hbm.at[q], wi.at[q]) for q in part]
    ins = [pltpu.make_async_copy(s, d, sem.at[i]) for i, (s, d) in enumerate(pairs)]
    outs = [pltpu.make_async_copy(s, d, sem.at[len(ins) + i]) for i, (s, d) in enumerate([(de, out_hbm), (wo, wo_hbm)] + [(wi.at[q], wi_hbm.at[q]) for q in part])]
    for cp in ins:
        cp.start()
    ins[0].wait()
    own = (st[0] >= 0) & (st[0] < rows)
    n = jnp.sum(ones_at(own)).astype(jnp.int32)
    for i, o in zip(ins[5:], outs[1:]):
        i.wait()
        o.start()
    for cp in ins[1:5]:
        cp.wait()

    def page(p, _):
        @pl.when(p > 0)
        def _():
            run([pltpu.make_async_copy(h_hbm, h, sem.at[0])])
            rank, g, _ = target_ranks(st, rows)
            target_page(p, st, rank, g, lambda r: token_rows(h, r), lh, li, lg)
            run([pltpu.make_async_copy(li, si, sem.at[1]), pltpu.make_async_copy(lg, sg, sem.at[2])])

        @pl.loop(0, jnp.minimum(n - p * LN, LN))
        def _(i):
            de[pl.ds(si[0, i], 1), :] += sg[0, i] * lh[pl.ds(i, 1), :]
        return 0
    lax.fori_loop(0, (n + LN - 1) // LN, page, 0)
    outs[0].start()
    for cp in outs:
        cp.wait()


def fix(de, h, st, lh, li, lg, gwi, gwo):
    A = pl.BlockSpec(memory_space=pl.ANY)
    vm = lambda m: pltpu.VMEM(m.shape, m.dtype)
    like = lambda m: jax.ShapeDtypeStruct(m.shape, F32)
    return pl.pallas_call(
        fix_kernel, name="fix", out_shape=(like(de), like(gwi), like(gwo)), in_specs=[A] * 8, out_specs=(A,) * 3,
        scratch_shapes=[vm(de), vm(h), vm(st), vm(gwi), vm(gwo), vm(lh), vm(li), vm(lg), pltpu.SMEM(li.shape, jnp.int32), pltpu.SMEM(lg.shape, F32), DMA((16,))],
        compiler_params=pltpu.CompilerParams(vmem_limit_bytes=VMEM_ALL),
    )(de, h, st, lh, li, lg, gwi, gwo)


def solution(mesh):
    def local_step(*args):
        loss, de, gwi, gwo, *rest, _ = step(*args)
        return loss.reshape(()), *fix(de, *rest, gwi, gwo)

    return jax.shard_map(local_step, mesh=mesh, in_specs=(P("dp", None), P(), P(), P("dp", None), P(), P(), P("dp")), out_specs=(P(), P("dp", None), P(), P()), check_vma=False)
```
